8 devices in a mesh: part: 1 (over z), data: 2 (over y), model: 4 (over x, core).
Axes of the slice: x: 2, y: 2, z: 1, core: 2. Of those that a mesh axis runs over, the one named last changes fastest.
Arguments:
- x: bfloat16 [2, 32, 1024, 768], P(None, ('part', 'data'), 'model')
- lengths: int32 [2, 32], P(None, ('part', 'data'))
- norm_gain: bfloat16 [2, 768], P(None, 'data')
- w_in: bfloat16 [2, 768, 6912], P(None, 'data', 'model')
- w_kv: bfloat16 [2, 768, 128], P(None, 'data')
- w_out: bfloat16 [2, 3840, 768], P(None, 'model', 'data')
Outputs:
- output: bfloat16 [2, 32, 1024, 768], P(None, ('part', 'data'), 'model')
All inputs are finite; a program needn't handle non-finite values.
Results may differ from the reference program's by a relative error of at most 0.0131665.
Values are sent between devices in bfloat16 or wider.
A program may use at most 1 GiB of HBM per device.

```python
import math
import jax
import jax.numpy as jnp
from jax import lax

N_MICRO = 2
N_LAYERS = 2
N_SEQS = 32
SEQ_LEN = 1024
D_MODEL = 768
N_HEADS = 12
HEAD_DIM = 64
D_FF = 3072
MODEL_SHARDS = 4
FF_HEAD = D_FF // N_HEADS
UNIT_IN = HEAD_DIM + 2 * FF_HEAD
UNIT_OUT = HEAD_DIM + FF_HEAD
SHARD_ROWS = (N_HEADS // MODEL_SHARDS) * UNIT_OUT
NORM_EPS = 1e-6
NEG_BIG = -1e30
Q_GAIN = math.sqrt(max(math.log(SEQ_LEN / 8.0), 1.0))


def setup_inputs(seed: int = 0, part: int = 0) -> dict:
    part_keys = jax.random.split(jax.random.fold_in(jax.random.key(seed), part), 2)
    shared_keys = jax.random.split(jax.random.key(seed + 1), 4)
    x_act = jax.random.normal(part_keys[0], (N_MICRO, N_SEQS, SEQ_LEN, D_MODEL), jnp.float32)
    seq_lens = jax.random.randint(part_keys[1], (N_MICRO, N_SEQS), SEQ_LEN // 4, SEQ_LEN + 1)
    seq_lens = seq_lens.at[0, 0].set(SEQ_LEN).at[1, 0].set(SEQ_LEN // 4)
    gain_vals = jax.random.uniform(shared_keys[0], (N_LAYERS, D_MODEL), jnp.float32, 0.5, 1.5)
    col_scale = jnp.concatenate([jnp.full((HEAD_DIM,), Q_GAIN, jnp.float32), jnp.ones((2 * FF_HEAD,), jnp.float32)]) * (D_MODEL ** -0.5)
    w_in_vals = jax.random.normal(shared_keys[1], (N_LAYERS, D_MODEL, N_HEADS, UNIT_IN), jnp.float32) * col_scale
    w_kv_vals = jax.random.normal(shared_keys[2], (N_LAYERS, D_MODEL, 2 * HEAD_DIM), jnp.float32) * (D_MODEL ** -0.5)
    row_scale = jnp.concatenate([jnp.full((HEAD_DIM,), (N_HEADS * HEAD_DIM) ** -0.5, jnp.float32), jnp.full((FF_HEAD,), D_FF ** -0.5, jnp.float32)])
    w_out_vals = jax.random.normal(shared_keys[3], (N_LAYERS, N_HEADS, UNIT_OUT, D_MODEL), jnp.float32) * row_scale[:, None]
    return {
        "x": x_act.astype(jnp.bfloat16),
        "lengths": seq_lens.astype(jnp.int32),
        "norm_gain": gain_vals.astype(jnp.bfloat16),
        "w_in": w_in_vals.reshape(N_LAYERS, D_MODEL, N_HEADS * UNIT_IN).astype(jnp.bfloat16),
        "w_kv": w_kv_vals.astype(jnp.bfloat16),
        "w_out": w_out_vals.reshape(N_LAYERS, N_HEADS * UNIT_OUT, D_MODEL).astype(jnp.bfloat16),
    }


def layer_one_seq(x_seq, seq_len, gain_vec, w_in_l, w_kv_l, w_out_l):
    x_f32 = x_seq.astype(jnp.float32)
    centered = x_f32 - jnp.mean(x_f32, axis=-1, keepdims=True)
    variance = jnp.mean(centered * centered, axis=-1, keepdims=True)
    h_act = (centered * lax.rsqrt(variance + NORM_EPS) * gain_vec.astype(jnp.float32)).astype(jnp.bfloat16)
    projected = jnp.dot(h_act, w_in_l, preferred_element_type=jnp.float32).astype(jnp.bfloat16)
    projected = projected.reshape(SEQ_LEN, N_HEADS, UNIT_IN)
    q_heads = projected[:, :, :HEAD_DIM]
    gate_act = projected[:, :, HEAD_DIM:HEAD_DIM + FF_HEAD]
    up_act = projected[:, :, HEAD_DIM + FF_HEAD:]
    kv_act = jnp.dot(h_act, w_kv_l, preferred_element_type=jnp.float32).astype(jnp.bfloat16)
    k_act = kv_act[:, :HEAD_DIM]
    v_act = kv_act[:, HEAD_DIM:]
    scores = jnp.einsum("qhc,kc->hqk", q_heads.astype(jnp.float32), k_act.astype(jnp.float32)) * (1.0 / math.sqrt(HEAD_DIM))
    positions = jnp.arange(SEQ_LEN)
    allowed = (positions[None, :] <= positions[:, None]) & (positions[None, :] < seq_len)
    scores = jnp.where(allowed[None], scores, NEG_BIG)
    attn_probs = jax.nn.softmax(scores, axis=-1).astype(jnp.bfloat16)
    attn_out = jnp.einsum("hqk,kc->qhc", attn_probs.astype(jnp.float32), v_act.astype(jnp.float32)).astype(jnp.bfloat16)
    mlp_out = (jax.nn.silu(gate_act.astype(jnp.float32)) * up_act.astype(jnp.float32)).astype(jnp.bfloat16)
    joined = jnp.concatenate([attn_out, mlp_out], axis=-1).reshape(SEQ_LEN, MODEL_SHARDS, SHARD_ROWS)
    w_groups = w_out_l.reshape(MODEL_SHARDS, SHARD_ROWS, D_MODEL)

    def add_group(running, group_pair):
        rows_in, w_rows = group_pair
        group_sum = jnp.dot(rows_in, w_rows, preferred_element_type=jnp.float32).astype(jnp.bfloat16)
        return running + group_sum.astype(jnp.float32), None

    z_sum, _ = lax.scan(add_group, jnp.zeros((SEQ_LEN, D_MODEL), jnp.float32), (jnp.swapaxes(joined, 0, 1), w_groups))
    return (x_f32 + z_sum).astype(jnp.bfloat16)


def reference(x, lengths, norm_gain, w_in, w_kv, w_out):
    seqs_x = x.reshape(N_MICRO * N_SEQS, SEQ_LEN, D_MODEL)
    seqs_len = lengths.reshape(N_MICRO * N_SEQS)

    def run_seq(seq_item):
        x_seq, seq_len = seq_item

        def one_layer(carry_x, weights):
            gain_l, w_in_l, w_kv_l, w_out_l = weights
            return layer_one_seq(carry_x, seq_len, gain_l, w_in_l, w_kv_l, w_out_l), None

        final_x, _ = lax.scan(one_layer, x_seq, (norm_gain, w_in, w_kv, w_out))
        return final_x

    y_all = lax.map(run_seq, (seqs_x, seqs_len))
    return y_all.reshape(N_MICRO, N_SEQS, SEQ_LEN, D_MODEL)
```

```python
import functools
import jax
import jax.numpy as jnp
from jax import lax
from jax.experimental import pallas as pl
from jax.experimental.pallas import tpu as pltpu
from jax.sharding import PartitionSpec as P

NORM_EPS = 1e-6
NEG_BIG = -1e30
F32 = jnp.float32
BF16 = jnp.bfloat16


def norm_rows(x_act, gain_row):
    x_f32 = x_act.astype(F32)
    centered = x_f32 - jnp.mean(x_f32, axis=-1, keepdims=True)
    variance = jnp.mean(centered * centered, axis=-1, keepdims=True)
    return (centered * lax.rsqrt(variance + NORM_EPS) * gain_row.astype(F32)).astype(BF16)


def kv_kernel(x_ref, gain_ref, w_kv_ref, kv_ref):
    n_seqs, t_loc, d_model = x_ref.shape
    h = norm_rows(x_ref[...].reshape(n_seqs * t_loc, d_model), gain_ref[...])
    kv = jnp.dot(h, w_kv_ref[...], preferred_element_type=F32).astype(BF16)
    kv_ref[...] = kv.reshape(kv_ref.shape)


def project_kv(x, gain, w_kv, micro, block=4):
    _, n_seqs, t_loc, d_model = x.shape
    width = w_kv.shape[1]
    return pl.pallas_call(
        kv_kernel,
        grid=(n_seqs // block,),
        in_specs=[
            pl.BlockSpec((None, block, t_loc, d_model), lambda b: (micro, b, 0, 0)),
            pl.BlockSpec((1, d_model), lambda b: (0, 0)),
            pl.BlockSpec((d_model, width), lambda b: (0, 0)),
        ],
        out_specs=pl.BlockSpec((block, t_loc, width), lambda b: (b, 0, 0)),
        out_shape=jax.ShapeDtypeStruct((n_seqs, t_loc, width), BF16),
        name="kv_proj",
        cost_estimate=pl.CostEstimate(
            flops=2 * n_seqs * t_loc * d_model * width, bytes_accessed=2 * n_seqs * t_loc * (d_model + width), transcendentals=0
        ),
    )(x, gain, w_kv)


def layer_kernel(n_groups, head_dim, has_next, has_prev, *refs):
    refs = list(refs)
    pos_ref, len_ref = refs[:2]
    x_ref, kv_ref, gain_ref, w_in_hbm, w_out_hbm = refs[2:7]
    refs = refs[7:]
    if has_next:
        gain_next_ref, w_kv_next_ref = refs[:2]
        refs = refs[2:]
    if has_prev:
        refs = refs[1:]
    y_ref = refs[0]
    refs = refs[1:]
    if has_next:
        kv_next_ref = refs[0]
        refs = refs[1:]
    w_in_ref, w_out_ref, h_ref, vt_ref, acc_ref, in_sem, out_sem = refs

    t_loc, d_model = x_ref.shape
    n_chunks = kv_ref.shape[0]
    rows_out = w_out_ref.shape[1]
    half = w_out_hbm.shape[3]
    n_parts = w_out_hbm.shape[1]
    in_loc = w_in_ref.shape[2]
    ff_loc = in_loc - rows_out
    q_loc = rows_out - ff_loc
    heads = q_loc // head_dim
    seq = pl.program_id(0)

    def in_copy(group):
        return pltpu.make_async_copy(w_in_hbm.at[group], w_in_ref.at[group], in_sem.at[group])

    def out_copy(group, part):
        return pltpu.make_async_copy(
            w_out_hbm.at[group, part], w_out_ref.at[group, :, pl.ds(part * half, half)], out_sem.at[group, part]
        )

    @pl.when(seq == 0)
    def _():
        for group in range(n_groups):
            in_copy(group).start()
            for part in range(n_parts):
                out_copy(group, part).start()

    pos = pos_ref[0]
    seq_len = len_ref[seq]
    n_live = jnp.minimum(pos + 1, (seq_len + t_loc - 1) // t_loc)

    h_ref[...] = norm_rows(x_ref[...], gain_ref[...])
    vt_ref[...] = kv_ref[...].reshape(n_chunks * t_loc, 2 * head_dim).T[head_dim:]
    acc_ref[...] = jnp.zeros_like(acc_ref)

    def run(n_keys):
        chunk = n_keys - 1
        lane = lax.broadcasted_iota(jnp.int32, (1, t_loc), 1)
        limit = jnp.minimum(lane + (pos - chunk) * t_loc, seq_len - chunk * t_loc - 1)
        key = lax.broadcasted_iota(jnp.int32, (t_loc, t_loc), 0)
        keys = kv_ref[:n_keys].reshape(n_keys * t_loc, 2 * head_dim)[:, :head_dim]

        def group_step(group, carry):
            @pl.when(seq == 0)
            def _():
                in_copy(group).wait()
                for part in range(n_parts):
                    out_copy(group, part).wait()

            h = h_ref[...]
            q = jnp.dot(h, w_in_ref[group, :, 2 * ff_loc :], preferred_element_type=F32).astype(BF16)
            q_t = (q * BF16(head_dim**-0.5)).T
            joined = []
            step = 256
            for col in range(0, ff_loc, step):
                gate = jnp.dot(h, w_in_ref[group, :, col : col + step], preferred_element_type=F32).astype(BF16).astype(F32)
                up = jnp.dot(h, w_in_ref[group, :, ff_loc + col : ff_loc + col + step], preferred_element_type=F32).astype(BF16).astype(F32)
                joined.append((jax.nn.silu(gate) * up).astype(BF16))
            outs = []
            for head in range(heads):
                scores = jnp.dot(keys, q_t[head * head_dim : (head + 1) * head_dim], preferred_element_type=F32)
                last = jnp.where(key <= limit, scores[chunk * t_loc :], NEG_BIG)
                top = jnp.max(last, axis=0, keepdims=True)
                if chunk:
                    top = jnp.maximum(top, jnp.max(scores[: chunk * t_loc], axis=0, keepdims=True))
                    scores = jnp.concatenate([scores[: chunk * t_loc], last], axis=0)
                else:
                    scores = last
                weights = jnp.exp(scores - top)
                total = jnp.sum(weights, axis=0, keepdims=True)
                out_t = jnp.dot(vt_ref[:, : n_keys * t_loc], weights.astype(BF16), preferred_element_type=F32)
                outs.append((out_t / total).astype(BF16))
            joined.append(jnp.concatenate(outs, axis=0).T)
            joined = jnp.concatenate(joined, axis=1)
            z = jnp.dot(joined, w_out_ref[group], preferred_element_type=F32)
            acc_ref[...] += z.astype(BF16).astype(F32)
            return carry

        lax.fori_loop(0, n_groups, group_step, 0)

    for n_keys in range(1, n_chunks + 1):
        pl.when(n_live == n_keys)(functools.partial(run, n_keys))

    y = (x_ref[...].astype(F32) + acc_ref[...]).astype(BF16)
    y_ref[...] = y
    if has_next:
        h_next = norm_rows(y, gain_next_ref[...])
        kv_next_ref[...] = jnp.dot(h_next, w_kv_next_ref[...], preferred_element_type=F32).astype(BF16)


def run_layer(pos, lengths, x, kv, gain, w_in, w_out, head_dim, micro, next_params=None, prev=None, whole=None):
    if x.ndim == 4:
        x_spec = pl.BlockSpec((None, None) + x.shape[2:], lambda b, *_: (micro, b, 0, 0))
    else:
        x_spec = pl.BlockSpec((None,) + x.shape[1:], lambda b, *_: (b, 0, 0))
    n_seqs, t_loc, d_model = x.shape[-3:]
    n_groups, _, in_loc = w_in.shape
    _, n_parts, rows_out, _ = w_out.shape
    n_chunks = kv.shape[0]
    width = kv.shape[3]
    anywhere = pl.BlockSpec(memory_space=pl.ANY)
    in_specs = [
        x_spec,
        pl.BlockSpec((n_chunks, None, t_loc, width), lambda b, *_: (0, b, 0, 0)),
        pl.BlockSpec((1, d_model), lambda b, *_: (0, 0)),
        anywhere,
        anywhere,
    ]
    args = [x, kv, gain, w_in, w_out]
    if next_params is not None:
        in_specs += [pl.BlockSpec((1, d_model), lambda b, *_: (0, 0)), pl.BlockSpec((d_model, width), lambda b, *_: (0, 0))]
        args += list(next_params)
    aliases = {}
    if prev is not None:
        in_specs.append(anywhere)
        aliases = {2 + len(args): 0}
        args.append(prev)
    if whole is None:
        out_shape = [jax.ShapeDtypeStruct((n_seqs, t_loc, d_model), BF16)]
        out_specs = [pl.BlockSpec((None, t_loc, d_model), lambda b, *_: (b, 0, 0))]
    else:
        out_shape = [jax.ShapeDtypeStruct((whole, n_seqs, t_loc, d_model), BF16)]
        out_specs = [pl.BlockSpec((None, None, t_loc, d_model), lambda b, *_: (micro, b, 0, 0))]
    if next_params is not None:
        out_shape.append(jax.ShapeDtypeStruct((n_seqs, t_loc, width), BF16))
        out_specs.append(pl.BlockSpec((None, t_loc, width), lambda b, *_: (b, 0, 0)))
    rows = n_seqs * t_loc
    flops = 2 * rows * n_groups * d_model * (in_loc + rows_out) + 8 * rows * n_groups * n_chunks * t_loc * (rows_out * 2 - in_loc + rows_out)
    return pl.pallas_call(
        functools.partial(layer_kernel, n_groups, head_dim, next_params is not None, prev is not None),
        grid_spec=pltpu.PrefetchScalarGridSpec(
            num_scalar_prefetch=2,
            grid=(n_seqs,),
            in_specs=in_specs,
            out_specs=out_specs,
            scratch_shapes=[
                pltpu.VMEM((n_groups, d_model, in_loc), BF16),
                pltpu.VMEM((n_groups, rows_out, d_model), BF16),
                pltpu.VMEM((t_loc, d_model), BF16),
                pltpu.VMEM((head_dim, n_chunks * t_loc), BF16),
                pltpu.VMEM((t_loc, d_model), F32),
                pltpu.SemaphoreType.DMA((n_groups,)),
                pltpu.SemaphoreType.DMA((n_groups, n_parts)),
            ],
        ),
        out_shape=out_shape,
        input_output_aliases=aliases,
        name="layer",
        compiler_params=pltpu.CompilerParams(dimension_semantics=("arbitrary",), vmem_limit_bytes=60 * 2**20),
        cost_estimate=pl.CostEstimate(flops=flops, bytes_accessed=4 * rows * d_model + 2 * n_groups * d_model * (in_loc + rows_out), transcendentals=0),
    )(pos, lengths, *args)


def solution(mesh):
    n_model = mesh.shape["model"]
    act_spec = P(None, ("part", "data"), "model", None)

    def local_fn(x, lengths, gain_blk, w_in_blk, w_kv_blk, w_out_blk):
        n_micro = x.shape[0]
        n_layers, d_half, in_loc = w_in_blk.shape
        out_loc = w_out_blk.shape[1]
        head_dim = w_kv_blk.shape[2] // 2
        ff_loc = in_loc - out_loc
        heads = (out_loc - ff_loc) // head_dim
        ff_head = ff_loc // heads
        pos = lax.axis_index("model").astype(jnp.int32).reshape(1)

        gain = lax.all_gather(gain_blk, "data", axis=1, tiled=True)
        w_kv = lax.all_gather(w_kv_blk, "data", axis=1, tiled=True)

        cols = w_in_blk.reshape(n_layers, d_half, heads, in_loc // heads)
        w_in_sorted = jnp.concatenate(
            [
                cols[..., head_dim : head_dim + ff_head].reshape(n_layers, d_half, ff_loc),
                cols[..., head_dim + ff_head :].reshape(n_layers, d_half, ff_loc),
                cols[..., :head_dim].reshape(n_layers, d_half, heads * head_dim),
            ],
            axis=-1,
        )
        rows = w_out_blk.reshape(n_layers, heads, out_loc // heads, d_half)
        w_out_sorted = jnp.concatenate(
            [rows[:, :, head_dim:].reshape(n_layers, ff_loc, d_half), rows[:, :, :head_dim].reshape(n_layers, heads * head_dim, d_half)],
            axis=1,
        )

        def weights(layer):
            w_in = lax.all_gather(w_in_sorted[layer], ("model", "data"), axis=0, tiled=False)
            w_out = lax.all_gather(w_out_sorted[layer], ("model", "data"), axis=0, tiled=False)
            return w_in.reshape(n_model, -1, in_loc), w_out.reshape(n_model, -1, out_loc, d_half)

        def gains(layer):
            return gain[layer].reshape(1, -1)

        kv = [
            lax.all_gather(project_kv(x, gains(0), w_kv[0], micro), "model", axis=0, tiled=False) for micro in range(n_micro)
        ]
        hidden = [x] * n_micro
        result = None
        for layer in range(n_layers):
            w_in, w_out = weights(layer)
            last = layer == n_layers - 1
            kv_next = []
            for micro in range(n_micro):
                outs = run_layer(
                    pos, lengths[micro], hidden[micro], kv[micro], gains(layer), w_in, w_out, head_dim, micro,
                    next_params=None if last else (gains(layer + 1), w_kv[layer + 1]),
                    prev=result if last else None,
                    whole=n_micro if last else None,
                )
                if last:
                    result = outs[0]
                else:
                    hidden[micro] = outs[0]
                    kv_next.append(lax.all_gather(outs[1], "model", axis=0, tiled=False))
            kv = kv_next
        return result

    return jax.shard_map(
        local_fn,
        mesh=mesh,
        in_specs=(act_spec, P(None, ("part", "data")), P(None, "data"), P(None, "data", "model"), P(None, "data", None), P(None, "model", "data")),
        out_specs=act_spec,
        check_vma=False,
    )
```

```python
import functools
import jax
import jax.numpy as jnp
from jax import lax
from jax.experimental import pallas as pl
from jax.experimental.pallas import tpu as pltpu
from jax.sharding import PartitionSpec as P

NORM_EPS = 1e-6
NEG_BIG = -1e30
F32 = jnp.float32
BF16 = jnp.bfloat16


def norm_rows(x_act, gain_row):
    x_f32 = x_act.astype(F32)
    centered = x_f32 - jnp.mean(x_f32, axis=-1, keepdims=True)
    variance = jnp.mean(centered * centered, axis=-1, keepdims=True)
    return (centered * lax.rsqrt(variance + NORM_EPS) * gain_row.astype(F32)).astype(BF16)


def kv_kernel(x_ref, gain_ref, w_kv_ref, kv_ref):
    n_seqs, t_loc, d_model = x_ref.shape
    h = norm_rows(x_ref[...].reshape(n_seqs * t_loc, d_model), gain_ref[...])
    kv = jnp.dot(h, w_kv_ref[...], preferred_element_type=F32).astype(BF16)
    kv_ref[...] = kv.reshape(kv_ref.shape)


def project_kv(x, gain, w_kv, micro, block=4):
    _, n_seqs, t_loc, d_model = x.shape
    width = w_kv.shape[1]
    return pl.pallas_call(
        kv_kernel,
        grid=(n_seqs // block,),
        in_specs=[
            pl.BlockSpec((None, block, t_loc, d_model), lambda b: (micro, b, 0, 0)),
            pl.BlockSpec((1, d_model), lambda b: (0, 0)),
            pl.BlockSpec((d_model, width), lambda b: (0, 0)),
        ],
        out_specs=pl.BlockSpec((block, t_loc, width), lambda b: (b, 0, 0)),
        out_shape=jax.ShapeDtypeStruct((n_seqs, t_loc, width), BF16),
        name="kv_proj",
        cost_estimate=pl.CostEstimate(
            flops=2 * n_seqs * t_loc * d_model * width, bytes_accessed=2 * n_seqs * t_loc * (d_model + width), transcendentals=0
        ),
    )(x, gain, w_kv)


def layer_kernel(n_groups, head_dim, has_next, has_prev, *refs):
    refs = list(refs)
    pos_ref, len_ref = refs[:2]
    x_after_ref, x_before_ref, kv_ref, kv_after_ref, gain_ref, w_in_hbm, w_out_hbm = refs[2:9]
    refs = refs[9:]
    if has_next:
        gain_next_ref, w_kv_next_ref = refs[:2]
        refs = refs[2:]
    if has_prev:
        refs = refs[1:]
    y_ref = refs[0]
    refs = refs[1:]
    if has_next:
        kv_next_ref = refs[0]
        refs = refs[1:]
    w_in_ref, w_out_ref, h_ref, vt_ref, joined_ref, acc_ref, s_ref, p_ref, in_sem, out_sem = refs

    t_loc, d_model = x_after_ref.shape
    n_chunks = kv_ref.shape[0]
    rows_out = w_out_ref.shape[1]
    half = w_out_hbm.shape[3]
    n_parts = w_out_hbm.shape[1]
    in_loc = w_in_ref.shape[2]
    ff_loc = in_loc - rows_out
    q_loc = rows_out - ff_loc
    heads = q_loc // head_dim
    step = pl.program_id(0)
    n_seqs = pl.num_programs(0) - 1
    tile = 256
    rows_part = t_loc // 2

    def in_copy(group):
        return pltpu.make_async_copy(w_in_hbm.at[group], w_in_ref.at[group], in_sem.at[group])

    def out_copy(group, part):
        return pltpu.make_async_copy(
            w_out_hbm.at[group, part], w_out_ref.at[group, :, pl.ds(part * half, half)], out_sem.at[group, part]
        )

    pos = pos_ref[0]
    slot = lax.rem(step, 2)
    other = 1 - slot

    def normalize_part(dst, src_ref, part):
        rows = pl.ds(part * rows_part, rows_part)
        h_ref[dst, rows] = norm_rows(src_ref[rows], gain_ref[...])

    def transpose_part(dst, src_ref, part):
        span = n_chunks // 2
        block = src_ref[pl.ds(part * span, span)].reshape(span * t_loc, 2 * head_dim)
        vt_ref[dst, part] = block.T[head_dim:]

    def epilogue_part(src, part):
        rows = pl.ds(part * rows_part, rows_part)
        y = (x_before_ref[rows].astype(F32) + acc_ref[src, rows]).astype(BF16)
        y_ref[rows] = y
        if has_next:
            h_next = norm_rows(y, gain_next_ref[...])
            kv_next_ref[rows] = jnp.dot(h_next, w_kv_next_ref[...], preferred_element_type=F32).astype(BF16)

    def project_out(joined_slot, group, dst, fresh, col):
        cols = slice(col, col + tile)
        z = jnp.dot(joined_ref[joined_slot], w_out_ref[group, :, cols], preferred_element_type=F32)
        z = z.astype(BF16).astype(F32)
        base = acc_ref[dst, :, cols]
        if fresh is not None:
            base = jnp.where(fresh, 0.0, base)
        acc_ref[dst, :, cols] = base + z

    @pl.when(step == 0)
    def _():
        for group in range(n_groups):
            in_copy(group).start()
            for part in range(n_parts):
                out_copy(n_groups - 1 if group == 0 else group - 1, part).start()
        for part in range(2):
            normalize_part(slot, x_before_ref, part)
            transpose_part(slot, kv_ref, part)
        joined_ref[1] = jnp.zeros_like(joined_ref[1])
        acc_ref[1] = jnp.zeros_like(acc_ref[1])

    @pl.when(step == n_seqs)
    def _():
        for col in range(0, d_model, tile):
            project_out(1, n_groups - 1, other, None, col)
        for part in range(2):
            epilogue_part(other, part)

    def run(n_keys):
        chunk = n_keys - 1
        seq_len = len_ref[jnp.minimum(step, n_seqs - 1)]
        lane = lax.broadcasted_iota(jnp.int32, (1, t_loc), 1)
        limit = jnp.minimum(lane + (pos - chunk) * t_loc, seq_len - chunk * t_loc - 1)
        key = lax.broadcasted_iota(jnp.int32, (t_loc, t_loc), 0)

        def trip(pair, carry):
            first = 2 * pair
            before = lax.rem(first + n_groups - 1, n_groups)

            @pl.when(step == 0)
            def _():
                @pl.when(pair == 0)
                def _():
                    for part in range(n_parts):
                        out_copy(n_groups - 1, part).wait()

                @pl.when(pair != 0)
                def _():
                    for part in range(n_parts):
                        out_copy(before, part).wait()

                in_copy(first).wait()
                in_copy(first + 1).wait()
                for part in range(n_parts):
                    out_copy(first, part).wait()

            h = h_ref[slot]
            dst_before = jnp.where(pair == 0, other, slot)
            queries = {}
            tops = {}
            sums = {}

            def query(sub):
                q = jnp.dot(h, w_in_ref[first + sub, :, 2 * ff_loc :], preferred_element_type=F32).astype(BF16)
                queries[sub] = (q * BF16(head_dim**-0.5)).T

            def gate_up(sub, part):
                col = part * tile
                gate = jnp.dot(h, w_in_ref[first + sub, :, col : col + tile], preferred_element_type=F32).astype(BF16).astype(F32)
                up = jnp.dot(h, w_in_ref[first + sub, :, ff_loc + col : ff_loc + col + tile], preferred_element_type=F32).astype(BF16).astype(F32)
                joined_ref[sub, :, col : col + tile] = (jax.nn.silu(gate) * up).astype(BF16)

            def score(sub, head):
                q_t = queries[sub][head * head_dim : (head + 1) * head_dim]
                best = None
                for c in range(n_keys):
                    s = jnp.dot(kv_ref[c, :, :head_dim], q_t, preferred_element_type=F32)
                    if c == chunk:
                        s = jnp.where(key <= limit, s, NEG_BIG)
                    s_ref[head, c * t_loc : (c + 1) * t_loc] = s
                    m = jnp.max(s.reshape(t_loc // 8, 8, t_loc), axis=0)
                    best = m if best is None else jnp.maximum(best, m)
                tops[sub, head] = jnp.max(best, axis=0, keepdims=True)

            def softmax(sub, head):
                total = None
                top = tops[sub, head]
                width = 64
                for r in range(0, n_keys * t_loc, width):
                    e = jnp.exp(s_ref[head, r : r + width] - top)
                    t = jnp.sum(e.reshape(width // 8, 8, t_loc), axis=0)
                    total = t if total is None else total + t
                    p_ref[head, r : r + width] = e.astype(BF16)
                sums[sub, head] = jnp.sum(total, axis=0, keepdims=True)

            outs = {}

            def value(sub, head):
                span = n_chunks // 2 * t_loc
                out_t = None
                for part in range(2):
                    size = min(span, n_keys * t_loc - part * span)
                    if size <= 0:
                        continue
                    o = jnp.dot(vt_ref[slot, part, :, :size], p_ref[head, part * span : part * span + size], preferred_element_type=F32)
                    out_t = o if out_t is None else out_t + o
                outs[sub, head] = (out_t / sums[sub, head]).astype(BF16)
                if head == heads - 1:
                    joined_ref[sub, :, ff_loc:] = jnp.concatenate([outs[sub, i] for i in range(heads)], axis=0).T

            for sub in range(2):
                query(sub)
                if sub == 0:
                    z = lambda i: project_out(1, before, dst_before, None, i * tile)
                else:
                    z = lambda i: project_out(0, first, slot, pair == 0, i * tile)
                z(0)
                score(sub, 0)
                z(1)
                score(sub, 1)
                softmax(sub, 0)
                z(2)
                gate_up(sub, 0)
                score(sub, 2)
                softmax(sub, 1)
                value(sub, 0)
                gate_up(sub, 1)
                softmax(sub, 2)
                value(sub, 1)
                gate_up(sub, 2)
                value(sub, 2)
                if sub == 0:
                    normalize_part(other, x_after_ref, pair)
                    transpose_part(other, kv_after_ref, pair)
                else:
                    epilogue_part(other, pair)
            return carry

        lax.fori_loop(0, n_groups // 2, trip, 0)

    seq_len = len_ref[jnp.minimum(step, n_seqs - 1)]
    n_live = jnp.minimum(pos + 1, (seq_len + t_loc - 1) // t_loc)
    for n_keys in range(1, n_chunks + 1):
        pl.when(jnp.logical_and(n_live == n_keys, step < n_seqs))(functools.partial(run, n_keys))


def run_layer(pos, lengths, x, kv, gain, w_in, w_out, head_dim, micro, next_params=None, prev=None, whole=None):
    n_seqs, t_loc, d_model = x.shape[-3:]

    def after(b):
        return jnp.minimum(b + 1, n_seqs - 1)

    def now(b):
        return jnp.minimum(b, n_seqs - 1)

    def before(b):
        return jnp.maximum(b - 1, 0)

    def x_spec(seq):
        if x.ndim == 4:
            return pl.BlockSpec((None, None) + x.shape[2:], lambda b, *_: (micro, seq(b), 0, 0))
        return pl.BlockSpec((None,) + x.shape[1:], lambda b, *_: (seq(b), 0, 0))

    n_groups, _, in_loc = w_in.shape
    _, n_parts, rows_out, _ = w_out.shape
    n_chunks = kv.shape[0]
    width = kv.shape[3]
    anywhere = pl.BlockSpec(memory_space=pl.ANY)
    in_specs = [
        x_spec(after),
        x_spec(before),
        pl.BlockSpec((n_chunks, None, t_loc, width), lambda b, *_: (0, now(b), 0, 0)),
        pl.BlockSpec((n_chunks, None, t_loc, width), lambda b, *_: (0, after(b), 0, 0)),
        pl.BlockSpec((1, d_model), lambda b, *_: (0, 0)),
        anywhere,
        anywhere,
    ]
    args = [x, x, kv, kv, gain, w_in, w_out]
    if next_params is not None:
        in_specs += [pl.BlockSpec((1, d_model), lambda b, *_: (0, 0)), pl.BlockSpec((d_model, width), lambda b, *_: (0, 0))]
        args += list(next_params)
    aliases = {}
    if prev is not None:
        in_specs.append(anywhere)
        aliases = {2 + len(args): 0}
        args.append(prev)
    if whole is None:
        out_shape = [jax.ShapeDtypeStruct((n_seqs, t_loc, d_model), BF16)]
        out_specs = [pl.BlockSpec((None, t_loc, d_model), lambda b, *_: (before(b), 0, 0))]
    else:
        out_shape = [jax.ShapeDtypeStruct((whole, n_seqs, t_loc, d_model), BF16)]
        out_specs = [pl.BlockSpec((None, None, t_loc, d_model), lambda b, *_: (micro, before(b), 0, 0))]
    if next_params is not None:
        out_shape.append(jax.ShapeDtypeStruct((n_seqs, t_loc, width), BF16))
        out_specs.append(pl.BlockSpec((None, t_loc, width), lambda b, *_: (before(b), 0, 0)))
    rows = n_seqs * t_loc
    heads = (2 * rows_out - in_loc) // head_dim
    flops = 2 * rows * n_groups * d_model * (in_loc + rows_out) + 8 * rows * n_groups * n_chunks * t_loc * (rows_out * 2 - in_loc + rows_out)
    return pl.pallas_call(
        functools.partial(layer_kernel, n_groups, head_dim, next_params is not None, prev is not None),
        grid_spec=pltpu.PrefetchScalarGridSpec(
            num_scalar_prefetch=2,
            grid=(n_seqs + 1,),
            in_specs=in_specs,
            out_specs=out_specs,
            scratch_shapes=[
                pltpu.VMEM((n_groups, d_model, in_loc), BF16),
                pltpu.VMEM((n_groups, rows_out, d_model), BF16),
                pltpu.VMEM((2, t_loc, d_model), BF16),
                pltpu.VMEM((2, 2, head_dim, n_chunks // 2 * t_loc), BF16),
                pltpu.VMEM((2, t_loc, rows_out), BF16),
                pltpu.VMEM((2, t_loc, d_model), F32),
                pltpu.VMEM((heads, n_chunks * t_loc, t_loc), F32),
                pltpu.VMEM((heads, n_chunks * t_loc, t_loc), BF16),
                pltpu.SemaphoreType.DMA((n_groups,)),
                pltpu.SemaphoreType.DMA((n_groups, n_parts)),
            ],
        ),
        out_shape=out_shape,
        input_output_aliases=aliases,
        name="layer",
        compiler_params=pltpu.CompilerParams(dimension_semantics=("arbitrary",), vmem_limit_bytes=60 * 2**20),
        cost_estimate=pl.CostEstimate(flops=flops, bytes_accessed=4 * rows * d_model + 2 * n_groups * d_model * (in_loc + rows_out), transcendentals=0),
    )(pos, lengths, *args)


def solution(mesh):
    n_model = mesh.shape["model"]
    act_spec = P(None, ("part", "data"), "model", None)

    def local_fn(x, lengths, gain_blk, w_in_blk, w_kv_blk, w_out_blk):
        n_micro = x.shape[0]
        n_layers, d_half, in_loc = w_in_blk.shape
        out_loc = w_out_blk.shape[1]
        head_dim = w_kv_blk.shape[2] // 2
        ff_loc = in_loc - out_loc
        heads = (out_loc - ff_loc) // head_dim
        ff_head = ff_loc // heads
        pos = lax.axis_index("model").astype(jnp.int32).reshape(1)

        gain = lax.all_gather(gain_blk, "data", axis=1, tiled=True)
        w_kv = lax.all_gather(w_kv_blk, "data", axis=1, tiled=True)

        cols = w_in_blk.reshape(n_layers, d_half, heads, in_loc // heads)
        w_in_sorted = jnp.concatenate(
            [
                cols[..., head_dim : head_dim + ff_head].reshape(n_layers, d_half, ff_loc),
                cols[..., head_dim + ff_head :].reshape(n_layers, d_half, ff_loc),
                cols[..., :head_dim].reshape(n_layers, d_half, heads * head_dim),
            ],
            axis=-1,
        )
        rows = w_out_blk.reshape(n_layers, heads, out_loc // heads, d_half)
        w_out_sorted = jnp.concatenate(
            [rows[:, :, head_dim:].reshape(n_layers, ff_loc, d_half), rows[:, :, :head_dim].reshape(n_layers, heads * head_dim, d_half)],
            axis=1,
        )

        def weights(layer):
            w_in = lax.all_gather(w_in_sorted[layer], ("model", "data"), axis=0, tiled=False)
            w_out = lax.all_gather(w_out_sorted[layer], ("model", "data"), axis=0, tiled=False)
            return w_in.reshape(n_model, -1, in_loc), w_out.reshape(n_model, -1, out_loc, d_half)

        def gains(layer):
            return gain[layer].reshape(1, -1)

        kv = [
            lax.all_gather(project_kv(x, gains(0), w_kv[0], micro), "model", axis=0, tiled=False) for micro in range(n_micro)
        ]
        hidden = [x] * n_micro
        result = None
        for layer in range(n_layers):
            w_in, w_out = weights(layer)
            last = layer == n_layers - 1
            kv_next = []
            for micro in range(n_micro):
                outs = run_layer(
                    pos, lengths[micro], hidden[micro], kv[micro], gains(layer), w_in, w_out, head_dim, micro,
                    next_params=None if last else (gains(layer + 1), w_kv[layer + 1]),
                    prev=result if last else None,
                    whole=n_micro if last else None,
                )
                if last:
                    result = outs[0]
                else:
                    hidden[micro] = outs[0]
                    kv_next.append(lax.all_gather(outs[1], "model", axis=0, tiled=False))
            kv = kv_next
        return result

    return jax.shard_map(
        local_fn,
        mesh=mesh,
        in_specs=(act_spec, P(None, ("part", "data")), P(None, "data"), P(None, "data", "model"), P(None, "data", None), P(None, "model", "data")),
        out_specs=act_spec,
        check_vma=False,
    )
```

```python
import functools
import jax
import jax.numpy as jnp
from jax import lax
from jax.experimental import pallas as pl
from jax.experimental.pallas import tpu as pltpu
from jax.sharding import PartitionSpec as P

NORM_EPS = 1e-6
NEG_BIG = -1e30
F32 = jnp.float32
BF16 = jnp.bfloat16


def norm_rows(x_act, gain_row):
    x_f32 = x_act.astype(F32)
    centered = x_f32 - jnp.mean(x_f32, axis=-1, keepdims=True)
    variance = jnp.mean(centered * centered, axis=-1, keepdims=True)
    return (centered * lax.rsqrt(variance + NORM_EPS) * gain_row.astype(F32)).astype(BF16)


def kv_kernel(x_ref, gain_ref, w_kv_ref, kv_ref):
    n_seqs, t_loc, d_model = x_ref.shape
    h = norm_rows(x_ref[...].reshape(n_seqs * t_loc, d_model), gain_ref[...])
    kv = jnp.dot(h, w_kv_ref[...], preferred_element_type=F32).astype(BF16)
    kv_ref[...] = kv.reshape(kv_ref.shape)


def project_kv(x, gain, w_kv, micro, block=4):
    _, n_seqs, t_loc, d_model = x.shape
    width = w_kv.shape[1]
    return pl.pallas_call(
        kv_kernel,
        grid=(n_seqs // block,),
        in_specs=[
            pl.BlockSpec((None, block, t_loc, d_model), lambda b: (micro, b, 0, 0)),
            pl.BlockSpec((1, d_model), lambda b: (0, 0)),
            pl.BlockSpec((d_model, width), lambda b: (0, 0)),
        ],
        out_specs=pl.BlockSpec((block, t_loc, width), lambda b: (b, 0, 0)),
        out_shape=jax.ShapeDtypeStruct((n_seqs, t_loc, width), BF16),
        name="kv_proj",
        cost_estimate=pl.CostEstimate(
            flops=2 * n_seqs * t_loc * d_model * width, bytes_accessed=2 * n_seqs * t_loc * (d_model + width), transcendentals=0
        ),
    )(x, gain, w_kv)


def layer_kernel(n_groups, head_dim, has_next, has_prev, *refs):
    refs = list(refs)
    pos_ref, len_ref = refs[:2]
    x_after_ref, x_before_ref, kv_ref, kv_after_ref, gain_ref, w_in_hbm, w_out_hbm = refs[2:9]
    refs = refs[9:]
    if has_next:
        gain_next_ref, w_kv_next_ref = refs[:2]
        refs = refs[2:]
    if has_prev:
        refs = refs[1:]
    y_ref = refs[0]
    refs = refs[1:]
    if has_next:
        kv_next_ref = refs[0]
        refs = refs[1:]
    w_in_ref, w_out_ref, h_ref, vt_ref, joined_ref, acc_ref, s_ref, p_ref, query_ref, in_sem, out_sem = refs

    t_loc, d_model = x_after_ref.shape
    n_chunks = kv_ref.shape[0]
    rows_out = w_out_ref.shape[1]
    half = w_out_hbm.shape[3]
    n_parts = w_out_hbm.shape[1]
    in_loc = w_in_ref.shape[2]
    ff_loc = in_loc - rows_out
    q_loc = rows_out - ff_loc
    heads = q_loc // head_dim
    step = pl.program_id(0)
    n_seqs = pl.num_programs(0) - 1
    tile = 256
    lanes = 128
    rows_part = t_loc // 2

    def in_copy(group):
        return pltpu.make_async_copy(w_in_hbm.at[group], w_in_ref.at[group], in_sem.at[group])

    def out_copy(group, part):
        return pltpu.make_async_copy(
            w_out_hbm.at[group, part], w_out_ref.at[group, :, pl.ds(part * half, half)], out_sem.at[group, part]
        )

    pos = pos_ref[0]
    slot = lax.rem(step, 2)
    other = 1 - slot

    def project_query(src, group, dst):
        q = jnp.dot(h_ref[src], w_in_ref[group, :, 2 * ff_loc :], preferred_element_type=F32).astype(BF16)
        query_ref[dst] = (q * BF16(head_dim**-0.5)).T

    def normalize_part(dst, src_ref, part):
        rows = pl.ds(part * rows_part, rows_part)
        h_ref[dst, rows] = norm_rows(src_ref[rows], gain_ref[...])

    def transpose_part(dst, src_ref, part):
        span = n_chunks // 2
        block = src_ref[pl.ds(part * span, span)].reshape(span * t_loc, 2 * head_dim)
        vt_ref[dst, part] = block.T[head_dim:]

    def epilogue_part(src, part):
        rows = pl.ds(part * rows_part, rows_part)
        y = (x_before_ref[rows].astype(F32) + acc_ref[src, rows]).astype(BF16)
        y_ref[rows] = y
        if has_next:
            h_next = norm_rows(y, gain_next_ref[...])
            kv_next_ref[rows] = jnp.dot(h_next, w_kv_next_ref[...], preferred_element_type=F32).astype(BF16)

    def project_out(joined_slot, group, dst, fresh, col):
        cols = slice(col, col + tile)
        z = jnp.dot(joined_ref[joined_slot], w_out_ref[group, :, cols], preferred_element_type=F32)
        z = z.astype(BF16).astype(F32)
        base = acc_ref[dst, :, cols]
        if fresh is not None:
            base = jnp.where(fresh, 0.0, base)
        acc_ref[dst, :, cols] = base + z

    @pl.when(step == 0)
    def _():
        for group in range(n_groups):
            in_copy(group).start()
            for part in range(n_parts):
                out_copy(n_groups - 1 if group == 0 else group - 1, part).start()
        for part in range(2):
            normalize_part(slot, x_before_ref, part)
            transpose_part(slot, kv_ref, part)
        joined_ref[1] = jnp.zeros_like(joined_ref[1])
        acc_ref[1] = jnp.zeros_like(acc_ref[1])
        in_copy(0).wait()
        project_query(slot, 0, 0)

    @pl.when(step == n_seqs)
    def _():
        for col in range(0, d_model, tile):
            project_out(1, n_groups - 1, other, None, col)
        for part in range(2):
            epilogue_part(other, part)

    def run(n_keys):
        chunk = n_keys - 1
        seq_len = len_ref[jnp.minimum(step, n_seqs - 1)]
        lane = lax.broadcasted_iota(jnp.int32, (1, t_loc), 1)
        limit = jnp.minimum(lane + (pos - chunk) * t_loc, seq_len - chunk * t_loc - 1)
        key = lax.broadcasted_iota(jnp.int32, (t_loc, t_loc), 0)

        def trip(pair, carry):
            first = 2 * pair
            before = lax.rem(first + n_groups - 1, n_groups)

            @pl.when(step == 0)
            def _():
                @pl.when(pair == 0)
                def _():
                    for part in range(n_parts):
                        out_copy(n_groups - 1, part).wait()

                @pl.when(pair != 0)
                def _():
                    for part in range(n_parts):
                        out_copy(before, part).wait()

                in_copy(first + 1).wait()

                @pl.when(pair < n_groups // 2 - 1)
                def _():
                    in_copy(first + 2).wait()

                for part in range(n_parts):
                    out_copy(first, part).wait()

            h = h_ref[slot]
            dst_before = jnp.where(pair == 0, other, slot)
            tops = {}
            sums = {}

            def query(sub):
                if sub == 0:
                    project_query(slot, first + 1, 1)
                else:
                    project_query(jnp.where(pair == n_groups // 2 - 1, other, slot), lax.rem(first + 2, n_groups), 0)

            def gate_up(sub, part):
                for col in range(part * tile, (part + 1) * tile, lanes):
                    both = jnp.dot(h, w_in_ref[first + sub, :, 2 * col : 2 * (col + lanes)], preferred_element_type=F32)
                    both = both.astype(BF16).astype(F32)
                    gate, up = both[:, :lanes], both[:, lanes:]
                    joined_ref[sub, :, col : col + lanes] = (jax.nn.silu(gate) * up).astype(BF16)

            def score(sub, head):
                q_t = query_ref[sub, head * head_dim : (head + 1) * head_dim]
                best = None
                for c in range(n_keys):
                    s = jnp.dot(kv_ref[c, :, :head_dim], q_t, preferred_element_type=F32)
                    if c == chunk:
                        s = jnp.where(key <= limit, s, NEG_BIG)
                    s_ref[head, c * t_loc : (c + 1) * t_loc] = s
                    m = jnp.max(s.reshape(t_loc // 8, 8, t_loc), axis=0)
                    best = m if best is None else jnp.maximum(best, m)
                tops[sub, head] = jnp.max(best, axis=0, keepdims=True)

            def softmax(sub, head):
                total = None
                top = tops[sub, head]
                width = 16
                for r in range(0, n_keys * t_loc, width):
                    e = jnp.exp(s_ref[head, r : r + width] - top)
                    t = jnp.sum(e.reshape(width // 8, 8, t_loc), axis=0)
                    total = t if total is None else total + t
                    p_ref[head, r : r + width] = e.astype(BF16)
                sums[sub, head] = jnp.sum(total, axis=0, keepdims=True)

            outs = {}

            def value(sub, head):
                span = n_chunks // 2 * t_loc
                out_t = None
                for part in range(2):
                    size = min(span, n_keys * t_loc - part * span)
                    if size <= 0:
                        continue
                    o = jnp.dot(vt_ref[slot, part, :, :size], p_ref[head, part * span : part * span + size], preferred_element_type=F32)
                    out_t = o if out_t is None else out_t + o
                outs[sub, head] = (out_t / sums[sub, head]).astype(BF16)
                if head == heads - 1:
                    joined_ref[sub, :, ff_loc:] = jnp.concatenate([outs[sub, i] for i in range(heads)], axis=0).T

            for sub in range(2):
                if sub == 0:
                    z = lambda i: project_out(1, before, dst_before, None, i * tile)
                else:
                    z = lambda i: project_out(0, first, slot, pair == 0, i * tile)
                score(sub, 0)
                z(0)
                score(sub, 1)
                softmax(sub, 0)
                z(1)
                score(sub, 2)
                softmax(sub, 1)
                value(sub, 0)
                z(2)
                gate_up(sub, 0)
                if sub == 0:
                    query(sub)
                    normalize_part(other, x_after_ref, pair)
                    transpose_part(other, kv_after_ref, pair)
                softmax(sub, 2)
                value(sub, 1)
                gate_up(sub, 1)
                if sub == 1:
                    query(sub)
                    epilogue_part(other, pair)
                value(sub, 2)
                gate_up(sub, 2)
            return carry

        lax.fori_loop(0, n_groups // 2, trip, 0)

    seq_len = len_ref[jnp.minimum(step, n_seqs - 1)]
    n_live = jnp.minimum(pos + 1, (seq_len + t_loc - 1) // t_loc)
    for n_keys in range(1, n_chunks + 1):
        pl.when(jnp.logical_and(n_live == n_keys, step < n_seqs))(functools.partial(run, n_keys))


def run_layer(pos, lengths, x, kv, gain, w_in, w_out, head_dim, micro, next_params=None, prev=None, whole=None):
    n_seqs, t_loc, d_model = x.shape[-3:]

    def after(b):
        return jnp.minimum(b + 1, n_seqs - 1)

    def now(b):
        return jnp.minimum(b, n_seqs - 1)

    def before(b):
        return jnp.maximum(b - 1, 0)

    def x_spec(seq):
        if x.ndim == 4:
            return pl.BlockSpec((None, None) + x.shape[2:], lambda b, *_: (micro, seq(b), 0, 0))
        return pl.BlockSpec((None,) + x.shape[1:], lambda b, *_: (seq(b), 0, 0))

    n_groups, _, in_loc = w_in.shape
    _, n_parts, rows_out, _ = w_out.shape
    n_chunks = kv.shape[0]
    width = kv.shape[3]
    anywhere = pl.BlockSpec(memory_space=pl.ANY)
    in_specs = [
        x_spec(after),
        x_spec(before),
        pl.BlockSpec((n_chunks, None, t_loc, width), lambda b, *_: (0, now(b), 0, 0)),
        pl.BlockSpec((n_chunks, None, t_loc, width), lambda b, *_: (0, after(b), 0, 0)),
        pl.BlockSpec((1, d_model), lambda b, *_: (0, 0)),
        anywhere,
        anywhere,
    ]
    args = [x, x, kv, kv, gain, w_in, w_out]
    if next_params is not None:
        in_specs += [pl.BlockSpec((1, d_model), lambda b, *_: (0, 0)), pl.BlockSpec((d_model, width), lambda b, *_: (0, 0))]
        args += list(next_params)
    aliases = {}
    if prev is not None:
        in_specs.append(anywhere)
        aliases = {2 + len(args): 0}
        args.append(prev)
    if whole is None:
        out_shape = [jax.ShapeDtypeStruct((n_seqs, t_loc, d_model), BF16)]
        out_specs = [pl.BlockSpec((None, t_loc, d_model), lambda b, *_: (before(b), 0, 0))]
    else:
        out_shape = [jax.ShapeDtypeStruct((whole, n_seqs, t_loc, d_model), BF16)]
        out_specs = [pl.BlockSpec((None, None, t_loc, d_model), lambda b, *_: (micro, before(b), 0, 0))]
    if next_params is not None:
        out_shape.append(jax.ShapeDtypeStruct((n_seqs, t_loc, width), BF16))
        out_specs.append(pl.BlockSpec((None, t_loc, width), lambda b, *_: (before(b), 0, 0)))
    rows = n_seqs * t_loc
    heads = (2 * rows_out - in_loc) // head_dim
    flops = 2 * rows * n_groups * d_model * (in_loc + rows_out) + 8 * rows * n_groups * n_chunks * t_loc * (rows_out * 2 - in_loc + rows_out)
    return pl.pallas_call(
        functools.partial(layer_kernel, n_groups, head_dim, next_params is not None, prev is not None),
        grid_spec=pltpu.PrefetchScalarGridSpec(
            num_scalar_prefetch=2,
            grid=(n_seqs + 1,),
            in_specs=in_specs,
            out_specs=out_specs,
            scratch_shapes=[
                pltpu.VMEM((n_groups, d_model, in_loc), BF16),
                pltpu.VMEM((n_groups, rows_out, d_model), BF16),
                pltpu.VMEM((2, t_loc, d_model), BF16),
                pltpu.VMEM((2, 2, head_dim, n_chunks // 2 * t_loc), BF16),
                pltpu.VMEM((2, t_loc, rows_out), BF16),
                pltpu.VMEM((2, t_loc, d_model), F32),
                pltpu.VMEM((heads, n_chunks * t_loc, t_loc), F32),
                pltpu.VMEM((heads, n_chunks * t_loc, t_loc), BF16),
                pltpu.VMEM((2, heads * head_dim, t_loc), BF16),
                pltpu.SemaphoreType.DMA((n_groups,)),
                pltpu.SemaphoreType.DMA((n_groups, n_parts)),
            ],
        ),
        out_shape=out_shape,
        input_output_aliases=aliases,
        name="layer",
        compiler_params=pltpu.CompilerParams(dimension_semantics=("arbitrary",), vmem_limit_bytes=60 * 2**20),
        cost_estimate=pl.CostEstimate(flops=flops, bytes_accessed=4 * rows * d_model + 2 * n_groups * d_model * (in_loc + rows_out), transcendentals=0),
    )(pos, lengths, *args)


def solution(mesh):
    n_model = mesh.shape["model"]
    act_spec = P(None, ("part", "data"), "model", None)

    def local_fn(x, lengths, gain_blk, w_in_blk, w_kv_blk, w_out_blk):
        n_micro = x.shape[0]
        n_layers, d_half, in_loc = w_in_blk.shape
        out_loc = w_out_blk.shape[1]
        head_dim = w_kv_blk.shape[2] // 2
        ff_loc = in_loc - out_loc
        heads = (out_loc - ff_loc) // head_dim
        ff_head = ff_loc // heads
        pos = lax.axis_index("model").astype(jnp.int32).reshape(1)

        gain = lax.all_gather(gain_blk, "data", axis=1, tiled=True)
        w_kv = lax.all_gather(w_kv_blk, "data", axis=1, tiled=True)

        lanes = 128
        cols = w_in_blk.reshape(n_layers, d_half, heads, in_loc // heads)
        gate_cols = cols[..., head_dim : head_dim + ff_head].reshape(n_layers, d_half, ff_loc // lanes, 1, lanes)
        up_cols = cols[..., head_dim + ff_head :].reshape(n_layers, d_half, ff_loc // lanes, 1, lanes)
        w_in_sorted = jnp.concatenate(
            [
                jnp.concatenate([gate_cols, up_cols], axis=3).reshape(n_layers, d_half, 2 * ff_loc),
                cols[..., :head_dim].reshape(n_layers, d_half, heads * head_dim),
            ],
            axis=-1,
        )
        rows = w_out_blk.reshape(n_layers, heads, out_loc // heads, d_half)
        w_out_sorted = jnp.concatenate(
            [rows[:, :, head_dim:].reshape(n_layers, ff_loc, d_half), rows[:, :, :head_dim].reshape(n_layers, heads * head_dim, d_half)],
            axis=1,
        )

        def weights(layer):
            w_in = lax.all_gather(w_in_sorted[layer], ("model", "data"), axis=0, tiled=False)
            w_out = lax.all_gather(w_out_sorted[layer], ("model", "data"), axis=0, tiled=False)
            return w_in.reshape(n_model, -1, in_loc), w_out.reshape(n_model, -1, out_loc, d_half)

        def gains(layer):
            return gain[layer].reshape(1, -1)

        kv = [
            lax.all_gather(project_kv(x, gains(0), w_kv[0], micro), "model", axis=0, tiled=False) for micro in range(n_micro)
        ]
        hidden = [x] * n_micro
        result = None
        for layer in range(n_layers):
            w_in, w_out = weights(layer)
            last = layer == n_layers - 1
            kv_next = []
            for micro in range(n_micro):
                outs = run_layer(
                    pos, lengths[micro], hidden[micro], kv[micro], gains(layer), w_in, w_out, head_dim, micro,
                    next_params=None if last else (gains(layer + 1), w_kv[layer + 1]),
                    prev=result if last else None,
                    whole=n_micro if last else None,
                )
                if last:
                    result = outs[0]
                else:
                    hidden[micro] = outs[0]
                    kv_next.append(lax.all_gather(outs[1], "model", axis=0, tiled=False))
            kv = kv_next
        return result

    return jax.shard_map(
        local_fn,
        mesh=mesh,
        in_specs=(act_spec, P(None, ("part", "data")), P(None, "data"), P(None, "data", "model"), P(None, "data", None), P(None, "model", "data")),
        out_specs=act_spec,
        check_vma=False,
    )
```

```python
import functools
import jax
import jax.numpy as jnp
from jax import lax
from jax.experimental import pallas as pl
from jax.experimental.pallas import tpu as pltpu
from jax.sharding import PartitionSpec as P

NORM_EPS = 1e-6
NEG_BIG = -1e30
F32 = jnp.float32
BF16 = jnp.bfloat16
LANES = 128
MESH = pl.DeviceIdType.MESH


def norm_rows(x_act, gain_row):
    x_f32 = x_act.astype(F32)
    centered = x_f32 - jnp.mean(x_f32, axis=-1, keepdims=True)
    variance = jnp.mean(centered * centered, axis=-1, keepdims=True)
    return (centered * lax.rsqrt(variance + NORM_EPS) * gain_row.astype(F32)).astype(BF16)


def sort_kernel(head_dim, in_ref, out_ref, in_sorted_ref, out_sorted_ref):
    in_loc = in_ref.shape[1]
    out_loc = out_ref.shape[0]
    ff_loc = in_loc - out_loc
    heads = (out_loc - ff_loc) // head_dim
    ff_head = ff_loc // heads
    unit_in = in_loc // heads
    unit_out = out_loc // heads
    blocks = ff_head // LANES
    for head in range(heads):
        base = head * unit_in
        for part in range(blocks):
            col = 2 * LANES * (head * blocks + part)
            gate = base + head_dim + part * LANES
            up = gate + ff_head
            in_sorted_ref[:, col : col + LANES] = in_ref[:, gate : gate + LANES]
            in_sorted_ref[:, col + LANES : col + 2 * LANES] = in_ref[:, up : up + LANES]
        row = head * unit_out
        out_sorted_ref[head * ff_head : (head + 1) * ff_head] = out_ref[row + head_dim : row + unit_out]
        out_sorted_ref[ff_loc + head * head_dim : ff_loc + (head + 1) * head_dim] = out_ref[row : row + head_dim]
    in_sorted_ref[:, 2 * ff_loc :] = jnp.concatenate([in_ref[:, h * unit_in : h * unit_in + head_dim] for h in range(heads)], axis=1)


def sort_weights(w_in, w_out, layer, head_dim):
    def spec(a):
        return pl.BlockSpec((None,) + a.shape[1:], lambda i: (layer, 0, 0))

    def out_spec(a):
        return pl.BlockSpec(a.shape[1:], lambda i: (0, 0))

    return pl.pallas_call(
        functools.partial(sort_kernel, head_dim),
        grid=(1,),
        in_specs=[spec(w_in), spec(w_out)],
        out_specs=[out_spec(w_in), out_spec(w_out)],
        out_shape=[jax.ShapeDtypeStruct(w_in.shape[1:], BF16), jax.ShapeDtypeStruct(w_out.shape[1:], BF16)],
        name="sort_weights",
        cost_estimate=pl.CostEstimate(flops=10**6, bytes_accessed=4 * (w_in[0].size + w_out[0].size), transcendentals=0),
    )(w_in, w_out)


def startup_kernel(
    x_hbm, gain_ref, w_kv_ref, w_in_ref, w_out_ref,
    w_in_hbm, w_out_hbm, kv_hbm, gain_out_ref, w_kv_out_ref,
    in_buf, out_buf, kv_buf, gain_buf, w_kv_buf, x_buf,
    own_send, own_recv, fwd_send, fwd_recv, small_send, small_recv,
    kv_send, kv_recv, x_sem, store_sem, kv_store_sem,
):
    data = lax.axis_index("data")
    model = lax.axis_index("model")
    n_layers, d_half, width = w_kv_ref.shape
    n_micro, n_seqs, t_loc, d_model = x_hbm.shape
    block = x_buf.shape[1]
    per_micro = n_seqs // block
    n_blocks = n_micro * per_micro

    chip = model // 2
    core = model % 2
    mate = 2 * chip + 1 - core
    across = 2 * (1 - chip) + core
    across_mate = 2 * (1 - chip) + 1 - core
    flip = 1 - data
    to_mate = {"model": mate}
    to_x = {"model": across}
    to_y = {"data": flip}

    barrier = pltpu.get_barrier_semaphore()
    for peer in (to_mate, to_x, to_y):
        pl.semaphore_signal(barrier, inc=1, device_id=peer, device_id_type=MESH)
    pl.semaphore_wait(barrier, 3)

    def remote(src, dst, send, recv, peer):
        return pltpu.make_async_remote_copy(src_ref=src, dst_ref=dst, send_sem=send, recv_sem=recv, device_id=peer, device_id_type=MESH)

    def place(m, d):
        return 2 * m + d

    me = place(model, data)
    in_rows = d_half // 2
    out_rows = w_out_ref.shape[0] // 2

    def own_item(i):
        if i % 2 == 0:
            return w_in_ref.at[pl.ds(i // 2 * in_rows, in_rows)]
        return w_out_ref.at[pl.ds(i // 2 * out_rows, out_rows)]

    def buf_item(slot, i):
        if i % 2 == 0:
            return in_buf.at[slot, pl.ds(i // 2 * in_rows, in_rows)]
        return out_buf.at[slot, pl.ds(i // 2 * out_rows, out_rows)]

    def hbm_item(slot, i):
        if i % 2 == 0:
            return w_in_hbm.at[slot, pl.ds(i // 2 * in_rows, in_rows)]
        return w_out_hbm.at[slot, pl.ds(i // 2 * out_rows, out_rows)]

    gain_copy = remote(gain_ref, gain_buf.at[data], small_send.at[0], small_recv.at[0], to_y)
    w_kv_copy = remote(w_kv_ref, w_kv_buf.at[data], small_send.at[1], small_recv.at[1], to_y)
    gain_copy.start()
    w_kv_copy.start()

    def x_copy(t):
        return pltpu.make_async_copy(x_hbm.at[t // per_micro, pl.ds(t % per_micro * block, block)], x_buf.at[t % 2], x_sem.at[t % 2])

    x_copy(0).start()

    own = {}
    for i in range(4):
        for k, peer in enumerate((to_y, to_x, to_mate)):
            own[k, i] = remote(own_item(i), buf_item(me, i), own_send.at[k, i], own_recv.at[k, i], peer)
            own[k, i].start()
    stores = []

    def store(slot, i, src):
        copy = pltpu.make_async_copy(src, hbm_item(slot, i), store_sem.at[len(stores)])
        copy.start()
        stores.append(copy)

    for i in range(4):
        store(me, i, own_item(i))

    gain_copy.wait()
    w_kv_copy.wait()
    gain_buf[data] = gain_ref[...]
    w_kv_buf[data] = w_kv_ref[...]
    for layer in range(n_layers):
        for d in range(2):
            gain_out_ref[layer : layer + 1, d * d_half : (d + 1) * d_half] = gain_buf[d, layer : layer + 1]
            w_kv_out_ref[layer, d * d_half : (d + 1) * d_half] = w_kv_buf[d, layer]
    gain = jnp.concatenate([gain_buf[d, 0:1] for d in range(2)], axis=1)
    w_kv = jnp.concatenate([w_kv_buf[d, 0] for d in range(2)], axis=0)

    def kv_place(m, t):
        return kv_buf.at[t, m]

    def kv_copy(k, t, m, peer):
        return remote(kv_place(m, t), kv_place(m, t), kv_send.at[k, t], kv_recv.at[k, t], peer)

    def kv_store(k, t, m):
        return pltpu.make_async_copy(
            kv_place(m, t), kv_hbm.at[t // per_micro, m, pl.ds(t % per_micro * block, block)], kv_store_sem.at[k, t]
        )

    def send_kv(t):
        kv_copy(0, t, model, to_x).start()
        kv_copy(1, t, model, to_mate).start()
        kv_store(0, t, model).start()

    def kv_step(t, carry):
        @pl.when(t + 1 < n_blocks)
        def _():
            x_copy(t + 1).start()

        x_copy(t).wait()
        h = norm_rows(x_buf[t % 2].reshape(block * t_loc, d_model), gain)
        kv = jnp.dot(h, w_kv, preferred_element_type=F32).astype(BF16)
        kv_buf[t, model] = kv.reshape(block, t_loc, width)

        @pl.when(t > 0)
        def _():
            send_kv(t - 1)

        return carry

    lax.fori_loop(0, n_blocks, kv_step, 0)

    forward = {}
    for i in range(4):
        if i == 1:
            send_kv(n_blocks - 1)
        own[1, i].wait_recv()
        slot = place(across, data)
        forward[0, i] = remote(buf_item(slot, i), buf_item(slot, i), fwd_send.at[0, i], fwd_recv.at[0, i], to_y)
        forward[1, i] = remote(buf_item(slot, i), buf_item(slot, i), fwd_send.at[1, i], fwd_recv.at[1, i], to_mate)
        forward[0, i].start()
        forward[1, i].start()
        store(slot, i, buf_item(slot, i))
        own[0, i].wait_recv()
        slot = place(model, flip)
        forward[2, i] = remote(buf_item(slot, i), buf_item(slot, i), fwd_send.at[2, i], fwd_recv.at[2, i], to_mate)
        forward[2, i].start()
        store(slot, i, buf_item(slot, i))
        own[2, i].wait_recv()
        slot = place(mate, data)
        store(slot, i, buf_item(slot, i))

    for i in range(4):
        for t in range(i * n_blocks // 4, (i + 1) * n_blocks // 4):
            kv_copy(0, t, model, to_x).wait_recv()
            kv_copy(2, t, across, to_mate).start()
            kv_store(1, t, across).start()
            kv_copy(1, t, model, to_mate).wait_recv()
            kv_store(2, t, mate).start()
        forward[0, i].wait_recv()
        slot = place(across, flip)
        forward[3, i] = remote(buf_item(slot, i), buf_item(slot, i), fwd_send.at[3, i], fwd_recv.at[3, i], to_mate)
        forward[3, i].start()
        store(slot, i, buf_item(slot, i))
        for k, slot in ((1, place(across_mate, data)), (2, place(mate, flip))):
            forward[k, i].wait_recv()
            store(slot, i, buf_item(slot, i))

    for t in range(n_blocks):
        kv_copy(2, t, across, to_mate).wait_recv()
        kv_store(3, t, across_mate).start()
    for i in range(4):
        forward[3, i].wait_recv()
        slot = place(across_mate, flip)
        store(slot, i, buf_item(slot, i))

    for copy in own.values():
        copy.wait_send()
    for copy in forward.values():
        copy.wait_send()
    for t in range(n_blocks):
        kv_copy(0, t, model, to_x).wait_send()
        kv_copy(1, t, model, to_mate).wait_send()
        kv_copy(2, t, across, to_mate).wait_send()
        for k, m in enumerate((model, across, mate, across_mate)):
            kv_store(k, t, m).wait()
    for copy in stores:
        copy.wait()


def startup(x, gain, w_kv, w_in, w_out, n_model, n_data):
    n_micro, n_seqs, t_loc, d_model = x.shape
    n_layers, d_half, width = w_kv.shape
    _, in_loc = w_in.shape
    out_loc, _ = w_out.shape
    n_all = n_model * n_data
    block = 4
    n_blocks = n_micro * n_seqs // block
    vmem = pl.BlockSpec(memory_space=pltpu.VMEM)
    anywhere = pl.BlockSpec(memory_space=pl.ANY)
    dma = pltpu.SemaphoreType.DMA
    return pl.pallas_call(
        startup_kernel,
        in_specs=[anywhere, vmem, vmem, vmem, vmem],
        out_specs=[anywhere, anywhere, anywhere, vmem, vmem],
        out_shape=[
            jax.ShapeDtypeStruct((n_all, d_half, in_loc), BF16),
            jax.ShapeDtypeStruct((n_all, out_loc, d_half), BF16),
            jax.ShapeDtypeStruct((n_micro, n_model, n_seqs, t_loc, width), BF16),
            jax.ShapeDtypeStruct((n_layers, d_model), F32),
            jax.ShapeDtypeStruct((n_layers, d_model, width), BF16),
        ],
        scratch_shapes=[
            pltpu.VMEM((n_all, d_half, in_loc), BF16),
            pltpu.VMEM((n_all, out_loc, d_half), BF16),
            pltpu.VMEM((n_blocks, n_model, block, t_loc, width), BF16),
            pltpu.VMEM((n_data, n_layers, d_half), F32),
            pltpu.VMEM((n_data, n_layers, d_half, width), BF16),
            pltpu.VMEM((2, block, t_loc, d_model), BF16),
            dma((3, 4)), dma((3, 4)), dma((4, 4)), dma((4, 4)), dma((2,)), dma((2,)),
            dma((3, n_blocks)), dma((3, n_blocks)), dma((2,)), dma((4 * n_all,)), dma((4, n_blocks)),
        ],
        name="startup",
        compiler_params=pltpu.CompilerParams(collective_id=0, has_side_effects=True, vmem_limit_bytes=60 * 2**20),
        cost_estimate=pl.CostEstimate(flops=10**11, bytes_accessed=10**8, transcendentals=0),
    )(x, gain, w_kv, w_in, w_out)


def layer_kernel(n_groups, head_dim, has_next, has_prev, *refs):
    refs = list(refs)
    pos_ref, len_ref = refs[:2]
    x_after_ref, x_before_ref, kv_ref, kv_after_ref, gain_ref, w_in_hbm, w_out_hbm = refs[2:9]
    refs = refs[9:]
    if has_next:
        gain_next_ref, w_kv_next_ref = refs[:2]
        refs = refs[2:]
    if has_prev:
        refs = refs[1:]
    y_ref = refs[0]
    refs = refs[1:]
    if has_next:
        kv_next_ref = refs[0]
        refs = refs[1:]
    w_in_ref, w_out_ref, h_ref, vt_ref, joined_ref, acc_ref, s_ref, p_ref, query_ref, in_sem, out_sem = refs

    t_loc, d_model = x_after_ref.shape
    n_chunks = kv_ref.shape[0]
    rows_out = w_out_ref.shape[1]
    half = w_out_hbm.shape[3]
    n_parts = w_out_hbm.shape[1]
    in_loc = w_in_ref.shape[2]
    ff_loc = in_loc - rows_out
    q_loc = rows_out - ff_loc
    heads = q_loc // head_dim
    step = pl.program_id(0)
    n_seqs = pl.num_programs(0) - 1
    tile = 256
    lanes = LANES
    rows_part = t_loc // 2

    def in_copy(group):
        return pltpu.make_async_copy(w_in_hbm.at[group], w_in_ref.at[group], in_sem.at[group])

    def out_copy(group, part):
        return pltpu.make_async_copy(
            w_out_hbm.at[group, part], w_out_ref.at[group, :, pl.ds(part * half, half)], out_sem.at[group, part]
        )

    pos = pos_ref[0]
    slot = lax.rem(step, 2)
    other = 1 - slot

    def project_query(src, group, dst):
        q = jnp.dot(h_ref[src], w_in_ref[group, :, 2 * ff_loc :], preferred_element_type=F32).astype(BF16)
        query_ref[dst] = (q * BF16(head_dim**-0.5)).T

    def normalize_part(dst, src_ref, part):
        rows = pl.ds(part * rows_part, rows_part)
        h_ref[dst, rows] = norm_rows(src_ref[rows], gain_ref[...])

    def transpose_part(dst, src_ref, part):
        span = n_chunks // 2
        block = src_ref[pl.ds(part * span, span)].reshape(span * t_loc, 2 * head_dim)
        vt_ref[dst, part] = block.T[head_dim:]

    def epilogue_part(src, part):
        rows = pl.ds(part * rows_part, rows_part)
        y = (x_before_ref[rows].astype(F32) + acc_ref[src, rows]).astype(BF16)
        y_ref[rows] = y
        if has_next:
            h_next = norm_rows(y, gain_next_ref[...])
            kv_next_ref[rows] = jnp.dot(h_next, w_kv_next_ref[...], preferred_element_type=F32).astype(BF16)

    def project_out(joined_slot, group, dst, fresh, col):
        cols = slice(col, col + tile)
        z = jnp.dot(joined_ref[joined_slot], w_out_ref[group, :, cols], preferred_element_type=F32)
        z = z.astype(BF16).astype(F32)
        base = acc_ref[dst, :, cols]
        if fresh is not None:
            base = jnp.where(fresh, 0.0, base)
        acc_ref[dst, :, cols] = base + z

    @pl.when(step == 0)
    def _():
        for group in range(n_groups):
            in_copy(group).start()
            for part in range(n_parts):
                out_copy(n_groups - 1 if group == 0 else group - 1, part).start()
        for part in range(2):
            normalize_part(slot, x_before_ref, part)
            transpose_part(slot, kv_ref, part)
        joined_ref[1] = jnp.zeros_like(joined_ref[1])
        acc_ref[1] = jnp.zeros_like(acc_ref[1])
        in_copy(0).wait()
        project_query(slot, 0, 0)

    @pl.when(step == n_seqs)
    def _():
        for col in range(0, d_model, tile):
            project_out(1, n_groups - 1, other, None, col)
        for part in range(2):
            epilogue_part(other, part)

    def run(n_keys):
        chunk = n_keys - 1
        seq_len = len_ref[jnp.minimum(step, n_seqs - 1)]
        lane = lax.broadcasted_iota(jnp.int32, (1, t_loc), 1)
        limit = jnp.minimum(lane + (pos - chunk) * t_loc, seq_len - chunk * t_loc - 1)
        key = lax.broadcasted_iota(jnp.int32, (t_loc, t_loc), 0)

        def trip(pair, carry):
            first = 2 * pair
            before = lax.rem(first + n_groups - 1, n_groups)

            @pl.when(step == 0)
            def _():
                @pl.when(pair == 0)
                def _():
                    for part in range(n_parts):
                        out_copy(n_groups - 1, part).wait()

                @pl.when(pair != 0)
                def _():
                    for part in range(n_parts):
                        out_copy(before, part).wait()

                in_copy(first + 1).wait()

                @pl.when(pair < n_groups // 2 - 1)
                def _():
                    in_copy(first + 2).wait()

                for part in range(n_parts):
                    out_copy(first, part).wait()

            h = h_ref[slot]
            dst_before = jnp.where(pair == 0, other, slot)
            tops = {}
            sums = {}

            def query(sub):
                if sub == 0:
                    project_query(slot, first + 1, 1)
                else:
                    project_query(jnp.where(pair == n_groups // 2 - 1, other, slot), lax.rem(first + 2, n_groups), 0)

            def gate_up(sub, part):
                for col in range(part * tile, (part + 1) * tile, lanes):
                    both = jnp.dot(h, w_in_ref[first + sub, :, 2 * col : 2 * (col + lanes)], preferred_element_type=F32)
                    both = both.astype(BF16).astype(F32)
                    gate, up = both[:, :lanes], both[:, lanes:]
                    joined_ref[sub, :, col : col + lanes] = (jax.nn.silu(gate) * up).astype(BF16)

            def score(sub, head):
                q_t = query_ref[sub, head * head_dim : (head + 1) * head_dim]
                best = None
                for c in range(n_keys):
                    s = jnp.dot(kv_ref[c, :, :head_dim], q_t, preferred_element_type=F32)
                    if c == chunk:
                        s = jnp.where(key <= limit, s, NEG_BIG)
                    s_ref[head, c * t_loc : (c + 1) * t_loc] = s
                    m = jnp.max(s.reshape(t_loc // 8, 8, t_loc), axis=0)
                    best = m if best is None else jnp.maximum(best, m)
                tops[sub, head] = jnp.max(best, axis=0, keepdims=True)

            def softmax(sub, head):
                total = None
                top = tops[sub, head]
                width = 16
                for r in range(0, n_keys * t_loc, width):
                    e = jnp.exp(s_ref[head, r : r + width] - top)
                    t = jnp.sum(e.reshape(width // 8, 8, t_loc), axis=0)
                    total = t if total is None else total + t
                    p_ref[head, r : r + width] = e.astype(BF16)
                sums[sub, head] = jnp.sum(total, axis=0, keepdims=True)

            outs = {}

            def value(sub, head):
                span = n_chunks // 2 * t_loc
                out_t = None
                for part in range(2):
                    size = min(span, n_keys * t_loc - part * span)
                    if size <= 0:
                        continue
                    o = jnp.dot(vt_ref[slot, part, :, :size], p_ref[head, part * span : part * span + size], preferred_element_type=F32)
                    out_t = o if out_t is None else out_t + o
                outs[sub, head] = (out_t / sums[sub, head]).astype(BF16)
                if head == heads - 1:
                    joined_ref[sub, :, ff_loc:] = jnp.concatenate([outs[sub, i] for i in range(heads)], axis=0).T

            for sub in range(2):
                if sub == 0:
                    z = lambda i: project_out(1, before, dst_before, None, i * tile)
                else:
                    z = lambda i: project_out(0, first, slot, pair == 0, i * tile)
                score(sub, 0)
                z(0)
                score(sub, 1)
                softmax(sub, 0)
                z(1)
                score(sub, 2)
                softmax(sub, 1)
                value(sub, 0)
                z(2)
                gate_up(sub, 0)
                if sub == 0:
                    query(sub)
                    normalize_part(other, x_after_ref, pair)
                    transpose_part(other, kv_after_ref, pair)
                softmax(sub, 2)
                value(sub, 1)
                gate_up(sub, 1)
                if sub == 1:
                    query(sub)
                    epilogue_part(other, pair)
                value(sub, 2)
                gate_up(sub, 2)
            return carry

        lax.fori_loop(0, n_groups // 2, trip, 0)

    seq_len = len_ref[jnp.minimum(step, n_seqs - 1)]
    n_live = jnp.minimum(pos + 1, (seq_len + t_loc - 1) // t_loc)
    for n_keys in range(1, n_chunks + 1):
        pl.when(jnp.logical_and(n_live == n_keys, step < n_seqs))(functools.partial(run, n_keys))


def run_layer(pos, lengths, x, kv, gain, w_in, w_out, head_dim, micro, next_params=None, prev=None, whole=None):
    n_seqs, t_loc, d_model = x.shape[-3:]

    def after(b):
        return jnp.minimum(b + 1, n_seqs - 1)

    def now(b):
        return jnp.minimum(b, n_seqs - 1)

    def before(b):
        return jnp.maximum(b - 1, 0)

    def x_spec(seq):
        if x.ndim == 4:
            return pl.BlockSpec((None, None) + x.shape[2:], lambda b, *_: (micro, seq(b), 0, 0))
        return pl.BlockSpec((None,) + x.shape[1:], lambda b, *_: (seq(b), 0, 0))

    n_groups, _, in_loc = w_in.shape
    _, n_parts, rows_out, _ = w_out.shape
    n_chunks = kv.shape[-4]
    width = kv.shape[-1]

    def kv_spec(seq):
        if kv.ndim == 5:
            return pl.BlockSpec((None, n_chunks, None, t_loc, width), lambda b, *_: (micro, 0, seq(b), 0, 0))
        return pl.BlockSpec((n_chunks, None, t_loc, width), lambda b, *_: (0, seq(b), 0, 0))

    anywhere = pl.BlockSpec(memory_space=pl.ANY)
    in_specs = [
        x_spec(after),
        x_spec(before),
        kv_spec(now),
        kv_spec(after),
        pl.BlockSpec((1, d_model), lambda b, *_: (0, 0)),
        anywhere,
        anywhere,
    ]
    args = [x, x, kv, kv, gain, w_in, w_out]
    if next_params is not None:
        in_specs += [pl.BlockSpec((1, d_model), lambda b, *_: (0, 0)), pl.BlockSpec((d_model, width), lambda b, *_: (0, 0))]
        args += list(next_params)
    aliases = {}
    if prev is not None:
        in_specs.append(anywhere)
        aliases = {2 + len(args): 0}
        args.append(prev)
    if whole is None:
        out_shape = [jax.ShapeDtypeStruct((n_seqs, t_loc, d_model), BF16)]
        out_specs = [pl.BlockSpec((None, t_loc, d_model), lambda b, *_: (before(b), 0, 0))]
    else:
        out_shape = [jax.ShapeDtypeStruct((whole, n_seqs, t_loc, d_model), BF16)]
        out_specs = [pl.BlockSpec((None, None, t_loc, d_model), lambda b, *_: (micro, before(b), 0, 0))]
    if next_params is not None:
        out_shape.append(jax.ShapeDtypeStruct((n_seqs, t_loc, width), BF16))
        out_specs.append(pl.BlockSpec((None, t_loc, width), lambda b, *_: (before(b), 0, 0)))
    rows = n_seqs * t_loc
    heads = (2 * rows_out - in_loc) // head_dim
    flops = 2 * rows * n_groups * d_model * (in_loc + rows_out) + 8 * rows * n_groups * n_chunks * t_loc * (rows_out * 2 - in_loc + rows_out)
    return pl.pallas_call(
        functools.partial(layer_kernel, n_groups, head_dim, next_params is not None, prev is not None),
        grid_spec=pltpu.PrefetchScalarGridSpec(
            num_scalar_prefetch=2,
            grid=(n_seqs + 1,),
            in_specs=in_specs,
            out_specs=out_specs,
            scratch_shapes=[
                pltpu.VMEM((n_groups, d_model, in_loc), BF16),
                pltpu.VMEM((n_groups, rows_out, d_model), BF16),
                pltpu.VMEM((2, t_loc, d_model), BF16),
                pltpu.VMEM((2, 2, head_dim, n_chunks // 2 * t_loc), BF16),
                pltpu.VMEM((2, t_loc, rows_out), BF16),
                pltpu.VMEM((2, t_loc, d_model), F32),
                pltpu.VMEM((heads, n_chunks * t_loc, t_loc), F32),
                pltpu.VMEM((heads, n_chunks * t_loc, t_loc), BF16),
                pltpu.VMEM((2, heads * head_dim, t_loc), BF16),
                pltpu.SemaphoreType.DMA((n_groups,)),
                pltpu.SemaphoreType.DMA((n_groups, n_parts)),
            ],
        ),
        out_shape=out_shape,
        input_output_aliases=aliases,
        name="layer",
        compiler_params=pltpu.CompilerParams(dimension_semantics=("arbitrary",), vmem_limit_bytes=60 * 2**20),
        cost_estimate=pl.CostEstimate(flops=flops, bytes_accessed=4 * rows * d_model + 2 * n_groups * d_model * (in_loc + rows_out), transcendentals=0),
    )(pos, lengths, *args)


def solution(mesh):
    n_model = mesh.shape["model"]
    n_data = mesh.shape["data"]
    act_spec = P(None, ("part", "data"), "model", None)

    def local_fn(x, lengths, gain_blk, w_in_blk, w_kv_blk, w_out_blk):
        n_micro = x.shape[0]
        n_layers, d_half, in_loc = w_in_blk.shape
        out_loc = w_out_blk.shape[1]
        head_dim = w_kv_blk.shape[2] // 2
        pos = lax.axis_index("model").astype(jnp.int32).reshape(1)

        w_in_own, w_out_own = sort_weights(w_in_blk, w_out_blk, 0, head_dim)
        w_in_all, w_out_all, kv_all, gain, w_kv = startup(x, gain_blk.astype(F32), w_kv_blk, w_in_own, w_out_own, n_model, n_data)
        params = [(w_in_all, w_out_all)]
        for layer in range(1, n_layers):
            own = lax.optimization_barrier((sort_weights(w_in_blk, w_out_blk, layer, head_dim), kv_all))[0]
            params.append([lax.all_gather(w, ("model", "data"), axis=0, tiled=False) for w in own])

        def weights(layer):
            w_in, w_out = params[layer]
            return w_in.reshape(n_model, -1, in_loc), w_out.reshape(n_model, n_data, out_loc, d_half)

        def gains(layer):
            return gain[layer].reshape(1, -1)

        kv = [kv_all] * n_micro
        hidden = [x] * n_micro
        result = None
        for layer in range(n_layers):
            w_in, w_out = weights(layer)
            last = layer == n_layers - 1
            kv_next = []
            for micro in range(n_micro):
                outs = run_layer(
                    pos, lengths[micro], hidden[micro], kv[micro], gains(layer), w_in, w_out, head_dim, micro,
                    next_params=None if last else (gains(layer + 1), w_kv[layer + 1]),
                    prev=result if last else None,
                    whole=n_micro if last else None,
                )
                if last:
                    result = outs[0]
                else:
                    hidden[micro] = outs[0]
                    kv_next.append(lax.all_gather(outs[1], "model", axis=0, tiled=False))
            kv = kv_next
        return result

    return jax.shard_map(
        local_fn,
        mesh=mesh,
        in_specs=(act_spec, P(None, ("part", "data")), P(None, "data"), P(None, "data", "model"), P(None, "data", None), P(None, "model", "data")),
        out_specs=act_spec,
        check_vma=False,
    )
```

```python
import functools
import jax
import jax.numpy as jnp
from jax import lax
from jax.experimental import pallas as pl
from jax.experimental.pallas import tpu as pltpu
from jax.sharding import PartitionSpec as P

NORM_EPS = 1e-6
NEG_BIG = -1e30
F32 = jnp.float32
BF16 = jnp.bfloat16
LANES = 128
MESH = pl.DeviceIdType.MESH


def norm_rows(x_act, gain_row):
    x_f32 = x_act.astype(F32)
    centered = x_f32 - jnp.mean(x_f32, axis=-1, keepdims=True)
    variance = jnp.mean(centered * centered, axis=-1, keepdims=True)
    return (centered * lax.rsqrt(variance + NORM_EPS) * gain_row.astype(F32)).astype(BF16)


def sort_kernel(head_dim, in_ref, out_ref, *sorted_refs):
    n_layers, in_loc, _ = in_ref.shape
    out_loc = out_ref.shape[1]
    ff_loc = in_loc - out_loc
    heads = (out_loc - ff_loc) // head_dim
    ff_head = ff_loc // heads
    unit_in = in_loc // heads
    unit_out = out_loc // heads
    blocks = ff_head // LANES
    for layer in range(n_layers):
        in_sorted_ref, out_sorted_ref = sorted_refs[2 * layer : 2 * layer + 2]
        for head in range(heads):
            base = head * unit_in
            for part in range(blocks):
                col = 2 * LANES * (head * blocks + part)
                gate = base + head_dim + part * LANES
                up = gate + ff_head
                in_sorted_ref[:, col : col + LANES] = in_ref[layer, gate : gate + LANES].T
                in_sorted_ref[:, col + LANES : col + 2 * LANES] = in_ref[layer, up : up + LANES].T
            row = head * unit_out
            out_sorted_ref[head * ff_head : (head + 1) * ff_head] = out_ref[layer, row + head_dim : row + unit_out]
            out_sorted_ref[ff_loc + head * head_dim : ff_loc + (head + 1) * head_dim] = out_ref[layer, row : row + head_dim]
        queries = jnp.concatenate([in_ref[layer, h * unit_in : h * unit_in + head_dim] for h in range(heads)], axis=0)
        in_sorted_ref[:, 2 * ff_loc :] = queries.T


def sort_weights(w_in, w_out, head_dim):
    n_layers, d_half, in_loc = w_in.shape
    vmem = pl.BlockSpec(memory_space=pltpu.VMEM)
    outs = [jax.ShapeDtypeStruct(w_in.shape[1:], BF16), jax.ShapeDtypeStruct(w_out.shape[1:], BF16)] * n_layers
    outs = pl.pallas_call(
        functools.partial(sort_kernel, head_dim),
        in_specs=[vmem, vmem],
        out_specs=[vmem] * len(outs),
        out_shape=outs,
        name="sort_weights",
        cost_estimate=pl.CostEstimate(flops=10**6, bytes_accessed=4 * (w_in.size + w_out.size), transcendentals=0),
    )(jnp.swapaxes(w_in, 1, 2), w_out)
    return [outs[2 * layer : 2 * layer + 2] for layer in range(n_layers)]


def startup_kernel(
    n_layers, x_hbm, gain_ref, w_kv_ref, w_in_ref, w_out_ref, w_in_hbm, w_out_hbm, kv_hbm, kv_rest_hbm, *refs
):
    gain_out_refs, w_kv_out_refs = refs[:n_layers], refs[n_layers : 2 * n_layers]
    (
    in_buf, out_buf, kv_buf, gain_buf, w_kv_buf, x_buf,
    own_send, own_recv, fwd_send, fwd_recv, small_send, small_recv,
    kv_send, kv_recv, x_sem, store_sem, kv_store_sem, kv_rest_sem,
    ) = refs[2 * n_layers :]
    data = lax.axis_index("data")
    model = lax.axis_index("model")
    _, d_half, width = w_kv_ref.shape
    n_micro, n_seqs, t_loc, d_model = x_hbm.shape
    block = x_buf.shape[1]
    per_micro = n_seqs // block
    n_blocks = n_micro * per_micro

    chip = model // 2
    core = model % 2
    mate = 2 * chip + 1 - core
    across = 2 * (1 - chip) + core
    across_mate = 2 * (1 - chip) + 1 - core
    flip = 1 - data
    to_mate = {"model": mate}
    to_x = {"model": across}
    to_y = {"data": flip}

    barrier = pltpu.get_barrier_semaphore()
    for peer in (to_mate, to_x, to_y):
        pl.semaphore_signal(barrier, inc=1, device_id=peer, device_id_type=MESH)
    pl.semaphore_wait(barrier, 3)

    def remote(src, dst, send, recv, peer):
        return pltpu.make_async_remote_copy(src_ref=src, dst_ref=dst, send_sem=send, recv_sem=recv, device_id=peer, device_id_type=MESH)

    def place(m, d):
        return 2 * m + d

    me = place(model, data)
    in_rows = d_half // 2
    out_rows = w_out_ref.shape[0] // 2

    def own_item(i):
        if i % 2 == 0:
            return w_in_ref.at[pl.ds(i // 2 * in_rows, in_rows)]
        return w_out_ref.at[pl.ds(i // 2 * out_rows, out_rows)]

    def buf_item(slot, i):
        if i % 2 == 0:
            return in_buf.at[slot, pl.ds(i // 2 * in_rows, in_rows)]
        return out_buf.at[slot, pl.ds(i // 2 * out_rows, out_rows)]

    def hbm_item(slot, i):
        if i % 2 == 0:
            return w_in_hbm.at[slot, pl.ds(i // 2 * in_rows, in_rows)]
        return w_out_hbm.at[slot, pl.ds(i // 2 * out_rows, out_rows)]

    gain_copy = remote(gain_ref, gain_buf.at[data], small_send.at[0], small_recv.at[0], to_y)
    w_kv_copy = remote(w_kv_ref, w_kv_buf.at[data], small_send.at[1], small_recv.at[1], to_y)
    gain_copy.start()
    w_kv_copy.start()

    def x_copy(t):
        return pltpu.make_async_copy(x_hbm.at[t // per_micro, pl.ds(t % per_micro * block, block)], x_buf.at[t % 2], x_sem.at[t % 2])

    x_copy(0).start()

    own = {}
    for i in range(4):
        for k, peer in enumerate((to_y, to_x, to_mate)):
            own[k, i] = remote(own_item(i), buf_item(me, i), own_send.at[k, i], own_recv.at[k, i], peer)
            own[k, i].start()
    stores = []

    def store(slot, i, src):
        copy = pltpu.make_async_copy(src, hbm_item(slot, i), store_sem.at[len(stores)])
        copy.start()
        stores.append(copy)

    for i in range(4):
        store(me, i, own_item(i))

    gain_copy.wait()
    w_kv_copy.wait()
    gain_buf[data] = gain_ref[...]
    w_kv_buf[data] = w_kv_ref[...]
    for layer in range(n_layers):
        for d in range(2):
            gain_out_refs[layer][:, d * d_half : (d + 1) * d_half] = gain_buf[d, layer : layer + 1]
            w_kv_out_refs[layer][d * d_half : (d + 1) * d_half] = w_kv_buf[d, layer]
    gain = jnp.concatenate([gain_buf[d, 0:1] for d in range(2)], axis=1)
    w_kv = jnp.concatenate([w_kv_buf[d, 0] for d in range(2)], axis=0)

    def kv_place(m, t):
        return kv_buf.at[t, m]

    def kv_copy(k, t, m, peer):
        return remote(kv_place(m, t), kv_place(m, t), kv_send.at[k, t], kv_recv.at[k, t], peer)

    def kv_store(k, t, m):
        return pltpu.make_async_copy(kv_place(m, t), kv_hbm.at[m, pl.ds(t * block, block)], kv_store_sem.at[k, t])

    def kv_rest_store(t):
        rest = t - per_micro
        return pltpu.make_async_copy(
            kv_place(model, t), kv_rest_hbm.at[rest // per_micro, pl.ds(rest % per_micro * block, block)], kv_rest_sem.at[rest]
        )

    def send_kv(t):
        kv_copy(0, t, model, to_x).start()
        kv_copy(1, t, model, to_mate).start()
        kv_store(0, t, model).start()

    def kv_step(t, carry):
        @pl.when(t + 1 < n_blocks)
        def _():
            x_copy(t + 1).start()

        x_copy(t).wait()
        h = norm_rows(x_buf[t % 2].reshape(block * t_loc, d_model), gain)
        kv = jnp.dot(h, w_kv, preferred_element_type=F32).astype(BF16)
        kv_buf[t, model] = kv.reshape(block, t_loc, width)

        @pl.when(jnp.logical_and(t > 0, t <= per_micro))
        def _():
            send_kv(t - 1)

        @pl.when(t > per_micro)
        def _():
            kv_rest_store(t - 1).start()

        return carry

    lax.fori_loop(0, n_blocks, kv_step, 0)

    kv_rest_store(n_blocks - 1).start()

    forward = {}
    for i in range(4):
        own[1, i].wait_recv()
        slot = place(across, data)
        if i < 3:
            forward[0, i] = remote(buf_item(slot, i), buf_item(slot, i), fwd_send.at[0, i], fwd_recv.at[0, i], to_y)
            forward[0, i].start()
        forward[1, i] = remote(buf_item(slot, i), buf_item(slot, i), fwd_send.at[1, i], fwd_recv.at[1, i], to_mate)
        forward[1, i].start()
        store(slot, i, buf_item(slot, i))
        own[0, i].wait_recv()
        slot = place(model, flip)
        if i == 3:
            forward[0, i] = remote(buf_item(slot, i), buf_item(slot, i), fwd_send.at[0, i], fwd_recv.at[0, i], to_x)
            forward[0, i].start()
        forward[2, i] = remote(buf_item(slot, i), buf_item(slot, i), fwd_send.at[2, i], fwd_recv.at[2, i], to_mate)
        forward[2, i].start()
        store(slot, i, buf_item(slot, i))
        own[2, i].wait_recv()
        slot = place(mate, data)
        store(slot, i, buf_item(slot, i))

    for i in range(4):
        for t in range(i * per_micro // 4, (i + 1) * per_micro // 4):
            kv_copy(0, t, model, to_x).wait_recv()
            kv_copy(2, t, across, to_mate).start()
            kv_store(1, t, across).start()
            kv_copy(1, t, model, to_mate).wait_recv()
            kv_store(2, t, mate).start()
        forward[0, i].wait_recv()
        slot = place(across, flip)
        forward[3, i] = remote(buf_item(slot, i), buf_item(slot, i), fwd_send.at[3, i], fwd_recv.at[3, i], to_mate)
        forward[3, i].start()
        store(slot, i, buf_item(slot, i))
        for k, slot in ((1, place(across_mate, data)), (2, place(mate, flip))):
            forward[k, i].wait_recv()
            store(slot, i, buf_item(slot, i))

    for t in range(per_micro):
        kv_copy(2, t, across, to_mate).wait_recv()
        kv_store(3, t, across_mate).start()
    for i in range(4):
        forward[3, i].wait_recv()
        slot = place(across_mate, flip)
        store(slot, i, buf_item(slot, i))

    for copy in own.values():
        copy.wait_send()
    for copy in forward.values():
        copy.wait_send()
    for t in range(per_micro, n_blocks):
        kv_rest_store(t).wait()
    for t in range(per_micro):
        kv_copy(0, t, model, to_x).wait_send()
        kv_copy(1, t, model, to_mate).wait_send()
        kv_copy(2, t, across, to_mate).wait_send()
        for k, m in enumerate((model, across, mate, across_mate)):
            kv_store(k, t, m).wait()
    for copy in stores:
        copy.wait()


def startup(x, gain, w_kv, w_in, w_out, n_model, n_data):
    n_micro, n_seqs, t_loc, d_model = x.shape
    n_layers, d_half, width = w_kv.shape
    _, in_loc = w_in.shape
    out_loc, _ = w_out.shape
    n_all = n_model * n_data
    block = 4
    n_blocks = n_micro * n_seqs // block
    vmem = pl.BlockSpec(memory_space=pltpu.VMEM)
    anywhere = pl.BlockSpec(memory_space=pl.ANY)
    dma = pltpu.SemaphoreType.DMA
    per_micro = n_seqs // block
    outs = pl.pallas_call(
        functools.partial(startup_kernel, n_layers),
        in_specs=[anywhere, vmem, vmem, vmem, vmem],
        out_specs=[anywhere] * 4 + [vmem] * (2 * n_layers),
        out_shape=[
            jax.ShapeDtypeStruct((n_all, d_half, in_loc), BF16),
            jax.ShapeDtypeStruct((n_all, out_loc, d_half), BF16),
            jax.ShapeDtypeStruct((n_model, n_seqs, t_loc, width), BF16),
            jax.ShapeDtypeStruct((n_micro - 1, n_seqs, t_loc, width), BF16),
        ]
        + [jax.ShapeDtypeStruct((1, d_model), BF16)] * n_layers
        + [jax.ShapeDtypeStruct((d_model, width), BF16)] * n_layers,
        scratch_shapes=[
            pltpu.VMEM((n_all, d_half, in_loc), BF16),
            pltpu.VMEM((n_all, out_loc, d_half), BF16),
            pltpu.VMEM((n_blocks, n_model, block, t_loc, width), BF16),
            pltpu.VMEM((n_data, n_layers, d_half), BF16),
            pltpu.VMEM((n_data, n_layers, d_half, width), BF16),
            pltpu.VMEM((2, block, t_loc, d_model), BF16),
            dma((3, 4)), dma((3, 4)), dma((4, 4)), dma((4, 4)), dma((2,)), dma((2,)),
            dma((3, per_micro)), dma((3, per_micro)), dma((2,)), dma((4 * n_all,)), dma((4, per_micro)), dma((n_blocks - per_micro,)),
        ],
        name="startup",
        compiler_params=pltpu.CompilerParams(collective_id=0, has_side_effects=True, vmem_limit_bytes=60 * 2**20),
        cost_estimate=pl.CostEstimate(flops=10**11, bytes_accessed=10**8, transcendentals=0),
    )(x, gain, w_kv, w_in, w_out)
    return outs[:4], outs[4 : 4 + n_layers], outs[4 + n_layers :]


def layer_kernel(micro, n_groups, head_dim, has_next, has_prev, *refs):
    refs = list(refs)
    pos_ref, len_ref = refs[:2]
    x_after_ref, x_before_ref, kv_ref, kv_after_ref, gain_ref, w_in_hbm, w_out_hbm = refs[2:9]
    refs = refs[9:]
    if has_next:
        gain_next_ref, w_kv_next_ref = refs[:2]
        refs = refs[2:]
    if has_prev:
        refs = refs[1:]
    y_ref = refs[0]
    refs = refs[1:]
    if has_next:
        kv_next_ref = refs[0]
        refs = refs[1:]
    w_in_ref, w_out_ref, h_ref, vt_ref, joined_ref, acc_ref, s_ref, p_ref, query_ref, in_sem, out_sem = refs

    t_loc, d_model = x_after_ref.shape
    n_chunks = kv_ref.shape[0]
    rows_out = w_out_ref.shape[1]
    half = w_out_hbm.shape[3]
    n_parts = w_out_hbm.shape[1]
    in_loc = w_in_ref.shape[2]
    ff_loc = in_loc - rows_out
    q_loc = rows_out - ff_loc
    heads = q_loc // head_dim
    step = pl.program_id(0)
    n_seqs = pl.num_programs(0) - 1
    tile = 256
    lanes = LANES
    rows_part = t_loc // 2

    def query_copy(group):
        cols = pl.ds(2 * ff_loc, q_loc)
        return pltpu.make_async_copy(w_in_hbm.at[group, :, cols], w_in_ref.at[group, :, cols], in_sem.at[0, group])

    def in_copy(group):
        cols = pl.ds(0, 2 * ff_loc)
        return pltpu.make_async_copy(w_in_hbm.at[group, :, cols], w_in_ref.at[group, :, cols], in_sem.at[1, group])

    def out_copy(group, part):
        return pltpu.make_async_copy(
            w_out_hbm.at[group, part], w_out_ref.at[group, :, pl.ds(part * half, half)], out_sem.at[group, part]
        )

    def copies(*groups):
        return [in_copy(group) for group in groups] + [out_copy(group, part) for group in groups for part in range(n_parts)]

    pos = pos_ref[0]
    slot = lax.rem(step, 2)
    other = 1 - slot

    def project_query(src, group, dst):
        q = jnp.dot(h_ref[src], w_in_ref[group, :, 2 * ff_loc :], preferred_element_type=F32).astype(BF16)
        query_ref[dst] = (q * BF16(head_dim**-0.5)).T

    def normalize_part(dst, src_ref, part):
        rows = pl.ds(part * rows_part, rows_part)
        h_ref[dst, rows] = norm_rows(src_ref[rows], gain_ref[...])

    def transpose_part(dst, src_ref, part):
        span = n_chunks // 2
        block = src_ref[pl.ds(part * span, span)].reshape(span * t_loc, 2 * head_dim)
        vt_ref[dst, part] = block.T[head_dim:]

    def epilogue_part(src, part):
        rows = pl.ds(part * rows_part, rows_part)
        y = (x_before_ref[rows].astype(F32) + acc_ref[src, rows]).astype(BF16)
        y_ref[rows] = y
        if has_next:
            h_next = norm_rows(y, gain_next_ref[...])
            kv_next_ref[rows] = jnp.dot(h_next, w_kv_next_ref[...], preferred_element_type=F32).astype(BF16)

    def project_out(joined_slot, group, dst, fresh, col):
        cols = slice(col, col + tile)
        z = jnp.dot(joined_ref[joined_slot], w_out_ref[group, :, cols], preferred_element_type=F32)
        z = z.astype(BF16).astype(F32)
        base = acc_ref[dst, :, cols]
        if fresh is not None:
            base = jnp.where(fresh, 0.0, base)
        acc_ref[dst, :, cols] = base + z

    @pl.when(step == 0)
    def _():
        for group in range(n_groups):
            query_copy(group).start()
        for copy in [in_copy(0)] + [out_copy(0, part) for part in range(n_parts)] + [in_copy(1)]:
            copy.start()
        for part in range(2):
            normalize_part(slot, x_before_ref, part)
            transpose_part(slot, kv_ref, part)
        joined_ref[1] = jnp.zeros_like(joined_ref[1])
        acc_ref[1] = jnp.zeros_like(acc_ref[1])
        for group in range(n_groups):
            query_copy(group).wait()
        project_query(slot, 0, 0)

    @pl.when(step == n_seqs)
    def _():
        for col in range(0, d_model, tile):
            project_out(1, n_groups - 1, other, None, col)
        for part in range(2):
            epilogue_part(other, part)

    def run(n_keys):
        chunk = n_keys - 1
        seq_len = len_ref[micro, jnp.minimum(step, n_seqs - 1)]
        lane = lax.broadcasted_iota(jnp.int32, (1, t_loc), 1)
        limit = jnp.minimum(lane + (pos - chunk) * t_loc, seq_len - chunk * t_loc - 1)
        key = lax.broadcasted_iota(jnp.int32, (t_loc, t_loc), 0)

        def trip(pair, carry):
            first = 2 * pair
            before = jnp.where(jnp.logical_and(step == 0, pair == 0), 0, lax.rem(first + n_groups - 1, n_groups))

            @pl.when(step == 0)
            def _():
                early = [in_copy(0)] + [out_copy(0, part) for part in range(n_parts)] + [in_copy(1)]
                late = [out_copy(1, part) for part in range(n_parts)] + copies(*range(2, n_groups))

                @pl.when(pair == 0)
                def _():
                    for copy in early:
                        copy.wait()
                    for copy in late:
                        copy.start()

                @pl.when(pair == 1)
                def _():
                    for copy in late:
                        copy.wait()

            h = h_ref[slot]
            dst_before = jnp.where(pair == 0, other, slot)
            tops = {}
            sums = {}

            def query(sub):
                if sub == 0:
                    project_query(slot, first + 1, 1)
                else:
                    project_query(jnp.where(pair == n_groups // 2 - 1, other, slot), lax.rem(first + 2, n_groups), 0)

            def gate_up(sub, part):
                for col in range(part * tile, (part + 1) * tile, lanes):
                    both = jnp.dot(h, w_in_ref[first + sub, :, 2 * col : 2 * (col + lanes)], preferred_element_type=F32)
                    both = both.astype(BF16).astype(F32)
                    gate, up = both[:, :lanes], both[:, lanes:]
                    joined_ref[sub, :, col : col + lanes] = (jax.nn.silu(gate) * up).astype(BF16)

            def score(sub, head):
                q_t = query_ref[sub, head * head_dim : (head + 1) * head_dim]
                best = None
                for c in range(n_keys):
                    s = jnp.dot(kv_ref[c, :, :head_dim], q_t, preferred_element_type=F32)
                    if c == chunk:
                        s = jnp.where(key <= limit, s, NEG_BIG)
                    s_ref[head, c * t_loc : (c + 1) * t_loc] = s
                    m = jnp.max(s.reshape(t_loc // 8, 8, t_loc), axis=0)
                    best = m if best is None else jnp.maximum(best, m)
                tops[sub, head] = jnp.max(best, axis=0, keepdims=True)

            def softmax(sub, head):
                total = None
                top = tops[sub, head]
                width = 16
                for r in range(0, n_keys * t_loc, width):
                    e = jnp.exp(s_ref[head, r : r + width] - top)
                    t = jnp.sum(e.reshape(width // 8, 8, t_loc), axis=0)
                    total = t if total is None else total + t
                    p_ref[head, r : r + width] = e.astype(BF16)
                sums[sub, head] = jnp.sum(total, axis=0, keepdims=True)

            outs = {}

            def value(sub, head):
                span = n_chunks // 2 * t_loc
                out_t = None
                for part in range(2):
                    size = min(span, n_keys * t_loc - part * span)
                    if size <= 0:
                        continue
                    o = jnp.dot(vt_ref[slot, part, :, :size], p_ref[head, part * span : part * span + size], preferred_element_type=F32)
                    out_t = o if out_t is None else out_t + o
                outs[sub, head] = (out_t / sums[sub, head]).astype(BF16)
                if head == heads - 1:
                    joined_ref[sub, :, ff_loc:] = jnp.concatenate([outs[sub, i] for i in range(heads)], axis=0).T

            for sub in range(2):
                if sub == 0:
                    z = lambda i: project_out(1, before, dst_before, None, i * tile)
                else:
                    z = lambda i: project_out(0, first, slot, pair == 0, i * tile)
                score(sub, 0)
                z(0)
                score(sub, 1)
                softmax(sub, 0)
                z(1)
                score(sub, 2)
                softmax(sub, 1)
                value(sub, 0)
                z(2)
                gate_up(sub, 0)
                if sub == 0:
                    query(sub)
                    normalize_part(other, x_after_ref, pair)
                    transpose_part(other, kv_after_ref, pair)
                softmax(sub, 2)
                value(sub, 1)
                gate_up(sub, 1)
                if sub == 1:
                    query(sub)
                    epilogue_part(other, pair)
                value(sub, 2)
                gate_up(sub, 2)
            return carry

        lax.fori_loop(0, n_groups // 2, trip, 0)

    seq_len = len_ref[micro, jnp.minimum(step, n_seqs - 1)]
    n_live = jnp.minimum(pos + 1, (seq_len + t_loc - 1) // t_loc)
    for n_keys in range(1, n_chunks + 1):
        pl.when(jnp.logical_and(n_live == n_keys, step < n_seqs))(functools.partial(run, n_keys))


def run_layer(pos, lengths, x, kv, gain, w_in, w_out, head_dim, micro, next_params=None, prev=None, whole=None):
    n_seqs, t_loc, d_model = x.shape[-3:]

    def after(b):
        return jnp.minimum(b + 1, n_seqs - 1)

    def now(b):
        return jnp.minimum(b, n_seqs - 1)

    def before(b):
        return jnp.maximum(b - 1, 0)

    def x_spec(seq):
        if x.ndim == 4:
            return pl.BlockSpec((None, None) + x.shape[2:], lambda b, *_: (micro, seq(b), 0, 0))
        return pl.BlockSpec((None,) + x.shape[1:], lambda b, *_: (seq(b), 0, 0))

    n_groups, _, in_loc = w_in.shape
    _, n_parts, rows_out, _ = w_out.shape
    n_chunks = kv.shape[0]
    width = kv.shape[-1]

    def kv_spec(seq):
        return pl.BlockSpec((n_chunks, None, t_loc, width), lambda b, *_: (0, seq(b), 0, 0))

    anywhere = pl.BlockSpec(memory_space=pl.ANY)
    in_specs = [
        x_spec(after),
        x_spec(before),
        kv_spec(now),
        kv_spec(after),
        pl.BlockSpec((1, d_model), lambda b, *_: (0, 0)),
        anywhere,
        anywhere,
    ]
    args = [x, x, kv, kv, gain, w_in, w_out]
    if next_params is not None:
        in_specs += [pl.BlockSpec((1, d_model), lambda b, *_: (0, 0)), pl.BlockSpec((d_model, width), lambda b, *_: (0, 0))]
        args += list(next_params)
    aliases = {}
    if prev is not None:
        in_specs.append(anywhere)
        aliases = {2 + len(args): 0}
        args.append(prev)
    if whole is None:
        out_shape = [jax.ShapeDtypeStruct((n_seqs, t_loc, d_model), BF16)]
        out_specs = [pl.BlockSpec((None, t_loc, d_model), lambda b, *_: (before(b), 0, 0))]
    else:
        out_shape = [jax.ShapeDtypeStruct((whole, n_seqs, t_loc, d_model), BF16)]
        out_specs = [pl.BlockSpec((None, None, t_loc, d_model), lambda b, *_: (micro, before(b), 0, 0))]
    if next_params is not None:
        out_shape.append(jax.ShapeDtypeStruct((n_seqs, t_loc, width), BF16))
        out_specs.append(pl.BlockSpec((None, t_loc, width), lambda b, *_: (before(b), 0, 0)))
    rows = n_seqs * t_loc
    heads = (2 * rows_out - in_loc) // head_dim
    flops = 2 * rows * n_groups * d_model * (in_loc + rows_out) + 8 * rows * n_groups * n_chunks * t_loc * (rows_out * 2 - in_loc + rows_out)
    return pl.pallas_call(
        functools.partial(layer_kernel, micro, n_groups, head_dim, next_params is not None, prev is not None),
        grid_spec=pltpu.PrefetchScalarGridSpec(
            num_scalar_prefetch=2,
            grid=(n_seqs + 1,),
            in_specs=in_specs,
            out_specs=out_specs,
            scratch_shapes=[
                pltpu.VMEM((n_groups, d_model, in_loc), BF16),
                pltpu.VMEM((n_groups, rows_out, d_model), BF16),
                pltpu.VMEM((2, t_loc, d_model), BF16),
                pltpu.VMEM((2, 2, head_dim, n_chunks // 2 * t_loc), BF16),
                pltpu.VMEM((2, t_loc, rows_out), BF16),
                pltpu.VMEM((2, t_loc, d_model), F32),
                pltpu.VMEM((heads, n_chunks * t_loc, t_loc), F32),
                pltpu.VMEM((heads, n_chunks * t_loc, t_loc), BF16),
                pltpu.VMEM((2, heads * head_dim, t_loc), BF16),
                pltpu.SemaphoreType.DMA((2, n_groups)),
                pltpu.SemaphoreType.DMA((n_groups, n_parts)),
            ],
        ),
        out_shape=out_shape,
        input_output_aliases=aliases,
        name="layer",
        compiler_params=pltpu.CompilerParams(dimension_semantics=("arbitrary",), vmem_limit_bytes=60 * 2**20),
        cost_estimate=pl.CostEstimate(flops=flops, bytes_accessed=4 * rows * d_model + 2 * n_groups * d_model * (in_loc + rows_out), transcendentals=0),
    )(pos, lengths, *args)


def solution(mesh):
    n_model = mesh.shape["model"]
    n_data = mesh.shape["data"]
    act_spec = P(None, ("part", "data"), "model", None)

    def local_fn(x, lengths, gain_blk, w_in_blk, w_kv_blk, w_out_blk):
        n_micro = x.shape[0]
        n_layers, d_half, in_loc = w_in_blk.shape
        out_loc = w_out_blk.shape[1]
        head_dim = w_kv_blk.shape[2] // 2
        pos = lax.axis_index("model").astype(jnp.int32).reshape(1)

        own = sort_weights(w_in_blk, w_out_blk, head_dim)
        (w_in_all, w_out_all, kv_first, kv_rest), gain, w_kv = startup(x, gain_blk, w_kv_blk, *own[0], n_model, n_data)
        own, kv_first, kv_rest = lax.optimization_barrier((own[1:], kv_first, kv_rest))
        kv = [kv_first] + [lax.all_gather(kv_rest[micro], "model", axis=0, tiled=False) for micro in range(n_micro - 1)]
        params = [(w_in_all, w_out_all)]
        for pair in own:
            params.append([lax.all_gather(w, ("model", "data"), axis=0, tiled=False) for w in pair])

        def weights(layer):
            w_in, w_out = params[layer]
            return w_in.reshape(n_model, -1, in_loc), w_out.reshape(n_model, n_data, out_loc, d_half)

        hidden = [x] * n_micro
        result = None
        for layer in range(n_layers):
            w_in, w_out = weights(layer)
            last = layer == n_layers - 1
            kv_next = []
            for micro in range(n_micro):
                outs = run_layer(
                    pos, lengths, hidden[micro], kv[micro], gain[layer], w_in, w_out, head_dim, micro,
                    next_params=None if last else (gain[layer + 1], w_kv[layer + 1]),
                    prev=result if last else None,
                    whole=n_micro if last else None,
                )
                if last:
                    result = outs[0]
                else:
                    hidden[micro] = outs[0]
                    kv_next.append(lax.all_gather(outs[1], "model", axis=0, tiled=False))
            kv = kv_next
        return result

    return jax.shard_map(
        local_fn,
        mesh=mesh,
        in_specs=(act_spec, P(None, ("part", "data")), P(None, "data"), P(None, "data", "model"), P(None, "data", None), P(None, "model", "data")),
        out_specs=act_spec,
        check_vma=False,
    )
```

```python
import functools
import jax
import jax.numpy as jnp
from jax import lax
from jax.experimental import pallas as pl
from jax.experimental.pallas import tpu as pltpu
from jax.sharding import PartitionSpec as P

NORM_EPS = 1e-6
NEG_BIG = -1e30
F32 = jnp.float32
BF16 = jnp.bfloat16
LANES = 128
MESH = pl.DeviceIdType.MESH


def norm_rows(x_act, gain_row):
    x_f32 = x_act.astype(F32)
    centered = x_f32 - jnp.mean(x_f32, axis=-1, keepdims=True)
    variance = jnp.mean(centered * centered, axis=-1, keepdims=True)
    return (centered * lax.rsqrt(variance + NORM_EPS) * gain_row.astype(F32)).astype(BF16)


def sort_kernel(head_dim, in_ref, out_ref, *sorted_refs):
    n_layers, in_loc, _ = in_ref.shape
    out_loc = out_ref.shape[1]
    ff_loc = in_loc - out_loc
    heads = (out_loc - ff_loc) // head_dim
    ff_head = ff_loc // heads
    unit_in = in_loc // heads
    unit_out = out_loc // heads
    blocks = ff_head // LANES
    for layer in range(n_layers):
        in_sorted_ref, out_sorted_ref = sorted_refs[2 * layer : 2 * layer + 2]
        for head in range(heads):
            base = head * unit_in
            for part in range(blocks):
                col = 2 * LANES * (head * blocks + part)
                gate = base + head_dim + part * LANES
                up = gate + ff_head
                in_sorted_ref[:, col : col + LANES] = in_ref[layer, gate : gate + LANES].T
                in_sorted_ref[:, col + LANES : col + 2 * LANES] = in_ref[layer, up : up + LANES].T
            row = head * unit_out
            out_sorted_ref[head * ff_head : (head + 1) * ff_head] = out_ref[layer, row + head_dim : row + unit_out]
            out_sorted_ref[ff_loc + head * head_dim : ff_loc + (head + 1) * head_dim] = out_ref[layer, row : row + head_dim]
        queries = jnp.concatenate([in_ref[layer, h * unit_in : h * unit_in + head_dim] for h in range(heads)], axis=0)
        in_sorted_ref[:, 2 * ff_loc :] = queries.T


def sort_weights(w_in, w_out, head_dim):
    n_layers, d_half, in_loc = w_in.shape
    vmem = pl.BlockSpec(memory_space=pltpu.VMEM)
    outs = [jax.ShapeDtypeStruct(w_in.shape[1:], BF16), jax.ShapeDtypeStruct(w_out.shape[1:], BF16)] * n_layers
    outs = pl.pallas_call(
        functools.partial(sort_kernel, head_dim),
        in_specs=[vmem, vmem],
        out_specs=[vmem] * len(outs),
        out_shape=outs,
        name="sort_weights",
        cost_estimate=pl.CostEstimate(flops=10**6, bytes_accessed=4 * (w_in.size + w_out.size), transcendentals=0),
    )(jnp.swapaxes(w_in, 1, 2), w_out)
    return [outs[2 * layer : 2 * layer + 2] for layer in range(n_layers)]


def startup_kernel(
    n_layers, x_hbm, gain_ref, w_kv_ref, w_in_ref, w_out_ref, w_in_hbm, w_out_hbm, kv_hbm, kv_rest_hbm, ready_hbm, *refs
):
    gain_out_refs, w_kv_out_refs = refs[:n_layers], refs[n_layers : 2 * n_layers]
    (
    in_buf, out_buf, kv_buf, gain_buf, w_kv_buf, x_buf, h_buf, ready_w_buf, ready_buf,
    own_send, own_recv, fwd_send, fwd_recv, small_send, small_recv,
    kv_send, kv_recv, x_sem, store_sem, kv_store_sem, kv_rest_sem, ready_sem,
    ) = refs[2 * n_layers :]
    data = lax.axis_index("data")
    model = lax.axis_index("model")
    _, d_half, width = w_kv_ref.shape
    n_micro, n_seqs, t_loc, d_model = x_hbm.shape
    block = x_buf.shape[1]
    per_micro = n_seqs // block
    n_blocks = n_micro * per_micro

    chip = model // 2
    core = model % 2
    mate = 2 * chip + 1 - core
    across = 2 * (1 - chip) + core
    across_mate = 2 * (1 - chip) + 1 - core
    flip = 1 - data
    to_mate = {"model": mate}
    to_x = {"model": across}
    to_y = {"data": flip}

    barrier = pltpu.get_barrier_semaphore()
    for peer in (to_mate, to_x, to_y):
        pl.semaphore_signal(barrier, inc=1, device_id=peer, device_id_type=MESH)
    pl.semaphore_wait(barrier, 3)

    def remote(src, dst, send, recv, peer):
        return pltpu.make_async_remote_copy(src_ref=src, dst_ref=dst, send_sem=send, recv_sem=recv, device_id=peer, device_id_type=MESH)

    def place(m, d):
        return 2 * m + d

    me = place(model, data)
    in_rows = d_half // 2
    out_rows = w_out_ref.shape[0] // 2

    def own_item(i):
        if i < 2:
            return w_in_ref.at[pl.ds(i % 2 * in_rows, in_rows)]
        return w_out_ref.at[pl.ds(i % 2 * out_rows, out_rows)]

    def buf_item(slot, i):
        if i < 2:
            return in_buf.at[slot, pl.ds(i % 2 * in_rows, in_rows)]
        return out_buf.at[slot, pl.ds(i % 2 * out_rows, out_rows)]

    def hbm_item(slot, i):
        if i < 2:
            return w_in_hbm.at[slot, pl.ds(i % 2 * in_rows, in_rows)]
        return w_out_hbm.at[slot, pl.ds(i % 2 * out_rows, out_rows)]

    gain_copy = remote(gain_ref, gain_buf.at[data], small_send.at[0], small_recv.at[0], to_y)
    w_kv_copy = remote(w_kv_ref, w_kv_buf.at[data], small_send.at[1], small_recv.at[1], to_y)
    gain_copy.start()
    w_kv_copy.start()

    def x_copy(t):
        return pltpu.make_async_copy(x_hbm.at[t // per_micro, pl.ds(t % per_micro * block, block)], x_buf.at[t % 2], x_sem.at[t % 2])

    x_copy(0).start()

    own = {}
    for i in range(4):
        for k, peer in enumerate((to_y, to_x, to_mate)):
            own[k, i] = remote(own_item(i), buf_item(me, i), own_send.at[k, i], own_recv.at[k, i], peer)
            own[k, i].start()
    stores = []

    def store(slot, i, src):
        copy = pltpu.make_async_copy(src, hbm_item(slot, i), store_sem.at[len(stores)])
        copy.start()
        stores.append(copy)

    for i in range(4):
        store(me, i, own_item(i))

    gain_copy.wait()
    w_kv_copy.wait()
    gain_buf[data] = gain_ref[...]
    w_kv_buf[data] = w_kv_ref[...]
    for layer in range(n_layers):
        for d in range(2):
            gain_out_refs[layer][:, d * d_half : (d + 1) * d_half] = gain_buf[d, layer : layer + 1]
            w_kv_out_refs[layer][d * d_half : (d + 1) * d_half] = w_kv_buf[d, layer]
    gain = jnp.concatenate([gain_buf[d, 0:1] for d in range(2)], axis=1)
    w_kv = jnp.concatenate([w_kv_buf[d, 0] for d in range(2)], axis=0)

    def kv_place(m, t):
        return kv_buf.at[t, m]

    def kv_copy(k, t, m, peer):
        return remote(kv_place(m, t), kv_place(m, t), kv_send.at[k, t], kv_recv.at[k, t], peer)

    def kv_store(k, t, m):
        return pltpu.make_async_copy(kv_place(m, t), kv_hbm.at[m, pl.ds(t * block, block)], kv_store_sem.at[k, t])

    def kv_rest_store(t):
        rest = t - per_micro
        return pltpu.make_async_copy(
            kv_place(model, t), kv_rest_hbm.at[rest // per_micro, pl.ds(rest % per_micro * block, block)], kv_rest_sem.at[rest]
        )

    def send_kv(t):
        kv_copy(0, t, model, to_x).start()
        kv_copy(1, t, model, to_mate).start()
        kv_store(0, t, model).start()

    def kv_step(t, carry):
        @pl.when(t + 1 < n_blocks)
        def _():
            x_copy(t + 1).start()

        x_copy(t).wait()
        h = norm_rows(x_buf[t % 2].reshape(block * t_loc, d_model), gain)
        h_buf[t] = h
        kv = jnp.dot(h, w_kv, preferred_element_type=F32).astype(BF16)
        kv_buf[t, model] = kv.reshape(block, t_loc, width)

        @pl.when(jnp.logical_and(t > 0, t <= per_micro))
        def _():
            send_kv(t - 1)

        @pl.when(t > per_micro)
        def _():
            kv_rest_store(t - 1).start()

        return carry

    lax.fori_loop(0, n_blocks, kv_step, 0)

    kv_rest_store(n_blocks - 1).start()

    forward = {}

    def pass_on(k, i, slot, peer):
        forward[k, i] = remote(buf_item(slot, i), buf_item(slot, i), fwd_send.at[k, i], fwd_recv.at[k, i], peer)
        forward[k, i].start()

    def take_y(i):
        own[0, i].wait_recv()
        slot = place(model, flip)
        pass_on(2, i, slot, to_mate)
        store(slot, i, buf_item(slot, i))

    def take_mate(i):
        own[2, i].wait_recv()
        slot = place(mate, data)
        store(slot, i, buf_item(slot, i))

    def take_mate_y(i):
        forward[2, i].wait_recv()
        slot = place(mate, flip)
        store(slot, i, buf_item(slot, i))

    for i in range(2):
        take_y(i)
    for i in range(2):
        take_mate(i)
    for i in range(2):
        take_mate_y(i)

    cols = ready_w_buf.shape[2]
    ready_w_buf[core, pl.ds(data * d_half, d_half)] = w_in_ref[:, :cols]
    ready_w_buf[core, pl.ds(flip * d_half, d_half)] = in_buf[place(model, flip), :, :cols]
    ready_w_buf[1 - core, pl.ds(data * d_half, d_half)] = in_buf[place(mate, data), :, :cols]
    ready_w_buf[1 - core, pl.ds(flip * d_half, d_half)] = in_buf[place(mate, flip), :, :cols]

    rows = ready_buf.shape[1]
    per_block = block * t_loc // rows

    def ready_store(u):
        return pltpu.make_async_copy(ready_buf.at[u % 2], ready_hbm.at[pl.ds(u * rows, rows)], ready_sem.at[u % 2])

    def ready_step(u, carry):
        @pl.when(u >= 2)
        def _():
            ready_store(u - 2).wait()

        h = h_buf[u // per_block, pl.ds(u % per_block * rows, rows)]
        for sub in range(2):
            for col in range(0, cols // 2, LANES):
                both = jnp.dot(h, ready_w_buf[sub, :, 2 * col : 2 * (col + LANES)], preferred_element_type=F32)
                both = both.astype(BF16).astype(F32)
                gate, up = both[:, :LANES], both[:, LANES:]
                at = sub * (cols // 2) + col
                ready_buf[u % 2, :, at : at + LANES] = (jax.nn.silu(gate) * up).astype(BF16)
        ready_store(u).start()
        return carry

    n_ready = n_blocks * per_block
    first_part = n_ready * 3 // 8
    lax.fori_loop(0, first_part, ready_step, 0)

    for i in range(4):
        own[1, i].wait_recv()
        slot = place(across, data)
        if i < 3:
            pass_on(0, i, slot, to_y)
        pass_on(1, i, slot, to_mate)
        store(slot, i, buf_item(slot, i))
    for i in range(2, 4):
        take_y(i)
        if i == 3:
            pass_on(0, i, place(model, flip), to_x)
        take_mate(i)

    lax.fori_loop(first_part, n_ready, ready_step, 0)
    ready_store(n_ready - 2).wait()
    ready_store(n_ready - 1).wait()

    for i in range(4):
        for t in range(i * per_micro // 4, (i + 1) * per_micro // 4):
            kv_copy(0, t, model, to_x).wait_recv()
            kv_copy(2, t, across, to_mate).start()
            kv_store(1, t, across).start()
            kv_copy(1, t, model, to_mate).wait_recv()
            kv_store(2, t, mate).start()
        forward[0, i].wait_recv()
        slot = place(across, flip)
        pass_on(3, i, slot, to_mate)
        store(slot, i, buf_item(slot, i))
        forward[1, i].wait_recv()
        slot = place(across_mate, data)
        store(slot, i, buf_item(slot, i))
        if i >= 2:
            take_mate_y(i)

    for t in range(per_micro):
        kv_copy(2, t, across, to_mate).wait_recv()
        kv_store(3, t, across_mate).start()
    for i in range(4):
        forward[3, i].wait_recv()
        slot = place(across_mate, flip)
        store(slot, i, buf_item(slot, i))

    for copy in own.values():
        copy.wait_send()
    for copy in forward.values():
        copy.wait_send()
    for t in range(per_micro, n_blocks):
        kv_rest_store(t).wait()
    for t in range(per_micro):
        kv_copy(0, t, model, to_x).wait_send()
        kv_copy(1, t, model, to_mate).wait_send()
        kv_copy(2, t, across, to_mate).wait_send()
        for k, m in enumerate((model, across, mate, across_mate)):
            kv_store(k, t, m).wait()
    for copy in stores:
        copy.wait()


def startup(x, gain, w_kv, w_in, w_out, n_model, n_data):
    n_micro, n_seqs, t_loc, d_model = x.shape
    n_layers, d_half, width = w_kv.shape
    _, in_loc = w_in.shape
    out_loc, _ = w_out.shape
    n_all = n_model * n_data
    block = 4
    n_blocks = n_micro * n_seqs // block
    vmem = pl.BlockSpec(memory_space=pltpu.VMEM)
    anywhere = pl.BlockSpec(memory_space=pl.ANY)
    dma = pltpu.SemaphoreType.DMA
    per_micro = n_seqs // block
    ff_loc = in_loc - out_loc
    outs = pl.pallas_call(
        functools.partial(startup_kernel, n_layers),
        in_specs=[anywhere, vmem, vmem, vmem, vmem],
        out_specs=[anywhere] * 5 + [vmem] * (2 * n_layers),
        out_shape=[
            jax.ShapeDtypeStruct((n_all, d_half, in_loc), BF16),
            jax.ShapeDtypeStruct((n_all, out_loc, d_half), BF16),
            jax.ShapeDtypeStruct((n_model, n_seqs, t_loc, width), BF16),
            jax.ShapeDtypeStruct((n_micro - 1, n_seqs, t_loc, width), BF16),
            jax.ShapeDtypeStruct((n_micro * n_seqs * t_loc, 2 * ff_loc), BF16),
        ]
        + [jax.ShapeDtypeStruct((1, d_model), BF16)] * n_layers
        + [jax.ShapeDtypeStruct((d_model, width), BF16)] * n_layers,
        scratch_shapes=[
            pltpu.VMEM((n_all, d_half, in_loc), BF16),
            pltpu.VMEM((n_all, out_loc, d_half), BF16),
            pltpu.VMEM((n_blocks, n_model, block, t_loc, width), BF16),
            pltpu.VMEM((n_data, n_layers, d_half), BF16),
            pltpu.VMEM((n_data, n_layers, d_half, width), BF16),
            pltpu.VMEM((2, block, t_loc, d_model), BF16),
            pltpu.VMEM((n_blocks, block * t_loc, d_model), BF16),
            pltpu.VMEM((2, d_model, 2 * ff_loc), BF16),
            pltpu.VMEM((2, 2 * t_loc, 2 * ff_loc), BF16),
            dma((3, 4)), dma((3, 4)), dma((4, 4)), dma((4, 4)), dma((2,)), dma((2,)),
            dma((3, per_micro)), dma((3, per_micro)), dma((2,)), dma((4 * n_all,)), dma((4, per_micro)), dma((n_blocks - per_micro,)), dma((2,)),
        ],
        name="startup",
        compiler_params=pltpu.CompilerParams(collective_id=0, has_side_effects=True, vmem_limit_bytes=60 * 2**20),
        cost_estimate=pl.CostEstimate(flops=10**11, bytes_accessed=10**8, transcendentals=0),
    )(x, gain, w_kv, w_in, w_out)
    return outs[:5], outs[5 : 5 + n_layers], outs[5 + n_layers :]


def layer_kernel(micro, n_groups, head_dim, has_ready, has_next, has_prev, *refs):
    refs = list(refs)
    pos_ref, len_ref = refs[:2]
    x_after_ref, x_before_ref, kv_ref, kv_after_ref, gain_ref, w_in_hbm, w_out_hbm = refs[2:9]
    refs = refs[9:]
    ready_ref = None
    if has_ready:
        ready_ref = refs[0]
        refs = refs[1:]
    if has_next:
        gain_next_ref, w_kv_next_ref = refs[:2]
        refs = refs[2:]
    if has_prev:
        refs = refs[1:]
    y_ref = refs[0]
    refs = refs[1:]
    if has_next:
        kv_next_ref = refs[0]
        refs = refs[1:]
    w_in_ref, w_out_ref, h_ref, vt_ref, joined_ref, acc_ref, s_ref, p_ref, query_ref, in_sem, out_sem = refs

    t_loc, d_model = x_after_ref.shape
    n_chunks = kv_ref.shape[0]
    rows_out = w_out_ref.shape[1]
    half = w_out_hbm.shape[3]
    n_parts = w_out_hbm.shape[1]
    in_loc = w_in_ref.shape[2]
    ff_loc = in_loc - rows_out
    q_loc = rows_out - ff_loc
    heads = q_loc // head_dim
    step = pl.program_id(0)
    n_seqs = pl.num_programs(0) - 1
    tile = 256
    lanes = LANES
    rows_part = t_loc // 2

    pos = pos_ref[0]

    def source(group):
        if has_ready:
            chip = pos // 2
            return 2 * chip + group if group < 2 else 2 * (1 - chip) + group - 2
        return group

    def query_copy(group):
        cols = pl.ds(2 * ff_loc, q_loc)
        return pltpu.make_async_copy(w_in_hbm.at[source(group), :, cols], w_in_ref.at[group, :, cols], in_sem.at[0, group])

    def in_copy(group):
        cols = pl.ds(0, 2 * ff_loc)
        return pltpu.make_async_copy(w_in_hbm.at[source(group), :, cols], w_in_ref.at[group, :, cols], in_sem.at[1, group])

    def out_copy(group, part):
        return pltpu.make_async_copy(
            w_out_hbm.at[source(group), part], w_out_ref.at[group, :, pl.ds(part * half, half)], out_sem.at[group, part]
        )

    out_first = [out_copy(0, part) for part in range(n_parts)]
    early = out_first if has_ready else [in_copy(0)] + out_first + [in_copy(1)]

    def copies(*groups):
        return [in_copy(group) for group in groups] + [out_copy(group, part) for group in groups for part in range(n_parts)]

    slot = lax.rem(step, 2)
    other = 1 - slot

    def project_query(src, group, dst):
        q = jnp.dot(h_ref[src], w_in_ref[group, :, 2 * ff_loc :], preferred_element_type=F32).astype(BF16)
        query_ref[dst] = (q * BF16(head_dim**-0.5)).T

    def normalize_part(dst, src_ref, part):
        rows = pl.ds(part * rows_part, rows_part)
        h_ref[dst, rows] = norm_rows(src_ref[rows], gain_ref[...])

    def transpose_part(dst, src_ref, part):
        span = n_chunks // 2
        block = src_ref[pl.ds(part * span, span)].reshape(span * t_loc, 2 * head_dim)
        vt_ref[dst, part] = block.T[head_dim:]

    def epilogue_part(src, part):
        rows = pl.ds(part * rows_part, rows_part)
        y = (x_before_ref[rows].astype(F32) + acc_ref[src, rows]).astype(BF16)
        y_ref[rows] = y
        if has_next:
            h_next = norm_rows(y, gain_next_ref[...])
            kv_next_ref[rows] = jnp.dot(h_next, w_kv_next_ref[...], preferred_element_type=F32).astype(BF16)

    def project_out(joined_slot, group, dst, fresh, col):
        cols = slice(col, col + tile)
        z = jnp.dot(joined_ref[joined_slot], w_out_ref[group, :, cols], preferred_element_type=F32)
        z = z.astype(BF16).astype(F32)
        base = acc_ref[dst, :, cols]
        if fresh is not None:
            base = jnp.where(fresh, 0.0, base)
        acc_ref[dst, :, cols] = base + z

    @pl.when(step == 0)
    def _():
        for group in range(n_groups):
            query_copy(group).start()
        for copy in early:
            copy.start()
        for part in range(2):
            normalize_part(slot, x_before_ref, part)
            transpose_part(slot, kv_ref, part)
        joined_ref[1] = jnp.zeros_like(joined_ref[1])
        acc_ref[1] = jnp.zeros_like(acc_ref[1])
        for group in range(n_groups):
            query_copy(group).wait()
        project_query(slot, 0, 0)

    @pl.when(step == n_seqs)
    def _():
        for col in range(0, d_model, tile):
            project_out(1, n_groups - 1, other, None, col)
        for part in range(2):
            epilogue_part(other, part)

    def run(n_keys):
        chunk = n_keys - 1
        seq_len = len_ref[micro, jnp.minimum(step, n_seqs - 1)]
        lane = lax.broadcasted_iota(jnp.int32, (1, t_loc), 1)
        limit = jnp.minimum(lane + (pos - chunk) * t_loc, seq_len - chunk * t_loc - 1)
        key = lax.broadcasted_iota(jnp.int32, (t_loc, t_loc), 0)

        def trip(pair, carry):
            first = 2 * pair
            before = jnp.where(jnp.logical_and(step == 0, pair == 0), 0, lax.rem(first + n_groups - 1, n_groups))

            @pl.when(step == 0)
            def _():
                late = [out_copy(1, part) for part in range(n_parts)] + copies(*range(2, n_groups))

                @pl.when(pair == 0)
                def _():
                    for copy in early:
                        copy.wait()
                    for copy in late:
                        copy.start()

                @pl.when(pair == 1)
                def _():
                    for copy in late:
                        copy.wait()

            h = h_ref[slot]
            dst_before = jnp.where(pair == 0, other, slot)
            tops = {}
            sums = {}

            def query(sub):
                if sub == 0:
                    project_query(slot, first + 1, 1)
                else:
                    project_query(jnp.where(pair == n_groups // 2 - 1, other, slot), lax.rem(first + 2, n_groups), 0)

            def gate_up(sub, part):
                if has_ready and pair == 0:
                    cols = slice(part * tile, (part + 1) * tile)
                    joined_ref[sub, :, cols] = ready_ref[:, sub * ff_loc + part * tile : sub * ff_loc + (part + 1) * tile]
                    return
                for col in range(part * tile, (part + 1) * tile, lanes):
                    both = jnp.dot(h, w_in_ref[first + sub, :, 2 * col : 2 * (col + lanes)], preferred_element_type=F32)
                    both = both.astype(BF16).astype(F32)
                    gate, up = both[:, :lanes], both[:, lanes:]
                    joined_ref[sub, :, col : col + lanes] = (jax.nn.silu(gate) * up).astype(BF16)

            def score(sub, head):
                q_t = query_ref[sub, head * head_dim : (head + 1) * head_dim]
                best = None
                for c in range(n_keys):
                    s = jnp.dot(kv_ref[c, :, :head_dim], q_t, preferred_element_type=F32)
                    if c == chunk:
                        s = jnp.where(key <= limit, s, NEG_BIG)
                    s_ref[head, c * t_loc : (c + 1) * t_loc] = s
                    m = jnp.max(s.reshape(t_loc // 8, 8, t_loc), axis=0)
                    best = m if best is None else jnp.maximum(best, m)
                tops[sub, head] = jnp.max(best, axis=0, keepdims=True)

            def softmax(sub, head):
                total = None
                top = tops[sub, head]
                width = 16
                for r in range(0, n_keys * t_loc, width):
                    e = jnp.exp(s_ref[head, r : r + width] - top)
                    t = jnp.sum(e.reshape(width // 8, 8, t_loc), axis=0)
                    total = t if total is None else total + t
                    p_ref[head, r : r + width] = e.astype(BF16)
                sums[sub, head] = jnp.sum(total, axis=0, keepdims=True)

            outs = {}

            def value(sub, head):
                span = n_chunks // 2 * t_loc
                out_t = None
                for part in range(2):
                    size = min(span, n_keys * t_loc - part * span)
                    if size <= 0:
                        continue
                    o = jnp.dot(vt_ref[slot, part, :, :size], p_ref[head, part * span : part * span + size], preferred_element_type=F32)
                    out_t = o if out_t is None else out_t + o
                outs[sub, head] = (out_t / sums[sub, head]).astype(BF16)
                if head == heads - 1:
                    joined_ref[sub, :, ff_loc:] = jnp.concatenate([outs[sub, i] for i in range(heads)], axis=0).T

            for sub in range(2):
                if sub == 0:
                    z = lambda i: project_out(1, before, dst_before, None, i * tile)
                else:
                    z = lambda i: project_out(0, first, slot, pair == 0, i * tile)
                score(sub, 0)
                z(0)
                score(sub, 1)
                softmax(sub, 0)
                z(1)
                score(sub, 2)
                softmax(sub, 1)
                value(sub, 0)
                z(2)
                gate_up(sub, 0)
                if sub == 0:
                    query(sub)
                    normalize_part(other, x_after_ref, pair)
                    transpose_part(other, kv_after_ref, pair)
                softmax(sub, 2)
                value(sub, 1)
                gate_up(sub, 1)
                if sub == 1:
                    query(sub)
                    epilogue_part(other, pair)
                value(sub, 2)
                gate_up(sub, 2)
            return carry

        if has_ready:
            for pair in range(n_groups // 2):
                trip(pair, 0)
        else:
            lax.fori_loop(0, n_groups // 2, trip, 0)

    seq_len = len_ref[micro, jnp.minimum(step, n_seqs - 1)]
    n_live = jnp.minimum(pos + 1, (seq_len + t_loc - 1) // t_loc)
    for n_keys in range(1, n_chunks + 1):
        pl.when(jnp.logical_and(n_live == n_keys, step < n_seqs))(functools.partial(run, n_keys))


def run_layer(pos, lengths, x, kv, gain, w_in, w_out, head_dim, micro, ready=None, next_params=None, prev=None, whole=None):
    n_seqs, t_loc, d_model = x.shape[-3:]

    def after(b):
        return jnp.minimum(b + 1, n_seqs - 1)

    def now(b):
        return jnp.minimum(b, n_seqs - 1)

    def before(b):
        return jnp.maximum(b - 1, 0)

    def x_spec(seq):
        if x.ndim == 4:
            return pl.BlockSpec((None, None) + x.shape[2:], lambda b, *_: (micro, seq(b), 0, 0))
        return pl.BlockSpec((None,) + x.shape[1:], lambda b, *_: (seq(b), 0, 0))

    n_groups, _, in_loc = w_in.shape
    _, n_parts, rows_out, _ = w_out.shape
    n_chunks = kv.shape[0]
    width = kv.shape[-1]

    def kv_spec(seq):
        return pl.BlockSpec((n_chunks, None, t_loc, width), lambda b, *_: (0, seq(b), 0, 0))

    anywhere = pl.BlockSpec(memory_space=pl.ANY)
    in_specs = [
        x_spec(after),
        x_spec(before),
        kv_spec(now),
        kv_spec(after),
        pl.BlockSpec((1, d_model), lambda b, *_: (0, 0)),
        anywhere,
        anywhere,
    ]
    args = [x, x, kv, kv, gain, w_in, w_out]
    if ready is not None:
        in_specs.append(pl.BlockSpec((t_loc, ready.shape[1]), lambda b, *_: (micro * n_seqs + now(b), 0)))
        args.append(ready)
    if next_params is not None:
        in_specs += [pl.BlockSpec((1, d_model), lambda b, *_: (0, 0)), pl.BlockSpec((d_model, width), lambda b, *_: (0, 0))]
        args += list(next_params)
    aliases = {}
    if prev is not None:
        in_specs.append(anywhere)
        aliases = {2 + len(args): 0}
        args.append(prev)
    if whole is None:
        out_shape = [jax.ShapeDtypeStruct((n_seqs, t_loc, d_model), BF16)]
        out_specs = [pl.BlockSpec((None, t_loc, d_model), lambda b, *_: (before(b), 0, 0))]
    else:
        out_shape = [jax.ShapeDtypeStruct((whole, n_seqs, t_loc, d_model), BF16)]
        out_specs = [pl.BlockSpec((None, None, t_loc, d_model), lambda b, *_: (micro, before(b), 0, 0))]
    if next_params is not None:
        out_shape.append(jax.ShapeDtypeStruct((n_seqs, t_loc, width), BF16))
        out_specs.append(pl.BlockSpec((None, t_loc, width), lambda b, *_: (before(b), 0, 0)))
    rows = n_seqs * t_loc
    heads = (2 * rows_out - in_loc) // head_dim
    flops = 2 * rows * n_groups * d_model * (in_loc + rows_out) + 8 * rows * n_groups * n_chunks * t_loc * (rows_out * 2 - in_loc + rows_out)
    return pl.pallas_call(
        functools.partial(layer_kernel, micro, n_groups, head_dim, ready is not None, next_params is not None, prev is not None),
        grid_spec=pltpu.PrefetchScalarGridSpec(
            num_scalar_prefetch=2,
            grid=(n_seqs + 1,),
            in_specs=in_specs,
            out_specs=out_specs,
            scratch_shapes=[
                pltpu.VMEM((n_groups, d_model, in_loc), BF16),
                pltpu.VMEM((n_groups, rows_out, d_model), BF16),
                pltpu.VMEM((2, t_loc, d_model), BF16),
                pltpu.VMEM((2, 2, head_dim, n_chunks // 2 * t_loc), BF16),
                pltpu.VMEM((2, t_loc, rows_out), BF16),
                pltpu.VMEM((2, t_loc, d_model), F32),
                pltpu.VMEM((heads, n_chunks * t_loc, t_loc), F32),
                pltpu.VMEM((heads, n_chunks * t_loc, t_loc), BF16),
                pltpu.VMEM((2, heads * head_dim, t_loc), BF16),
                pltpu.SemaphoreType.DMA((2, n_groups)),
                pltpu.SemaphoreType.DMA((n_groups, n_parts)),
            ],
        ),
        out_shape=out_shape,
        input_output_aliases=aliases,
        name="layer",
        compiler_params=pltpu.CompilerParams(dimension_semantics=("arbitrary",), vmem_limit_bytes=60 * 2**20),
        cost_estimate=pl.CostEstimate(flops=flops, bytes_accessed=4 * rows * d_model + 2 * n_groups * d_model * (in_loc + rows_out), transcendentals=0),
    )(pos, lengths, *args)


def solution(mesh):
    n_model = mesh.shape["model"]
    n_data = mesh.shape["data"]
    act_spec = P(None, ("part", "data"), "model", None)

    def local_fn(x, lengths, gain_blk, w_in_blk, w_kv_blk, w_out_blk):
        n_micro = x.shape[0]
        n_layers, d_half, in_loc = w_in_blk.shape
        out_loc = w_out_blk.shape[1]
        head_dim = w_kv_blk.shape[2] // 2
        pos = lax.axis_index("model").astype(jnp.int32).reshape(1)

        own = sort_weights(w_in_blk, w_out_blk, head_dim)
        (w_in_all, w_out_all, kv_first, kv_rest, ready), gain, w_kv = startup(x, gain_blk, w_kv_blk, *own[0], n_model, n_data)
        own, kv_first, kv_rest = lax.optimization_barrier((own[1:], kv_first, kv_rest))
        kv = [kv_first] + [lax.all_gather(kv_rest[micro], "model", axis=0, tiled=False) for micro in range(n_micro - 1)]
        params = [(w_in_all, w_out_all)]
        for pair in own:
            params.append([lax.all_gather(w, ("model", "data"), axis=0, tiled=False) for w in pair])

        def weights(layer):
            w_in, w_out = params[layer]
            return w_in.reshape(n_model, -1, in_loc), w_out.reshape(n_model, n_data, out_loc, d_half)

        hidden = [x] * n_micro
        result = None
        for layer in range(n_layers):
            w_in, w_out = weights(layer)
            last = layer == n_layers - 1
            kv_next = []
            for micro in range(n_micro):
                outs = run_layer(
                    pos, lengths, hidden[micro], kv[micro], gain[layer], w_in, w_out, head_dim, micro,
                    ready=ready if layer == 0 else None,
                    next_params=None if last else (gain[layer + 1], w_kv[layer + 1]),
                    prev=result if last else None,
                    whole=n_micro if last else None,
                )
                if last:
                    result = outs[0]
                else:
                    hidden[micro] = outs[0]
                    kv_next.append(lax.all_gather(outs[1], "model", axis=0, tiled=False))
            kv = kv_next
        return result

    return jax.shard_map(
        local_fn,
        mesh=mesh,
        in_specs=(act_spec, P(None, ("part", "data")), P(None, "data"), P(None, "data", "model"), P(None, "data", None), P(None, "model", "data")),
        out_specs=act_spec,
        check_vma=False,
    )
```

```python
import functools
import jax
import jax.numpy as jnp
from jax import lax
from jax.experimental import pallas as pl
from jax.experimental.pallas import tpu as pltpu
from jax.sharding import PartitionSpec as P

NORM_EPS = 1e-6
NEG_BIG = -1e30
F32 = jnp.float32
BF16 = jnp.bfloat16
LANES = 128
MESH = pl.DeviceIdType.MESH


def norm_rows(x_act, gain_row):
    x_f32 = x_act.astype(F32)
    centered = x_f32 - jnp.mean(x_f32, axis=-1, keepdims=True)
    variance = jnp.mean(centered * centered, axis=-1, keepdims=True)
    return (centered * lax.rsqrt(variance + NORM_EPS) * gain_row.astype(F32)).astype(BF16)


def sort_kernel(head_dim, in_ref, out_ref, *sorted_refs):
    n_layers, in_loc, _ = in_ref.shape
    out_loc = out_ref.shape[1]
    ff_loc = in_loc - out_loc
    heads = (out_loc - ff_loc) // head_dim
    ff_head = ff_loc // heads
    unit_in = in_loc // heads
    unit_out = out_loc // heads
    blocks = ff_head // LANES
    for layer in range(n_layers):
        in_sorted_ref, out_sorted_ref = sorted_refs[2 * layer : 2 * layer + 2]
        for head in range(heads):
            base = head * unit_in
            for part in range(blocks):
                col = 2 * LANES * (head * blocks + part)
                gate = base + head_dim + part * LANES
                up = gate + ff_head
                in_sorted_ref[:, col : col + LANES] = in_ref[layer, gate : gate + LANES].T
                in_sorted_ref[:, col + LANES : col + 2 * LANES] = in_ref[layer, up : up + LANES].T
            row = head * unit_out
            out_sorted_ref[head * ff_head : (head + 1) * ff_head] = out_ref[layer, row + head_dim : row + unit_out]
            out_sorted_ref[ff_loc + head * head_dim : ff_loc + (head + 1) * head_dim] = out_ref[layer, row : row + head_dim]
        queries = jnp.concatenate([in_ref[layer, h * unit_in : h * unit_in + head_dim] for h in range(heads)], axis=0)
        in_sorted_ref[:, 2 * ff_loc :] = queries.T


def sort_weights(w_in, w_out, head_dim):
    n_layers, d_half, in_loc = w_in.shape
    vmem = pl.BlockSpec(memory_space=pltpu.VMEM)
    outs = [jax.ShapeDtypeStruct(w_in.shape[1:], BF16), jax.ShapeDtypeStruct(w_out.shape[1:], BF16)] * n_layers
    outs = pl.pallas_call(
        functools.partial(sort_kernel, head_dim),
        in_specs=[vmem, vmem],
        out_specs=[vmem] * len(outs),
        out_shape=outs,
        name="sort_weights",
        cost_estimate=pl.CostEstimate(flops=10**6, bytes_accessed=4 * (w_in.size + w_out.size), transcendentals=0),
    )(jnp.swapaxes(w_in, 1, 2), w_out)
    return [outs[2 * layer : 2 * layer + 2] for layer in range(n_layers)]


def startup_kernel(
    n_layers, x_hbm, gain_ref, w_kv_ref, w_in_ref, w_out_ref, w_in_hbm, w_out_hbm, kv_hbm, kv_rest_hbm, ready_hbm, *refs
):
    gain_out_refs, w_kv_out_refs = refs[:n_layers], refs[n_layers : 2 * n_layers]
    (
    in_buf, out_buf, kv_buf, gain_buf, w_kv_buf, x_buf, h_buf, ready_w_buf, ready_buf,
    own_send, own_recv, fwd_send, fwd_recv, small_send, small_recv,
    kv_send, kv_recv, x_sem, store_sem, kv_store_sem, kv_rest_sem, ready_sem,
    ) = refs[2 * n_layers :]
    data = lax.axis_index("data")
    model = lax.axis_index("model")
    _, d_half, width = w_kv_ref.shape
    n_micro, n_seqs, t_loc, d_model = x_hbm.shape
    block = x_buf.shape[1]
    per_micro = n_seqs // block
    n_blocks = n_micro * per_micro

    chip = model // 2
    core = model % 2
    mate = 2 * chip + 1 - core
    across = 2 * (1 - chip) + core
    across_mate = 2 * (1 - chip) + 1 - core
    flip = 1 - data
    to_mate = {"model": mate}
    to_x = {"model": across}
    to_y = {"data": flip}

    barrier = pltpu.get_barrier_semaphore()
    for peer in (to_mate, to_x, to_y):
        pl.semaphore_signal(barrier, inc=1, device_id=peer, device_id_type=MESH)
    pl.semaphore_wait(barrier, 3)

    def remote(src, dst, send, recv, peer):
        return pltpu.make_async_remote_copy(src_ref=src, dst_ref=dst, send_sem=send, recv_sem=recv, device_id=peer, device_id_type=MESH)

    def place(m, d):
        return 2 * m + d

    me = place(model, data)
    in_rows = d_half // 2
    out_rows = w_out_ref.shape[0] // 2

    def own_item(i):
        if i < 2:
            return w_in_ref.at[pl.ds(i % 2 * in_rows, in_rows)]
        return w_out_ref.at[pl.ds(i % 2 * out_rows, out_rows)]

    def buf_item(slot, i):
        if i < 2:
            return in_buf.at[slot, pl.ds(i % 2 * in_rows, in_rows)]
        return out_buf.at[slot, pl.ds(i % 2 * out_rows, out_rows)]

    def hbm_item(slot, i):
        if i < 2:
            return w_in_hbm.at[slot, pl.ds(i % 2 * in_rows, in_rows)]
        return w_out_hbm.at[slot, pl.ds(i % 2 * out_rows, out_rows)]

    gain_copy = remote(gain_ref, gain_buf.at[data], small_send.at[0], small_recv.at[0], to_y)
    w_kv_copy = remote(w_kv_ref, w_kv_buf.at[data], small_send.at[1], small_recv.at[1], to_y)
    gain_copy.start()
    w_kv_copy.start()

    def x_copy(t):
        return pltpu.make_async_copy(x_hbm.at[t // per_micro, pl.ds(t % per_micro * block, block)], x_buf.at[t % 2], x_sem.at[t % 2])

    x_copy(0).start()

    own = {}
    for i in range(4):
        for k, peer in enumerate((to_y, to_x, to_mate)):
            own[k, i] = remote(own_item(i), buf_item(me, i), own_send.at[k, i], own_recv.at[k, i], peer)
            own[k, i].start()
    stores = []

    def store(slot, i, src):
        copy = pltpu.make_async_copy(src, hbm_item(slot, i), store_sem.at[len(stores)])
        copy.start()
        stores.append(copy)

    for i in range(4):
        store(me, i, own_item(i))

    gain_copy.wait()
    w_kv_copy.wait()
    gain_buf[data] = gain_ref[...]
    w_kv_buf[data] = w_kv_ref[...]
    for layer in range(n_layers):
        for d in range(2):
            gain_out_refs[layer][:, d * d_half : (d + 1) * d_half] = gain_buf[d, layer : layer + 1]
            w_kv_out_refs[layer][d * d_half : (d + 1) * d_half] = w_kv_buf[d, layer]
    gain = jnp.concatenate([gain_buf[d, 0:1] for d in range(2)], axis=1)
    w_kv = jnp.concatenate([w_kv_buf[d, 0] for d in range(2)], axis=0)

    def kv_place(m, t):
        return kv_buf.at[t, m]

    def kv_copy(k, t, m, peer):
        return remote(kv_place(m, t), kv_place(m, t), kv_send.at[k, t], kv_recv.at[k, t], peer)

    def kv_store(k, t, m):
        return pltpu.make_async_copy(kv_place(m, t), kv_hbm.at[m, pl.ds(t * block, block)], kv_store_sem.at[k, t])

    def kv_rest_store(t):
        rest = t - per_micro
        return pltpu.make_async_copy(
            kv_place(model, t), kv_rest_hbm.at[rest // per_micro, pl.ds(rest % per_micro * block, block)], kv_rest_sem.at[rest]
        )

    def send_kv(t):
        kv_copy(0, t, model, to_x).start()
        kv_copy(1, t, model, to_mate).start()
        kv_store(0, t, model).start()

    def kv_step(t, carry):
        @pl.when(t + 1 < n_blocks)
        def _():
            x_copy(t + 1).start()

        x_copy(t).wait()
        h = norm_rows(x_buf[t % 2].reshape(block * t_loc, d_model), gain)
        h_buf[t] = h
        kv = jnp.dot(h, w_kv, preferred_element_type=F32).astype(BF16)
        kv_buf[t, model] = kv.reshape(block, t_loc, width)

        @pl.when(jnp.logical_and(t > 0, t <= per_micro))
        def _():
            send_kv(t - 1)

        @pl.when(t > per_micro)
        def _():
            kv_rest_store(t - 1).start()

        return carry

    lax.fori_loop(0, n_blocks, kv_step, 0)

    kv_rest_store(n_blocks - 1).start()

    forward = {}

    def pass_on(k, i, slot, peer):
        forward[k, i] = remote(buf_item(slot, i), buf_item(slot, i), fwd_send.at[k, i], fwd_recv.at[k, i], peer)
        forward[k, i].start()

    def take_y(i):
        own[0, i].wait_recv()
        slot = place(model, flip)
        pass_on(2, i, slot, to_mate)
        store(slot, i, buf_item(slot, i))

    def take_mate(i):
        own[2, i].wait_recv()
        slot = place(mate, data)
        store(slot, i, buf_item(slot, i))

    def take_mate_y(i):
        forward[2, i].wait_recv()
        slot = place(mate, flip)
        store(slot, i, buf_item(slot, i))

    for i in range(2):
        take_y(i)
    for i in range(2):
        take_mate(i)
    for i in range(2):
        take_mate_y(i)

    cols = ready_w_buf.shape[2]
    ready_w_buf[core, pl.ds(data * d_half, d_half)] = w_in_ref[:, :cols]
    ready_w_buf[core, pl.ds(flip * d_half, d_half)] = in_buf[place(model, flip), :, :cols]
    ready_w_buf[1 - core, pl.ds(data * d_half, d_half)] = in_buf[place(mate, data), :, :cols]
    ready_w_buf[1 - core, pl.ds(flip * d_half, d_half)] = in_buf[place(mate, flip), :, :cols]

    rows = ready_buf.shape[1]
    per_block = block * t_loc // rows

    def ready_store(u):
        return pltpu.make_async_copy(ready_buf.at[u % 2], ready_hbm.at[pl.ds(u * rows, rows)], ready_sem.at[u % 2])

    def ready_step(u, carry):
        @pl.when(u >= 2)
        def _():
            ready_store(u - 2).wait()

        h = h_buf[u // per_block, pl.ds(u % per_block * rows, rows)]
        for sub in range(2):
            for col in range(0, cols // 2, LANES):
                both = jnp.dot(h, ready_w_buf[sub, :, 2 * col : 2 * (col + LANES)], preferred_element_type=F32)
                both = both.astype(BF16).astype(F32)
                gate, up = both[:, :LANES], both[:, LANES:]
                at = sub * (cols // 2) + col
                ready_buf[u % 2, :, at : at + LANES] = (jax.nn.silu(gate) * up).astype(BF16)
        ready_store(u).start()
        return carry

    n_ready = n_blocks * per_block
    first_part = n_ready * 3 // 8
    lax.fori_loop(0, first_part, ready_step, 0)

    for i in range(4):
        own[1, i].wait_recv()
        slot = place(across, data)
        if i < 3:
            pass_on(0, i, slot, to_y)
        pass_on(1, i, slot, to_mate)
        store(slot, i, buf_item(slot, i))
    for i in range(2, 4):
        take_y(i)
        if i == 3:
            pass_on(0, i, place(model, flip), to_x)
        take_mate(i)

    lax.fori_loop(first_part, n_ready, ready_step, 0)
    ready_store(n_ready - 2).wait()
    ready_store(n_ready - 1).wait()

    for i in range(4):
        for t in range(i * per_micro // 4, (i + 1) * per_micro // 4):
            kv_copy(0, t, model, to_x).wait_recv()
            kv_copy(2, t, across, to_mate).start()
            kv_store(1, t, across).start()
            kv_copy(1, t, model, to_mate).wait_recv()
            kv_store(2, t, mate).start()
        forward[0, i].wait_recv()
        slot = place(across, flip)
        pass_on(3, i, slot, to_mate)
        store(slot, i, buf_item(slot, i))
        forward[1, i].wait_recv()
        slot = place(across_mate, data)
        store(slot, i, buf_item(slot, i))
        if i >= 2:
            take_mate_y(i)

    for t in range(per_micro):
        kv_copy(2, t, across, to_mate).wait_recv()
        kv_store(3, t, across_mate).start()
    for i in range(4):
        forward[3, i].wait_recv()
        slot = place(across_mate, flip)
        store(slot, i, buf_item(slot, i))

    for copy in own.values():
        copy.wait_send()
    for copy in forward.values():
        copy.wait_send()
    for t in range(per_micro, n_blocks):
        kv_rest_store(t).wait()
    for t in range(per_micro):
        kv_copy(0, t, model, to_x).wait_send()
        kv_copy(1, t, model, to_mate).wait_send()
        kv_copy(2, t, across, to_mate).wait_send()
        for k, m in enumerate((model, across, mate, across_mate)):
            kv_store(k, t, m).wait()
    for copy in stores:
        copy.wait()


def startup(x, gain, w_kv, w_in, w_out, n_model, n_data):
    n_micro, n_seqs, t_loc, d_model = x.shape
    n_layers, d_half, width = w_kv.shape
    _, in_loc = w_in.shape
    out_loc, _ = w_out.shape
    n_all = n_model * n_data
    block = 4
    n_blocks = n_micro * n_seqs // block
    vmem = pl.BlockSpec(memory_space=pltpu.VMEM)
    anywhere = pl.BlockSpec(memory_space=pl.ANY)
    dma = pltpu.SemaphoreType.DMA
    per_micro = n_seqs // block
    ff_loc = in_loc - out_loc
    outs = pl.pallas_call(
        functools.partial(startup_kernel, n_layers),
        in_specs=[anywhere, vmem, vmem, vmem, vmem],
        out_specs=[anywhere] * 5 + [vmem] * (2 * n_layers),
        out_shape=[
            jax.ShapeDtypeStruct((n_all, d_half, in_loc), BF16),
            jax.ShapeDtypeStruct((n_all, out_loc, d_half), BF16),
            jax.ShapeDtypeStruct((n_model, n_seqs, t_loc, width), BF16),
            jax.ShapeDtypeStruct((n_micro - 1, n_seqs, t_loc, width), BF16),
            jax.ShapeDtypeStruct((n_micro * n_seqs * t_loc, 2 * ff_loc), BF16),
        ]
        + [jax.ShapeDtypeStruct((1, d_model), BF16)] * n_layers
        + [jax.ShapeDtypeStruct((d_model, width), BF16)] * n_layers,
        scratch_shapes=[
            pltpu.VMEM((n_all, d_half, in_loc), BF16),
            pltpu.VMEM((n_all, out_loc, d_half), BF16),
            pltpu.VMEM((n_blocks, n_model, block, t_loc, width), BF16),
            pltpu.VMEM((n_data, n_layers, d_half), BF16),
            pltpu.VMEM((n_data, n_layers, d_half, width), BF16),
            pltpu.VMEM((2, block, t_loc, d_model), BF16),
            pltpu.VMEM((n_blocks, block * t_loc, d_model), BF16),
            pltpu.VMEM((2, d_model, 2 * ff_loc), BF16),
            pltpu.VMEM((2, 2 * t_loc, 2 * ff_loc), BF16),
            dma((3, 4)), dma((3, 4)), dma((4, 4)), dma((4, 4)), dma((2,)), dma((2,)),
            dma((3, per_micro)), dma((3, per_micro)), dma((2,)), dma((4 * n_all,)), dma((4, per_micro)), dma((n_blocks - per_micro,)), dma((2,)),
        ],
        name="startup",
        compiler_params=pltpu.CompilerParams(collective_id=0, has_side_effects=True, vmem_limit_bytes=60 * 2**20),
        cost_estimate=pl.CostEstimate(flops=10**11, bytes_accessed=10**8, transcendentals=0),
    )(x, gain, w_kv, w_in, w_out)
    return outs[:5], outs[5 : 5 + n_layers], outs[5 + n_layers :]


def layer_kernel(micro, n_groups, head_dim, has_ready, has_next, has_prev, *refs):
    refs = list(refs)
    pos_ref, len_ref = refs[:2]
    x_after_ref, x_before_ref, kv_ref, kv_after_ref, gain_ref, w_in_hbm, w_out_hbm = refs[2:9]
    refs = refs[9:]
    ready_ref = None
    if has_ready:
        ready_ref = refs[0]
        refs = refs[1:]
    if has_next:
        gain_next_ref, w_kv_next_ref = refs[:2]
        refs = refs[2:]
    if has_prev:
        refs = refs[1:]
    y_ref = refs[0]
    refs = refs[1:]
    if has_next:
        kv_next_ref = refs[0]
        refs = refs[1:]
    w_in_ref, w_out_ref, h_ref, vt_ref, joined_ref, acc_ref, s_ref, p_ref, query_ref, in_sem, out_sem = refs

    t_loc, d_model = x_after_ref.shape
    n_chunks = kv_ref.shape[0]
    rows_out = w_out_ref.shape[1]
    half = w_out_hbm.shape[3]
    n_parts = w_out_hbm.shape[1]
    in_loc = w_in_ref.shape[2]
    ff_loc = in_loc - rows_out
    q_loc = rows_out - ff_loc
    heads = q_loc // head_dim
    step = pl.program_id(0)
    n_seqs = pl.num_programs(0) - 1
    tile = 256
    lanes = LANES
    rows_part = t_loc // 2

    pos = pos_ref[0]

    def source(group):
        if has_ready:
            chip = pos // 2
            return 2 * (chip if group % 2 == 0 else 1 - chip) + group // 2
        return group

    def query_copy(group):
        cols = pl.ds(2 * ff_loc, q_loc)
        return pltpu.make_async_copy(w_in_hbm.at[source(group), :, cols], w_in_ref.at[group, :, cols], in_sem.at[0, group])

    def in_copy(group):
        cols = pl.ds(0, 2 * ff_loc)
        return pltpu.make_async_copy(w_in_hbm.at[source(group), :, cols], w_in_ref.at[group, :, cols], in_sem.at[1, group])

    def out_copy(group, part):
        return pltpu.make_async_copy(
            w_out_hbm.at[source(group), part], w_out_ref.at[group, :, pl.ds(part * half, half)], out_sem.at[group, part]
        )

    out_first = [out_copy(0, part) for part in range(n_parts)]
    early = out_first + [in_copy(1)] if has_ready else [in_copy(0)] + out_first + [in_copy(1)]

    def copies(*groups):
        return [in_copy(group) for group in groups if not has_ready or group % 2] + [out_copy(group, part) for group in groups for part in range(n_parts)]

    slot = lax.rem(step, 2)
    other = 1 - slot

    def project_query(src, group, dst):
        q = jnp.dot(h_ref[src], w_in_ref[group, :, 2 * ff_loc :], preferred_element_type=F32).astype(BF16)
        query_ref[dst] = (q * BF16(head_dim**-0.5)).T

    def normalize_part(dst, src_ref, part):
        rows = pl.ds(part * rows_part, rows_part)
        h_ref[dst, rows] = norm_rows(src_ref[rows], gain_ref[...])

    def transpose_part(dst, src_ref, part):
        span = n_chunks // 2
        block = src_ref[pl.ds(part * span, span)].reshape(span * t_loc, 2 * head_dim)
        vt_ref[dst, part] = block.T[head_dim:]

    def epilogue_part(src, part):
        rows = pl.ds(part * rows_part, rows_part)
        y = (x_before_ref[rows].astype(F32) + acc_ref[src, rows]).astype(BF16)
        y_ref[rows] = y
        if has_next:
            h_next = norm_rows(y, gain_next_ref[...])
            kv_next_ref[rows] = jnp.dot(h_next, w_kv_next_ref[...], preferred_element_type=F32).astype(BF16)

    def project_out(joined_slot, group, dst, fresh, col):
        cols = slice(col, col + tile)
        z = jnp.dot(joined_ref[joined_slot], w_out_ref[group, :, cols], preferred_element_type=F32)
        z = z.astype(BF16).astype(F32)
        base = acc_ref[dst, :, cols]
        if fresh is not None:
            base = jnp.where(fresh, 0.0, base)
        acc_ref[dst, :, cols] = base + z

    @pl.when(step == 0)
    def _():
        for group in range(n_groups):
            query_copy(group).start()
        for copy in early:
            copy.start()
        for part in range(2):
            normalize_part(slot, x_before_ref, part)
            transpose_part(slot, kv_ref, part)
        joined_ref[1] = jnp.zeros_like(joined_ref[1])
        acc_ref[1] = jnp.zeros_like(acc_ref[1])
        for group in range(n_groups):
            query_copy(group).wait()
        project_query(slot, 0, 0)

    @pl.when(step == n_seqs)
    def _():
        for col in range(0, d_model, tile):
            project_out(1, n_groups - 1, other, None, col)
        for part in range(2):
            epilogue_part(other, part)

    def run(n_keys):
        chunk = n_keys - 1
        seq_len = len_ref[micro, jnp.minimum(step, n_seqs - 1)]
        lane = lax.broadcasted_iota(jnp.int32, (1, t_loc), 1)
        limit = jnp.minimum(lane + (pos - chunk) * t_loc, seq_len - chunk * t_loc - 1)
        key = lax.broadcasted_iota(jnp.int32, (t_loc, t_loc), 0)

        def trip(pair, carry):
            first = 2 * pair
            before = jnp.where(jnp.logical_and(step == 0, pair == 0), 0, lax.rem(first + n_groups - 1, n_groups))

            @pl.when(step == 0)
            def _():
                late = [out_copy(1, part) for part in range(n_parts)] + copies(*range(2, n_groups))

                @pl.when(pair == 0)
                def _():
                    for copy in early:
                        copy.wait()
                    for copy in late:
                        copy.start()

                @pl.when(pair == 1)
                def _():
                    for copy in late:
                        copy.wait()

            h = h_ref[slot]
            dst_before = jnp.where(pair == 0, other, slot)
            tops = {}
            sums = {}

            def query(sub):
                if sub == 0:
                    project_query(slot, first + 1, 1)
                else:
                    project_query(jnp.where(pair == n_groups // 2 - 1, other, slot), lax.rem(first + 2, n_groups), 0)

            def gate_up(sub, part):
                if has_ready and sub == 0:
                    cols = pl.ds(pl.multiple_of(pair * ff_loc + part * tile, LANES), tile)
                    joined_ref[sub, :, part * tile : (part + 1) * tile] = ready_ref[:, cols]
                    return
                for col in range(part * tile, (part + 1) * tile, lanes):
                    both = jnp.dot(h, w_in_ref[first + sub, :, 2 * col : 2 * (col + lanes)], preferred_element_type=F32)
                    both = both.astype(BF16).astype(F32)
                    gate, up = both[:, :lanes], both[:, lanes:]
                    joined_ref[sub, :, col : col + lanes] = (jax.nn.silu(gate) * up).astype(BF16)

            def score(sub, head):
                q_t = query_ref[sub, head * head_dim : (head + 1) * head_dim]
                best = None
                for c in range(n_keys):
                    s = jnp.dot(kv_ref[c, :, :head_dim], q_t, preferred_element_type=F32)
                    if c == chunk:
                        s = jnp.where(key <= limit, s, NEG_BIG)
                    s_ref[head, c * t_loc : (c + 1) * t_loc] = s
                    m = jnp.max(s.reshape(t_loc // 8, 8, t_loc), axis=0)
                    best = m if best is None else jnp.maximum(best, m)
                tops[sub, head] = jnp.max(best, axis=0, keepdims=True)

            def softmax(sub, head):
                total = None
                top = tops[sub, head]
                width = 16
                for r in range(0, n_keys * t_loc, width):
                    e = jnp.exp(s_ref[head, r : r + width] - top)
                    t = jnp.sum(e.reshape(width // 8, 8, t_loc), axis=0)
                    total = t if total is None else total + t
                    p_ref[head, r : r + width] = e.astype(BF16)
                sums[sub, head] = jnp.sum(total, axis=0, keepdims=True)

            outs = {}

            def value(sub, head):
                span = n_chunks // 2 * t_loc
                out_t = None
                for part in range(2):
                    size = min(span, n_keys * t_loc - part * span)
                    if size <= 0:
                        continue
                    o = jnp.dot(vt_ref[slot, part, :, :size], p_ref[head, part * span : part * span + size], preferred_element_type=F32)
                    out_t = o if out_t is None else out_t + o
                outs[sub, head] = (out_t / sums[sub, head]).astype(BF16)
                if head == heads - 1:
                    joined_ref[sub, :, ff_loc:] = jnp.concatenate([outs[sub, i] for i in range(heads)], axis=0).T

            for sub in range(2):
                if sub == 0:
                    z = lambda i: project_out(1, before, dst_before, None, i * tile)
                else:
                    z = lambda i: project_out(0, first, slot, pair == 0, i * tile)
                score(sub, 0)
                z(0)
                score(sub, 1)
                softmax(sub, 0)
                z(1)
                score(sub, 2)
                softmax(sub, 1)
                value(sub, 0)
                z(2)
                gate_up(sub, 0)
                if sub == 0:
                    query(sub)
                    normalize_part(other, x_after_ref, pair)
                    transpose_part(other, kv_after_ref, pair)
                softmax(sub, 2)
                value(sub, 1)
                gate_up(sub, 1)
                if sub == 1:
                    query(sub)
                    epilogue_part(other, pair)
                value(sub, 2)
                gate_up(sub, 2)
            return carry

        lax.fori_loop(0, n_groups // 2, trip, 0)

    seq_len = len_ref[micro, jnp.minimum(step, n_seqs - 1)]
    n_live = jnp.minimum(pos + 1, (seq_len + t_loc - 1) // t_loc)
    for n_keys in range(1, n_chunks + 1):
        pl.when(jnp.logical_and(n_live == n_keys, step < n_seqs))(functools.partial(run, n_keys))


def run_layer(pos, lengths, x, kv, gain, w_in, w_out, head_dim, micro, ready=None, next_params=None, prev=None, whole=None):
    n_seqs, t_loc, d_model = x.shape[-3:]

    def after(b):
        return jnp.minimum(b + 1, n_seqs - 1)

    def now(b):
        return jnp.minimum(b, n_seqs - 1)

    def before(b):
        return jnp.maximum(b - 1, 0)

    def x_spec(seq):
        if x.ndim == 4:
            return pl.BlockSpec((None, None) + x.shape[2:], lambda b, *_: (micro, seq(b), 0, 0))
        return pl.BlockSpec((None,) + x.shape[1:], lambda b, *_: (seq(b), 0, 0))

    n_groups, _, in_loc = w_in.shape
    _, n_parts, rows_out, _ = w_out.shape
    n_chunks = kv.shape[0]
    width = kv.shape[-1]

    def kv_spec(seq):
        return pl.BlockSpec((n_chunks, None, t_loc, width), lambda b, *_: (0, seq(b), 0, 0))

    anywhere = pl.BlockSpec(memory_space=pl.ANY)
    in_specs = [
        x_spec(after),
        x_spec(before),
        kv_spec(now),
        kv_spec(after),
        pl.BlockSpec((1, d_model), lambda b, *_: (0, 0)),
        anywhere,
        anywhere,
    ]
    args = [x, x, kv, kv, gain, w_in, w_out]
    if ready is not None:
        in_specs.append(pl.BlockSpec((t_loc, ready.shape[1]), lambda b, *_: (micro * n_seqs + now(b), 0)))
        args.append(ready)
    if next_params is not None:
        in_specs += [pl.BlockSpec((1, d_model), lambda b, *_: (0, 0)), pl.BlockSpec((d_model, width), lambda b, *_: (0, 0))]
        args += list(next_params)
    aliases = {}
    if prev is not None:
        in_specs.append(anywhere)
        aliases = {2 + len(args): 0}
        args.append(prev)
    if whole is None:
        out_shape = [jax.ShapeDtypeStruct((n_seqs, t_loc, d_model), BF16)]
        out_specs = [pl.BlockSpec((None, t_loc, d_model), lambda b, *_: (before(b), 0, 0))]
    else:
        out_shape = [jax.ShapeDtypeStruct((whole, n_seqs, t_loc, d_model), BF16)]
        out_specs = [pl.BlockSpec((None, None, t_loc, d_model), lambda b, *_: (micro, before(b), 0, 0))]
    if next_params is not None:
        out_shape.append(jax.ShapeDtypeStruct((n_seqs, t_loc, width), BF16))
        out_specs.append(pl.BlockSpec((None, t_loc, width), lambda b, *_: (before(b), 0, 0)))
    rows = n_seqs * t_loc
    heads = (2 * rows_out - in_loc) // head_dim
    flops = 2 * rows * n_groups * d_model * (in_loc + rows_out) + 8 * rows * n_groups * n_chunks * t_loc * (rows_out * 2 - in_loc + rows_out)
    return pl.pallas_call(
        functools.partial(layer_kernel, micro, n_groups, head_dim, ready is not None, next_params is not None, prev is not None),
        grid_spec=pltpu.PrefetchScalarGridSpec(
            num_scalar_prefetch=2,
            grid=(n_seqs + 1,),
            in_specs=in_specs,
            out_specs=out_specs,
            scratch_shapes=[
                pltpu.VMEM((n_groups, d_model, in_loc), BF16),
                pltpu.VMEM((n_groups, rows_out, d_model), BF16),
                pltpu.VMEM((2, t_loc, d_model), BF16),
                pltpu.VMEM((2, 2, head_dim, n_chunks // 2 * t_loc), BF16),
                pltpu.VMEM((2, t_loc, rows_out), BF16),
                pltpu.VMEM((2, t_loc, d_model), F32),
                pltpu.VMEM((heads, n_chunks * t_loc, t_loc), F32),
                pltpu.VMEM((heads, n_chunks * t_loc, t_loc), BF16),
                pltpu.VMEM((2, heads * head_dim, t_loc), BF16),
                pltpu.SemaphoreType.DMA((2, n_groups)),
                pltpu.SemaphoreType.DMA((n_groups, n_parts)),
            ],
        ),
        out_shape=out_shape,
        input_output_aliases=aliases,
        name="layer",
        compiler_params=pltpu.CompilerParams(dimension_semantics=("arbitrary",), vmem_limit_bytes=60 * 2**20),
        cost_estimate=pl.CostEstimate(flops=flops, bytes_accessed=4 * rows * d_model + 2 * n_groups * d_model * (in_loc + rows_out), transcendentals=0),
    )(pos, lengths, *args)


def solution(mesh):
    n_model = mesh.shape["model"]
    n_data = mesh.shape["data"]
    act_spec = P(None, ("part", "data"), "model", None)

    def local_fn(x, lengths, gain_blk, w_in_blk, w_kv_blk, w_out_blk):
        n_micro = x.shape[0]
        n_layers, d_half, in_loc = w_in_blk.shape
        out_loc = w_out_blk.shape[1]
        head_dim = w_kv_blk.shape[2] // 2
        pos = lax.axis_index("model").astype(jnp.int32).reshape(1)

        own = sort_weights(w_in_blk, w_out_blk, head_dim)
        (w_in_all, w_out_all, kv_first, kv_rest, ready), gain, w_kv = startup(x, gain_blk, w_kv_blk, *own[0], n_model, n_data)
        own, kv_first, kv_rest = lax.optimization_barrier((own[1:], kv_first, kv_rest))
        kv = [kv_first] + [lax.all_gather(kv_rest[micro], "model", axis=0, tiled=False) for micro in range(n_micro - 1)]
        params = [(w_in_all, w_out_all)]
        for pair in own:
            params.append([lax.all_gather(w, ("model", "data"), axis=0, tiled=False) for w in pair])

        def weights(layer):
            w_in, w_out = params[layer]
            return w_in.reshape(n_model, -1, in_loc), w_out.reshape(n_model, n_data, out_loc, d_half)

        hidden = [x] * n_micro
        result = None
        for layer in range(n_layers):
            w_in, w_out = weights(layer)
            last = layer == n_layers - 1
            kv_next = []
            for micro in range(n_micro):
                outs = run_layer(
                    pos, lengths, hidden[micro], kv[micro], gain[layer], w_in, w_out, head_dim, micro,
                    ready=ready if layer == 0 else None,
                    next_params=None if last else (gain[layer + 1], w_kv[layer + 1]),
                    prev=result if last else None,
                    whole=n_micro if last else None,
                )
                if last:
                    result = outs[0]
                else:
                    hidden[micro] = outs[0]
                    kv_next.append(lax.all_gather(outs[1], "model", axis=0, tiled=False))
            kv = kv_next
        return result

    return jax.shard_map(
        local_fn,
        mesh=mesh,
        in_specs=(act_spec, P(None, ("part", "data")), P(None, "data"), P(None, "data", "model"), P(None, "data", None), P(None, "model", "data")),
        out_specs=act_spec,
        check_vma=False,
    )
```

```python
import functools
import jax
import jax.numpy as jnp
from jax import lax
from jax.experimental import pallas as pl
from jax.experimental.pallas import tpu as pltpu
from jax.sharding import PartitionSpec as P

NORM_EPS = 1e-6
NEG_BIG = -1e30
F32 = jnp.float32
BF16 = jnp.bfloat16
LANES = 128
MESH = pl.DeviceIdType.MESH


def norm_rows(x_act, gain_row):
    x_f32 = x_act.astype(F32)
    centered = x_f32 - jnp.mean(x_f32, axis=-1, keepdims=True)
    variance = jnp.mean(centered * centered, axis=-1, keepdims=True)
    return (centered * lax.rsqrt(variance + NORM_EPS) * gain_row.astype(F32)).astype(BF16)


def sort_kernel(head_dim, in_ref, out_ref, *sorted_refs):
    n_layers, in_loc, _ = in_ref.shape
    out_loc = out_ref.shape[1]
    ff_loc = in_loc - out_loc
    heads = (out_loc - ff_loc) // head_dim
    ff_head = ff_loc // heads
    unit_in = in_loc // heads
    unit_out = out_loc // heads
    blocks = ff_head // LANES
    for layer in range(n_layers):
        in_sorted_ref, out_sorted_ref = sorted_refs[2 * layer : 2 * layer + 2]
        for head in range(heads):
            base = head * unit_in
            for part in range(blocks):
                col = 2 * LANES * (head * blocks + part)
                gate = base + head_dim + part * LANES
                up = gate + ff_head
                in_sorted_ref[:, col : col + LANES] = in_ref[layer, gate : gate + LANES].T
                in_sorted_ref[:, col + LANES : col + 2 * LANES] = in_ref[layer, up : up + LANES].T
            row = head * unit_out
            out_sorted_ref[head * ff_head : (head + 1) * ff_head] = out_ref[layer, row + head_dim : row + unit_out]
            out_sorted_ref[ff_loc + head * head_dim : ff_loc + (head + 1) * head_dim] = out_ref[layer, row : row + head_dim]
        queries = jnp.concatenate([in_ref[layer, h * unit_in : h * unit_in + head_dim] for h in range(heads)], axis=0)
        in_sorted_ref[:, 2 * ff_loc :] = queries.T


def sort_weights(w_in, w_out, head_dim):
    n_layers, d_half, in_loc = w_in.shape
    vmem = pl.BlockSpec(memory_space=pltpu.VMEM)
    outs = [jax.ShapeDtypeStruct(w_in.shape[1:], BF16), jax.ShapeDtypeStruct(w_out.shape[1:], BF16)] * n_layers
    outs = pl.pallas_call(
        functools.partial(sort_kernel, head_dim),
        in_specs=[vmem, vmem],
        out_specs=[vmem] * len(outs),
        out_shape=outs,
        name="sort_weights",
        cost_estimate=pl.CostEstimate(flops=10**6, bytes_accessed=4 * (w_in.size + w_out.size), transcendentals=0),
    )(jnp.swapaxes(w_in, 1, 2), w_out)
    return [outs[2 * layer : 2 * layer + 2] for layer in range(n_layers)]


def startup_kernel(
    n_layers, x_hbm, gain_ref, w_kv_ref, w_in_ref, w_out_ref, w_in_hbm, w_out_hbm, kv_hbm, kv_rest_hbm, ready_hbm, *refs
):
    gain_out_refs, w_kv_out_refs = refs[:n_layers], refs[n_layers : 2 * n_layers]
    (
    in_buf, out_buf, kv_buf, gain_buf, w_kv_buf, x_buf, h_buf, ready_w_buf, ready_buf,
    own_send, own_recv, fwd_send, fwd_recv, small_send, small_recv,
    kv_send, kv_recv, x_sem, store_sem, kv_store_sem, kv_rest_sem, ready_sem,
    ) = refs[2 * n_layers :]
    data = lax.axis_index("data")
    model = lax.axis_index("model")
    _, d_half, width = w_kv_ref.shape
    n_micro, n_seqs, t_loc, d_model = x_hbm.shape
    block = x_buf.shape[1]
    per_micro = n_seqs // block
    n_blocks = n_micro * per_micro

    chip = model // 2
    core = model % 2
    mate = 2 * chip + 1 - core
    across = 2 * (1 - chip) + core
    across_mate = 2 * (1 - chip) + 1 - core
    flip = 1 - data
    to_mate = {"model": mate}
    to_x = {"model": across}
    to_y = {"data": flip}

    barrier = pltpu.get_barrier_semaphore()
    for peer in (to_mate, to_x, to_y):
        pl.semaphore_signal(barrier, inc=1, device_id=peer, device_id_type=MESH)
    pl.semaphore_wait(barrier, 3)

    def remote(src, dst, send, recv, peer):
        return pltpu.make_async_remote_copy(src_ref=src, dst_ref=dst, send_sem=send, recv_sem=recv, device_id=peer, device_id_type=MESH)

    def place(m, d):
        return 2 * m + d

    me = place(model, data)
    in_rows = d_half // 2
    out_rows = w_out_ref.shape[0] // 2

    def own_item(i):
        if i < 2:
            return w_in_ref.at[pl.ds(i % 2 * in_rows, in_rows)]
        return w_out_ref.at[pl.ds(i % 2 * out_rows, out_rows)]

    def buf_item(slot, i):
        if i < 2:
            return in_buf.at[slot, pl.ds(i % 2 * in_rows, in_rows)]
        return out_buf.at[slot, pl.ds(i % 2 * out_rows, out_rows)]

    def hbm_item(slot, i):
        if i < 2:
            return w_in_hbm.at[slot, pl.ds(i % 2 * in_rows, in_rows)]
        return w_out_hbm.at[slot, pl.ds(i % 2 * out_rows, out_rows)]

    gain_copy = remote(gain_ref, gain_buf.at[data], small_send.at[0], small_recv.at[0], to_y)
    w_kv_copy = remote(w_kv_ref, w_kv_buf.at[data], small_send.at[1], small_recv.at[1], to_y)
    gain_copy.start()
    w_kv_copy.start()

    def x_copy(t):
        return pltpu.make_async_copy(x_hbm.at[t // per_micro, pl.ds(t % per_micro * block, block)], x_buf.at[t % 2], x_sem.at[t % 2])

    x_copy(0).start()

    own = {}
    for i in range(4):
        for k, peer in enumerate((to_y, to_x, to_mate)):
            own[k, i] = remote(own_item(i), buf_item(me, i), own_send.at[k, i], own_recv.at[k, i], peer)
            own[k, i].start()
    stores = []

    def store(slot, i, src):
        copy = pltpu.make_async_copy(src, hbm_item(slot, i), store_sem.at[len(stores)])
        copy.start()
        stores.append(copy)

    for i in range(4):
        store(me, i, own_item(i))

    gain_copy.wait()
    w_kv_copy.wait()
    gain_buf[data] = gain_ref[...]
    w_kv_buf[data] = w_kv_ref[...]
    for layer in range(n_layers):
        for d in range(2):
            gain_out_refs[layer][:, d * d_half : (d + 1) * d_half] = gain_buf[d, layer : layer + 1]
            w_kv_out_refs[layer][d * d_half : (d + 1) * d_half] = w_kv_buf[d, layer]
    gain = jnp.concatenate([gain_buf[d, 0:1] for d in range(2)], axis=1)
    w_kv = jnp.concatenate([w_kv_buf[d, 0] for d in range(2)], axis=0)

    def kv_place(m, t):
        return kv_buf.at[t, m]

    def kv_copy(k, t, m, peer):
        return remote(kv_place(m, t), kv_place(m, t), kv_send.at[k, t], kv_recv.at[k, t], peer)

    def kv_store(k, t, m):
        return pltpu.make_async_copy(kv_place(m, t), kv_hbm.at[m, pl.ds(t * block, block)], kv_store_sem.at[k, t])

    def kv_rest_store(t):
        rest = t - per_micro
        return pltpu.make_async_copy(
            kv_place(model, t), kv_rest_hbm.at[rest // per_micro, pl.ds(rest % per_micro * block, block)], kv_rest_sem.at[rest]
        )

    def send_kv(t):
        kv_copy(0, t, model, to_x).start()
        kv_copy(1, t, model, to_mate).start()
        kv_store(0, t, model).start()

    def kv_step(t, carry):
        @pl.when(t + 1 < n_blocks)
        def _():
            x_copy(t + 1).start()

        x_copy(t).wait()
        h = norm_rows(x_buf[t % 2].reshape(block * t_loc, d_model), gain)
        h_buf[t] = h
        kv = jnp.dot(h, w_kv, preferred_element_type=F32).astype(BF16)
        kv_buf[t, model] = kv.reshape(block, t_loc, width)

        @pl.when(jnp.logical_and(t > 0, t <= per_micro))
        def _():
            send_kv(t - 1)

        @pl.when(t > per_micro)
        def _():
            kv_rest_store(t - 1).start()

        return carry

    lax.fori_loop(0, n_blocks, kv_step, 0)

    kv_rest_store(n_blocks - 1).start()

    forward = {}

    def pass_on(k, i, slot, peer):
        forward[k, i] = remote(buf_item(slot, i), buf_item(slot, i), fwd_send.at[k, i], fwd_recv.at[k, i], peer)
        forward[k, i].start()

    def take_y(i):
        own[0, i].wait_recv()
        slot = place(model, flip)
        pass_on(2, i, slot, to_mate)
        store(slot, i, buf_item(slot, i))

    def take_mate(i):
        own[2, i].wait_recv()
        slot = place(mate, data)
        store(slot, i, buf_item(slot, i))

    def take_mate_y(i):
        forward[2, i].wait_recv()
        slot = place(mate, flip)
        store(slot, i, buf_item(slot, i))

    for i in range(2):
        take_y(i)
    for i in range(2):
        take_mate(i)
    for i in range(2):
        take_mate_y(i)

    cols = ready_w_buf.shape[2]
    ready_w_buf[core, pl.ds(data * d_half, d_half)] = w_in_ref[:, :cols]
    ready_w_buf[core, pl.ds(flip * d_half, d_half)] = in_buf[place(model, flip), :, :cols]
    ready_w_buf[1 - core, pl.ds(data * d_half, d_half)] = in_buf[place(mate, data), :, :cols]
    ready_w_buf[1 - core, pl.ds(flip * d_half, d_half)] = in_buf[place(mate, flip), :, :cols]

    rows = ready_buf.shape[1]
    per_block = block * t_loc // rows

    def ready_store(u):
        return pltpu.make_async_copy(ready_buf.at[u % 2], ready_hbm.at[pl.ds(u * rows, rows)], ready_sem.at[u % 2])

    def ready_step(u, carry):
        @pl.when(u >= 2)
        def _():
            ready_store(u - 2).wait()

        h = h_buf[u // per_block, pl.ds(u % per_block * rows, rows)]
        for sub in range(2):
            for col in range(0, cols // 2, LANES):
                both = jnp.dot(h, ready_w_buf[sub, :, 2 * col : 2 * (col + LANES)], preferred_element_type=F32)
                both = both.astype(BF16).astype(F32)
                gate, up = both[:, :LANES], both[:, LANES:]
                at = sub * (cols // 2) + col
                ready_buf[u % 2, :, at : at + LANES] = (jax.nn.silu(gate) * up).astype(BF16)
        ready_store(u).start()
        return carry

    n_ready = n_blocks * per_block
    first_part = n_ready * 3 // 8
    lax.fori_loop(0, first_part, ready_step, 0)

    for i in range(4):
        own[1, i].wait_recv()
        slot = place(across, data)
        if i < 3:
            pass_on(0, i, slot, to_y)
        pass_on(1, i, slot, to_mate)
        store(slot, i, buf_item(slot, i))
    for i in range(2, 4):
        take_y(i)
        if i == 3:
            pass_on(0, i, place(model, flip), to_x)
        take_mate(i)

    lax.fori_loop(first_part, n_ready, ready_step, 0)
    ready_store(n_ready - 2).wait()
    ready_store(n_ready - 1).wait()

    for i in range(4):
        for t in range(i * per_micro // 4, (i + 1) * per_micro // 4):
            kv_copy(0, t, model, to_x).wait_recv()
            kv_copy(2, t, across, to_mate).start()
            kv_store(1, t, across).start()
            kv_copy(1, t, model, to_mate).wait_recv()
            kv_store(2, t, mate).start()
        forward[0, i].wait_recv()
        slot = place(across, flip)
        pass_on(3, i, slot, to_mate)
        store(slot, i, buf_item(slot, i))
        forward[1, i].wait_recv()
        slot = place(across_mate, data)
        store(slot, i, buf_item(slot, i))
        if i >= 2:
            take_mate_y(i)

    for t in range(per_micro):
        kv_copy(2, t, across, to_mate).wait_recv()
        kv_store(3, t, across_mate).start()
    for i in range(4):
        forward[3, i].wait_recv()
        slot = place(across_mate, flip)
        store(slot, i, buf_item(slot, i))

    for copy in own.values():
        copy.wait_send()
    for copy in forward.values():
        copy.wait_send()
    for t in range(per_micro, n_blocks):
        kv_rest_store(t).wait()
    for t in range(per_micro):
        kv_copy(0, t, model, to_x).wait_send()
        kv_copy(1, t, model, to_mate).wait_send()
        kv_copy(2, t, across, to_mate).wait_send()
        for k, m in enumerate((model, across, mate, across_mate)):
            kv_store(k, t, m).wait()
    for copy in stores:
        copy.wait()


def startup(x, gain, w_kv, w_in, w_out, n_model, n_data):
    n_micro, n_seqs, t_loc, d_model = x.shape
    n_layers, d_half, width = w_kv.shape
    _, in_loc = w_in.shape
    out_loc, _ = w_out.shape
    n_all = n_model * n_data
    block = 4
    n_blocks = n_micro * n_seqs // block
    vmem = pl.BlockSpec(memory_space=pltpu.VMEM)
    anywhere = pl.BlockSpec(memory_space=pl.ANY)
    dma = pltpu.SemaphoreType.DMA
    per_micro = n_seqs // block
    ff_loc = in_loc - out_loc
    outs = pl.pallas_call(
        functools.partial(startup_kernel, n_layers),
        in_specs=[anywhere, vmem, vmem, vmem, vmem],
        out_specs=[anywhere] * 5 + [vmem] * (2 * n_layers),
        out_shape=[
            jax.ShapeDtypeStruct((n_all, d_half, in_loc), BF16),
            jax.ShapeDtypeStruct((n_all, out_loc, d_half), BF16),
            jax.ShapeDtypeStruct((n_model, n_seqs, t_loc, width), BF16),
            jax.ShapeDtypeStruct((n_micro - 1, n_seqs, t_loc, width), BF16),
            jax.ShapeDtypeStruct((n_micro * n_seqs * t_loc, 2 * ff_loc), BF16),
        ]
        + [jax.ShapeDtypeStruct((1, d_model), BF16)] * n_layers
        + [jax.ShapeDtypeStruct((d_model, width), BF16)] * n_layers,
        scratch_shapes=[
            pltpu.VMEM((n_all, d_half, in_loc), BF16),
            pltpu.VMEM((n_all, out_loc, d_half), BF16),
            pltpu.VMEM((n_blocks, n_model, block, t_loc, width), BF16),
            pltpu.VMEM((n_data, n_layers, d_half), BF16),
            pltpu.VMEM((n_data, n_layers, d_half, width), BF16),
            pltpu.VMEM((2, block, t_loc, d_model), BF16),
            pltpu.VMEM((n_blocks, block * t_loc, d_model), BF16),
            pltpu.VMEM((2, d_model, 2 * ff_loc), BF16),
            pltpu.VMEM((2, 2 * t_loc, 2 * ff_loc), BF16),
            dma((3, 4)), dma((3, 4)), dma((4, 4)), dma((4, 4)), dma((2,)), dma((2,)),
            dma((3, per_micro)), dma((3, per_micro)), dma((2,)), dma((4 * n_all,)), dma((4, per_micro)), dma((n_blocks - per_micro,)), dma((2,)),
        ],
        name="startup",
        compiler_params=pltpu.CompilerParams(collective_id=0, has_side_effects=True, vmem_limit_bytes=60 * 2**20),
        cost_estimate=pl.CostEstimate(flops=10**11, bytes_accessed=10**8, transcendentals=0),
    )(x, gain, w_kv, w_in, w_out)
    return outs[:5], outs[5 : 5 + n_layers], outs[5 + n_layers :]


def layer_kernel(micro, n_groups, head_dim, has_ready, has_next, has_prev, *refs):
    refs = list(refs)
    pos_ref, len_ref = refs[:2]
    x_after_ref, x_before_ref, kv_ref, kv_after_ref, gain_ref, w_in_hbm, w_out_hbm = refs[2:9]
    refs = refs[9:]
    ready_ref = None
    if has_ready:
        ready_ref = refs[0]
        refs = refs[1:]
    if has_next:
        gain_next_ref, w_kv_next_ref = refs[:2]
        refs = refs[2:]
    if has_prev:
        refs = refs[1:]
    y_ref = refs[0]
    refs = refs[1:]
    if has_next:
        kv_next_ref = refs[0]
        refs = refs[1:]
    w_in_ref, w_out_ref, h_ref, vt_ref, joined_ref, acc_ref, s_ref, p_ref, query_ref, in_sem, out_sem = refs

    t_loc, d_model = x_after_ref.shape
    n_chunks = kv_ref.shape[0]
    rows_out = w_out_ref.shape[1]
    half = w_out_hbm.shape[3]
    n_parts = w_out_hbm.shape[1]
    in_loc = w_in_ref.shape[2]
    ff_loc = in_loc - rows_out
    q_loc = rows_out - ff_loc
    heads = q_loc // head_dim
    step = pl.program_id(0)
    n_seqs = pl.num_programs(0) - 1
    tile = 256
    lanes = LANES
    rows_part = t_loc // 2

    pos = pos_ref[0]

    def source(group):
        if has_ready:
            chip = pos // 2
            return 2 * (chip if group % 2 == 0 else 1 - chip) + group // 2
        return group

    def query_copy(group):
        cols = pl.ds(2 * ff_loc, q_loc)
        return pltpu.make_async_copy(w_in_hbm.at[source(group), :, cols], w_in_ref.at[group, :, cols], in_sem.at[0, group])

    def in_copy(group):
        cols = pl.ds(0, 2 * ff_loc)
        return pltpu.make_async_copy(w_in_hbm.at[source(group), :, cols], w_in_ref.at[group, :, cols], in_sem.at[1, group])

    def out_copy(group, part):
        return pltpu.make_async_copy(
            w_out_hbm.at[source(group), part], w_out_ref.at[group, :, pl.ds(part * half, half)], out_sem.at[group, part]
        )

    out_first = [out_copy(0, part) for part in range(n_parts)]
    early = out_first + [in_copy(1)] if has_ready else [in_copy(0)] + out_first + [in_copy(1)]

    def copies(*groups):
        return [in_copy(group) for group in groups if not has_ready or group % 2] + [out_copy(group, part) for group in groups for part in range(n_parts)]

    slot = lax.rem(step, 2)
    other = 1 - slot

    def project_query(src, group, dst):
        q = jnp.dot(h_ref[src], w_in_ref[group, :, 2 * ff_loc :], preferred_element_type=F32).astype(BF16)
        query_ref[dst] = (q * BF16(head_dim**-0.5)).T

    def normalize_part(dst, src_ref, part):
        rows = pl.ds(part * rows_part, rows_part)
        h_ref[dst, rows] = norm_rows(src_ref[rows], gain_ref[...])

    def transpose_part(dst, src_ref, part):
        span = n_chunks // 2
        block = src_ref[pl.ds(part * span, span)].reshape(span * t_loc, 2 * head_dim)
        vt_ref[dst, part] = block.T[head_dim:]

    def epilogue_part(src, part):
        rows = pl.ds(part * rows_part, rows_part)
        y = (x_before_ref[rows].astype(F32) + acc_ref[src, rows]).astype(BF16)
        y_ref[rows] = y
        if has_next:
            h_next = norm_rows(y, gain_next_ref[...])
            kv_next_ref[rows] = jnp.dot(h_next, w_kv_next_ref[...], preferred_element_type=F32).astype(BF16)

    def project_out(joined_slot, group, dst, fresh, col):
        cols = slice(col, col + tile)
        z = jnp.dot(joined_ref[joined_slot], w_out_ref[group, :, cols], preferred_element_type=F32)
        z = z.astype(BF16).astype(F32)
        base = acc_ref[dst, :, cols]
        if fresh is not None:
            base = jnp.where(fresh, 0.0, base)
        acc_ref[dst, :, cols] = base + z

    @pl.when(step == 0)
    def _():
        for group in range(n_groups):
            query_copy(group).start()
        for copy in early:
            copy.start()
        for part in range(2):
            normalize_part(slot, x_before_ref, part)
            transpose_part(slot, kv_ref, part)
        joined_ref[1] = jnp.zeros_like(joined_ref[1])
        acc_ref[1] = jnp.zeros_like(acc_ref[1])
        for group in range(n_groups):
            query_copy(group).wait()
        project_query(slot, 0, 0)

    @pl.when(step == n_seqs)
    def _():
        for col in range(0, d_model, tile):
            project_out(1, n_groups - 1, other, None, col)
        for part in range(2):
            epilogue_part(other, part)

    def run(n_keys):
        chunk = n_keys - 1
        seq_len = len_ref[micro, jnp.minimum(step, n_seqs - 1)]
        lane = lax.broadcasted_iota(jnp.int32, (1, t_loc), 1)
        limit = jnp.minimum(lane + (pos - chunk) * t_loc, seq_len - chunk * t_loc - 1)
        key = lax.broadcasted_iota(jnp.int32, (t_loc, t_loc), 0)

        def trip(pair, carry):
            first = 2 * pair
            before = jnp.where(jnp.logical_and(step == 0, pair == 0), 0, lax.rem(first + n_groups - 1, n_groups))

            @pl.when(step == 0)
            def _():
                late = [out_copy(1, part) for part in range(n_parts)] + copies(*range(2, n_groups))

                @pl.when(pair == 0)
                def _():
                    for copy in early:
                        copy.wait()
                    for copy in late:
                        copy.start()

                @pl.when(pair == 1)
                def _():
                    for copy in late:
                        copy.wait()

            h = h_ref[slot]
            dst_before = jnp.where(pair == 0, other, slot)
            tops = {}
            sums = {}

            def query(sub):
                if sub == 0:
                    project_query(slot, first + 1, 1)
                else:
                    project_query(jnp.where(pair == n_groups // 2 - 1, other, slot), lax.rem(first + 2, n_groups), 0)

            def gate_up(sub, part):
                if has_ready and sub == 0:
                    cols = pl.ds(pl.multiple_of(pair * ff_loc + part * tile, LANES), tile)
                    joined_ref[sub, :, part * tile : (part + 1) * tile] = ready_ref[:, cols]
                    return
                for col in range(part * tile, (part + 1) * tile, lanes):
                    both = jnp.dot(h, w_in_ref[first + sub, :, 2 * col : 2 * (col + lanes)], preferred_element_type=F32)
                    both = both.astype(BF16).astype(F32)
                    gate, up = both[:, :lanes], both[:, lanes:]
                    joined_ref[sub, :, col : col + lanes] = (jax.nn.silu(gate) * up).astype(BF16)

            def score(sub, head):
                q_t = query_ref[sub, head * head_dim : (head + 1) * head_dim]
                best = None
                for c in range(n_keys):
                    s = jnp.dot(kv_ref[c, :, :head_dim], q_t, preferred_element_type=F32)
                    if c == chunk:
                        s = jnp.where(key <= limit, s, NEG_BIG)
                    s_ref[head, c * t_loc : (c + 1) * t_loc] = s
                    m = jnp.max(s.reshape(t_loc // 8, 8, t_loc), axis=0)
                    best = m if best is None else jnp.maximum(best, m)
                tops[sub, head] = jnp.max(best, axis=0, keepdims=True)

            def softmax(sub, head):
                total = None
                top = tops[sub, head]
                width = 16
                for r in range(0, n_keys * t_loc, width):
                    e = jnp.exp(s_ref[head, r : r + width] - top)
                    t = jnp.sum(e.reshape(width // 8, 8, t_loc), axis=0)
                    total = t if total is None else total + t
                    p_ref[head, r : r + width] = e.astype(BF16)
                sums[sub, head] = jnp.sum(total, axis=0, keepdims=True)

            outs = {}

            def value(sub, head):
                span = n_chunks // 2 * t_loc
                out_t = None
                for part in range(2):
                    size = min(span, n_keys * t_loc - part * span)
                    if size <= 0:
                        continue
                    o = jnp.dot(vt_ref[slot, part, :, :size], p_ref[head, part * span : part * span + size], preferred_element_type=F32)
                    out_t = o if out_t is None else out_t + o
                outs[sub, head] = (out_t / sums[sub, head]).astype(BF16)
                if head == heads - 1:
                    joined_ref[sub, :, ff_loc:] = jnp.concatenate([outs[sub, i] for i in range(heads)], axis=0).T

            for sub in range(2):
                if sub == 0:
                    z = lambda i: project_out(1, before, dst_before, None, i * tile)
                else:
                    z = lambda i: project_out(0, first, slot, pair == 0, i * tile)
                score(sub, 0)
                z(0)
                score(sub, 1)
                softmax(sub, 0)
                z(1)
                score(sub, 2)
                softmax(sub, 1)
                value(sub, 0)
                z(2)
                gate_up(sub, 0)
                if sub == 0:
                    query(sub)
                    normalize_part(other, x_after_ref, pair)
                    transpose_part(other, kv_after_ref, pair)
                softmax(sub, 2)
                value(sub, 1)
                gate_up(sub, 1)
                if sub == 1:
                    query(sub)
                    epilogue_part(other, pair)
                value(sub, 2)
                gate_up(sub, 2)
            return carry

        lax.fori_loop(0, n_groups // 2, trip, 0)

    seq_len = len_ref[micro, jnp.minimum(step, n_seqs - 1)]
    n_live = jnp.minimum(pos + 1, (seq_len + t_loc - 1) // t_loc)
    for n_keys in range(1, n_chunks + 1):
        pl.when(jnp.logical_and(n_live == n_keys, step < n_seqs))(functools.partial(run, n_keys))


def run_layer(pos, lengths, x, kv, gain, w_in, w_out, head_dim, micro, ready=None, next_params=None, prev=None, whole=None):
    n_seqs, t_loc, d_model = x.shape[-3:]

    def after(b):
        return jnp.minimum(b + 1, n_seqs - 1)

    def now(b):
        return jnp.minimum(b, n_seqs - 1)

    def before(b):
        return jnp.maximum(b - 1, 0)

    def x_spec(seq):
        if x.ndim == 4:
            return pl.BlockSpec((None, None) + x.shape[2:], lambda b, *_: (micro, seq(b), 0, 0))
        return pl.BlockSpec((None,) + x.shape[1:], lambda b, *_: (seq(b), 0, 0))

    n_groups, _, in_loc = w_in.shape
    _, n_parts, rows_out, _ = w_out.shape
    n_chunks = kv.shape[0]
    width = kv.shape[-1]

    def kv_spec(seq):
        return pl.BlockSpec((n_chunks, None, t_loc, width), lambda b, *_: (0, seq(b), 0, 0))

    anywhere = pl.BlockSpec(memory_space=pl.ANY)
    in_specs = [
        x_spec(after),
        x_spec(before),
        kv_spec(now),
        kv_spec(after),
        pl.BlockSpec((1, d_model), lambda b, *_: (0, 0)),
        anywhere,
        anywhere,
    ]
    args = [x, x, kv, kv, gain, w_in, w_out]
    if ready is not None:
        in_specs.append(pl.BlockSpec((t_loc, ready.shape[1]), lambda b, *_: (micro * n_seqs + now(b), 0)))
        args.append(ready)
    if next_params is not None:
        in_specs += [pl.BlockSpec((1, d_model), lambda b, *_: (0, 0)), pl.BlockSpec((d_model, width), lambda b, *_: (0, 0))]
        args += list(next_params)
    aliases = {}
    if prev is not None:
        in_specs.append(anywhere)
        aliases = {2 + len(args): 0}
        args.append(prev)
    if whole is None:
        out_shape = [jax.ShapeDtypeStruct((n_seqs, t_loc, d_model), BF16)]
        out_specs = [pl.BlockSpec((None, t_loc, d_model), lambda b, *_: (before(b), 0, 0))]
    else:
        out_shape = [jax.ShapeDtypeStruct((whole, n_seqs, t_loc, d_model), BF16)]
        out_specs = [pl.BlockSpec((None, None, t_loc, d_model), lambda b, *_: (micro, before(b), 0, 0))]
    if next_params is not None:
        out_shape.append(jax.ShapeDtypeStruct((n_seqs, t_loc, width), BF16))
        out_specs.append(pl.BlockSpec((None, t_loc, width), lambda b, *_: (before(b), 0, 0)))
    rows = n_seqs * t_loc
    heads = (2 * rows_out - in_loc) // head_dim
    flops = 2 * rows * n_groups * d_model * (in_loc + rows_out) + 8 * rows * n_groups * n_chunks * t_loc * (rows_out * 2 - in_loc + rows_out)
    return pl.pallas_call(
        functools.partial(layer_kernel, micro, n_groups, head_dim, ready is not None, next_params is not None, prev is not None),
        grid_spec=pltpu.PrefetchScalarGridSpec(
            num_scalar_prefetch=2,
            grid=(n_seqs + 1,),
            in_specs=in_specs,
            out_specs=out_specs,
            scratch_shapes=[
                pltpu.VMEM((n_groups, d_model, in_loc), BF16),
                pltpu.VMEM((n_groups, rows_out, d_model), BF16),
                pltpu.VMEM((2, t_loc, d_model), BF16),
                pltpu.VMEM((2, 2, head_dim, n_chunks // 2 * t_loc), BF16),
                pltpu.VMEM((2, t_loc, rows_out), BF16),
                pltpu.VMEM((2, t_loc, d_model), F32),
                pltpu.VMEM((heads, n_chunks * t_loc, t_loc), F32),
                pltpu.VMEM((heads, n_chunks * t_loc, t_loc), BF16),
                pltpu.VMEM((2, heads * head_dim, t_loc), BF16),
                pltpu.SemaphoreType.DMA((2, n_groups)),
                pltpu.SemaphoreType.DMA((n_groups, n_parts)),
            ],
        ),
        out_shape=out_shape,
        input_output_aliases=aliases,
        name="layer",
        compiler_params=pltpu.CompilerParams(dimension_semantics=("arbitrary",), vmem_limit_bytes=60 * 2**20),
        cost_estimate=pl.CostEstimate(flops=flops, bytes_accessed=4 * rows * d_model + 2 * n_groups * d_model * (in_loc + rows_out), transcendentals=0),
    )(pos, lengths, *args)


def solution(mesh):
    n_model = mesh.shape["model"]
    n_data = mesh.shape["data"]
    act_spec = P(None, ("part", "data"), "model", None)

    def local_fn(x, lengths, gain_blk, w_in_blk, w_kv_blk, w_out_blk):
        n_micro = x.shape[0]
        n_layers, d_half, in_loc = w_in_blk.shape
        out_loc = w_out_blk.shape[1]
        head_dim = w_kv_blk.shape[2] // 2
        pos = lax.axis_index("model").astype(jnp.int32).reshape(1)

        own = sort_weights(w_in_blk, w_out_blk, head_dim)
        (w_in_all, w_out_all, kv_first, kv_rest, ready), gain, w_kv = startup(x, gain_blk, w_kv_blk, *own[0], n_model, n_data)
        own, kv_first, kv_rest = lax.optimization_barrier((own[1:], kv_first, kv_rest))
        kv = [kv_first] + [lax.all_gather(kv_rest[micro], "model", axis=0, tiled=False) for micro in range(n_micro - 1)]
        params = [(w_in_all, w_out_all)]
        for pair in own:
            params.append([lax.all_gather(w, ("model", "data"), axis=0, tiled=False) for w in pair])
        if n_micro > 1 and n_layers > 1:
            kv[1], params[1][0] = lax.optimization_barrier((kv[1], params[1][0]))

        def weights(layer):
            w_in, w_out = params[layer]
            return w_in.reshape(n_model, -1, in_loc), w_out.reshape(n_model, n_data, out_loc, d_half)

        hidden = [x] * n_micro
        result = None
        for layer in range(n_layers):
            w_in, w_out = weights(layer)
            last = layer == n_layers - 1
            kv_next = []
            for micro in range(n_micro):
                outs = run_layer(
                    pos, lengths, hidden[micro], kv[micro], gain[layer], w_in, w_out, head_dim, micro,
                    ready=ready if layer == 0 else None,
                    next_params=None if last else (gain[layer + 1], w_kv[layer + 1]),
                    prev=result if last else None,
                    whole=n_micro if last else None,
                )
                if last:
                    result = outs[0]
                else:
                    hidden[micro] = outs[0]
                    kv_next.append(lax.all_gather(outs[1], "model", axis=0, tiled=False))
            kv = kv_next
        return result

    return jax.shard_map(
        local_fn,
        mesh=mesh,
        in_specs=(act_spec, P(None, ("part", "data")), P(None, "data"), P(None, "data", "model"), P(None, "data", None), P(None, "model", "data")),
        out_specs=act_spec,
        check_vma=False,
    )
```
